256 devices in a mesh: clip: 2 (over y), ha: 64 (over x, z), ta: 2 (over core).
Axes of the slice: x: 4, y: 2, z: 16, core: 2. Of those that a mesh axis runs over, the one named last changes fastest.
The devices are a block of a 4x16x16 slice.
Arguments:
- latent_tokens: bfloat16 [16, 4096, 64], P('clip', ('ha', 'ta')), parts along dimension 0, may hold values from -8 to 8
- w_in: bfloat16 [3, 3, 3, 16, 384], replicated, may hold values from -0.3125 to 0.3125
- b_in: float32 [384], replicated, may hold values from -3 to 3
- gn_gain: float32 [384], replicated, may hold values from 0.1 to 1.9
- gn_shift: float32 [384], replicated, may hold values from -3 to 3
- w_mid: bfloat16 [3, 3, 3, 384, 384], replicated, may hold values from -0.109375 to 0.109375
- b_mid: float32 [384], replicated, may hold values from -3 to 3
Outputs:
- decoded: bfloat16 [16, 128, 128, 384], P(('clip', 'ta'), 'ha'), parts along dimension 0
The draws below stay inside these ranges and needn't reach their ends.
There are 2 independent parts, one for each index of `clip`. The reference program is written for one: setup_inputs(seed, part) draws one part's arguments, and reference() takes and returns one part's arrays. A program takes and returns all parts, laid end to end along the dimension named above; an argument that names none is the same for every part. Nothing has to cross between parts.
All inputs are finite; a program needn't handle non-finite values.
Results may differ from the reference program's by a relative error of at most 0.0054.
Values may be sent and summed in bfloat16 or wider, within the bound.
A program may use at most 64 MiB of HBM per device.

```python
import jax
import jax.numpy as jnp
from jax import lax

CH = 384
ZC = 16
GROUPS = 32
W = 128
FRAMES = 8
ROWS = 128
TOKENS_F = 4096


def draw_latent_tokens(key, part):
    keys = jax.random.split(key, 3)
    token = jnp.arange(TOKENS_F)
    entry = jnp.arange(4 * ZC)
    row_index = 2 * (token // (W // 2))[:, None] + (entry // (2 * ZC))[None, :]
    channel = entry % ZC
    rough = jnp.exp(jax.random.uniform(keys[0], (FRAMES, ROWS), minval=-1.15, maxval=1.15))
    chan_scale = jnp.exp(jax.random.uniform(keys[1], (ZC,), minval=-0.7, maxval=0.7))
    position = row_index.astype(jnp.float32) / max(ROWS - 1, 1)
    trend = 0.6 + 1.2 * position
    base = jax.random.normal(keys[2], (FRAMES, TOKENS_F, 4 * ZC))
    scale = 0.4 * rough[:, row_index] * trend[None] * chan_scale[channel][None, None, :]
    value = base * scale
    return jnp.clip(value, -8.0, 8.0).astype(jnp.bfloat16)


def gaussian(stream_key, extent, width, most, dtype=jnp.bfloat16):
    values = jax.random.normal(stream_key, extent, jnp.float32) * width
    return jnp.minimum(jnp.maximum(values, -most), most).astype(dtype)


def setup_inputs(seed: int = 0, part: int = 0) -> dict:
    splits = jax.random.split(jax.random.key(seed), 8)
    own_keys = jax.random.split(jax.random.fold_in(splits[7], part), 8)
    return {
        "latent_tokens": draw_latent_tokens(jax.random.fold_in(jax.random.fold_in(splits[7], part), 71), part),
        "w_in": gaussian(splits[1], (3, 3, 3, ZC, CH), (27 * ZC) ** -0.5, 0.3125),
        "b_in": gaussian(splits[2], (CH,), 0.5, 3.0, jnp.float32),
        "gn_gain": jnp.clip(1.0 + 0.18 * jax.random.normal(splits[3], (CH,), jnp.float32), 0.1, 1.9),
        "gn_shift": gaussian(splits[4], (CH,), 0.5, 3.0, jnp.float32),
        "w_mid": gaussian(splits[5], (3, 3, 3, CH, CH), (9 * CH) ** -0.5, 0.109375),
        "b_mid": gaussian(splits[6], (CH,), 0.5, 3.0, jnp.float32),
    }


def causal_conv(field, kernel):
    result = lax.conv_general_dilated(field[None].astype(jnp.float32), kernel.astype(jnp.float32), (1, 1, 1), [(2, 0), (1, 1), (1, 1)], dimension_numbers=('NDHWC', 'DHWIO', 'NDHWC'), precision=lax.Precision.HIGHEST)
    return result[0]

def reference(latent_tokens, w_in, b_in, gn_gain, gn_shift, w_mid, b_mid):
    latent = latent_tokens.reshape(FRAMES, ROWS // 2, W // 2, 2, 2, ZC)
    latent = latent.transpose(0, 1, 3, 2, 4, 5).reshape(FRAMES, ROWS, W, ZC)
    hidden = (causal_conv(latent, w_in) + b_in).astype(jnp.bfloat16)
    values = lax.optimization_barrier(hidden).astype(jnp.float32)
    grouped = values.reshape(FRAMES, ROWS, W, GROUPS, CH // GROUPS)
    mean = lax.optimization_barrier(jnp.mean(grouped, axis=(0, 1, 2, 4), keepdims=True))
    var = lax.optimization_barrier(jnp.mean((grouped - mean) * (grouped - mean), axis=(0, 1, 2, 4), keepdims=True))
    normed = ((grouped - mean) * lax.rsqrt(var + 1e-06)).reshape(FRAMES, ROWS, W, CH)
    active = jax.nn.silu(normed * gn_gain + gn_shift).astype(jnp.bfloat16)
    active = lax.optimization_barrier(active)
    branch = causal_conv(active, w_mid)
    return (values + branch + b_mid).astype(jnp.bfloat16)
```

```python
import functools

import jax
import jax.numpy as jnp
from jax import lax
from jax.experimental import pallas as pl
from jax.experimental.pallas import tpu as pltpu
from jax.sharding import PartitionSpec as P

GROUPS = 32
RING_X = 4
RING_Z = 16
EPS = 1e-06
MESH = pl.DeviceIdType.MESH
BF16 = jnp.bfloat16
F32 = jnp.float32


def exchange_kernel(
    tok_ref, w_hbm, b_ref, gain_ref, shift_ref, mid_hbm,
    h_ref, stat_ref, main_ref, rest_ref,
    packed, field, patch, w_big, mid, mine, plane_in, plane_sum, ring_in, sel, one_hot, spread,
    w_sem, mid_sem, send_sem, recv_sem, plane_send, plane_recv, ring_send, ring_recv, know_x, know_z,
):
    ha, ta = lax.axis_index("ha"), lax.axis_index("ta")
    n_ha = lax.axis_size("ha")
    x, z = ha // RING_Z, ha % RING_Z
    channels = h_ref.shape[-1] // 2
    members = channels // GROUPS

    def near(dx, dz, flip):
        hx = (x + dx) % RING_X
        hz = (z + dz) % RING_Z
        return {"ha": hx * RING_Z + hz, "ta": 1 - ta if flip else ta}

    barrier = pltpu.get_barrier_semaphore()

    def greet(device):
        pl.semaphore_signal(barrier, inc=1, device_id=device, device_id_type=MESH)

    greet(near(0, 0, True))
    for flip in (False, True):
        for dz in (1, RING_Z - 1):
            greet(near(0, dz, flip))
        for dx in (1, RING_X - 1):
            greet(near(dx, 0, flip))
    after_edge = (z == RING_Z - 1) & (ha < n_ha - 1)
    before_edge = (z == 0) & (ha > 0)

    @pl.when(after_edge)
    def _():
        for t in (0, 1):
            greet({"ha": ha + 1, "ta": t})

    @pl.when(before_edge)
    def _():
        for t in (0, 1):
            greet({"ha": ha - 1, "ta": t})

    pairs = packed.shape[0]
    for g in range(pairs):
        packed[g] = jnp.concatenate(
            [tok_ref[2 * g].astype(F32), tok_ref[2 * g + 1].astype(F32)], axis=-1
        ).astype(BF16)
    half = packed.shape[1]
    own = pl.ds(ta * half, half)
    ring_edge = jnp.where(after_edge, 2, 0) + jnp.where(before_edge, 2, 0)
    pl.semaphore_wait(barrier, 9 + ring_edge)

    def tokens_to(to_ha, to_ta, place, slot):
        if to_ta:
            src, dst = packed, field.at[pl.ds(0, 4), place, own]
        else:
            src, dst = packed.at[pl.ds(0, 2)], field.at[pl.ds(2, 2), place, own]
        return pltpu.make_async_remote_copy(
            src, dst, send_sem.at[slot], recv_sem.at[place, ta],
            device_id={"ha": to_ha, "ta": to_ta}, device_id_type=MESH,
        )

    def tokens_from(place, src_ta, frames_8):
        there = pl.ds(src_ta * half, half)
        if frames_8:
            src, dst = packed, field.at[pl.ds(0, 4), place, there]
        else:
            src, dst = packed.at[pl.ds(0, 2)], field.at[pl.ds(2, 2), place, there]
        return pltpu.make_async_remote_copy(
            src, dst, send_sem.at[0], recv_sem.at[place, src_ta],
            device_id={"ha": ha, "ta": ta}, device_id_type=MESH,
        )

    @pl.when(ha < n_ha - 1)
    def _():
        tokens_to(ha + 1, 1, 0, 0).start()
        tokens_to(ha + 1, 0, 0, 1).start()

    @pl.when(ha > 0)
    def _():
        tokens_to(ha - 1, 1, 2, 2).start()
        tokens_to(ha - 1, 0, 2, 3).start()

    @pl.when(ta == 0)
    def _():
        tokens_to(ha, 1, 1, 4).start()

    @pl.when(ta == 1)
    def _():
        tokens_to(ha, 0, 1, 4).start()

    w_copies = []
    for high in (0, 1):
        for p in range(3):
            for b in (0, 1):
                w_copies.append(
                    pltpu.make_async_copy(
                        w_hbm.at[p],
                        w_big.at[high, p, pl.ds(high, 3), pl.ds(16 * b, 48), pl.ds(channels * b, channels)],
                        w_sem.at[len(w_copies)],
                    )
                )
    for copy in w_copies:
        copy.start()
    for high in (0, 1):
        w_big[high, :, 3 * (1 - high)] = jnp.zeros_like(w_big[high, :, 0])
        for p in range(3):
            for q in range(3):
                w_big[high, p, high + q, 48:64, :channels] = jnp.zeros((16, channels), BF16)
                w_big[high, p, high + q, 0:16, channels:] = jnp.zeros((16, channels), BF16)

    @pl.when(ta == 0)
    def _():
        field[0:2] = jnp.zeros_like(field[0:2])
        field[2:4, 1, own] = packed[0:2]

    @pl.when(ta == 1)
    def _():
        field[0:4, 1, own] = packed[0:4]

    @pl.when(ha == 0)
    def _():
        field[:, 0] = jnp.zeros_like(field[:, 0])

    @pl.when(ha == n_ha - 1)
    def _():
        field[:, 2] = jnp.zeros_like(field[:, 2])

    k = lax.broadcasted_iota(jnp.int32, sel.shape, 0)
    n = lax.broadcasted_iota(jnp.int32, sel.shape, 1)
    step, lane = k // 128, k % 128
    column = 2 * step + (lane // 16) % 2 - 1
    same = (lane // 32 == n // 64) & (lane % 16 == n % 16)
    sel[...] = jnp.where(same & (column == (n // 16) % 4), 1.0, 0.0).astype(BF16)
    k = lax.broadcasted_iota(jnp.int32, one_hot.shape, 0)
    n = lax.broadcasted_iota(jnp.int32, one_hot.shape, 1)
    low = jnp.where(n < GROUPS, n * members, channels + (n - GROUPS) * members)
    one_hot[...] = jnp.where((n < 2 * GROUPS) & (k >= low) & (k < low + members), 1.0, 0.0)
    k = lax.broadcasted_iota(jnp.int32, spread.shape, 0)
    n = lax.broadcasted_iota(jnp.int32, spread.shape, 1)
    low = jnp.where(k < GROUPS, k * members, channels + (k - GROUPS) * members)
    spread[...] = jnp.where((k < 2 * GROUPS) & (n >= low) & (n < low + members), 1.0, 0.0)

    def tell(sem, device):
        pl.semaphore_signal(sem, inc=1, device_id=device, device_id_type=MESH)

    tell(know_x, near(1, 0, False))
    tell(know_x, near(RING_X - 1, 0, False))
    tell(know_z.at[0], near(0, 1, False))
    tell(know_z.at[0], near(0, RING_Z - 1, False))
    for copy in w_copies:
        copy.wait()
    pl.semaphore_wait(know_z.at[0], 2)
    tell(know_z.at[1], near(0, 2, False))
    tell(know_z.at[1], near(0, RING_Z - 2, False))

    for frames_8 in (False, True):

        @pl.when(ta == int(frames_8))
        def _():
            tokens_from(1, int(not frames_8), frames_8).wait_recv()

            @pl.when(ha > 0)
            def _():
                for t in (0, 1):
                    tokens_from(0, t, frames_8).wait_recv()

            @pl.when(ha < n_ha - 1)
            def _():
                for t in (0, 1):
                    tokens_from(2, t, frames_8).wait_recv()

    tokens = field.shape[2]
    row = lax.broadcasted_iota(jnp.int32, (tokens, 128), 0)
    for i in range(3):
        stack = []
        for g in range(pairs):
            now = field[g, i].astype(F32)
            left = jnp.where(row == 0, 0.0, pltpu.roll(now, 1, 0))
            right = jnp.where(row == tokens - 1, 0.0, pltpu.roll(now, tokens - 1, 0))
            stack.append(jnp.concatenate([left, now, right], axis=-1).astype(BF16))
        moved = jnp.dot(jnp.concatenate(stack, axis=0), sel[...], preferred_element_type=F32)
        moved = moved.astype(BF16)
        for g in range(pairs):
            for f in (0, 1):
                patch[2 * g + f, :, 128 * i : 128 * i + 128] = moved[
                    g * tokens : (g + 1) * tokens, 128 * f : 128 * f + 128
                ]

    bias = b_ref[...].reshape(1, -1)
    bias = jnp.concatenate([bias, bias], axis=-1)

    def hidden_rows(y, first, frames):
        lanes = slice(0, 256) if y < 2 else slice(128, 384)
        high = y % 2
        total = bias
        for p in range(3):
            lhs = patch[first + p : first + p + frames, :, lanes].reshape(frames * tokens, 256)
            total = total + jnp.dot(
                lhs, w_big[high, p].reshape(256, 2 * channels), preferred_element_type=F32
            )
        return total.astype(BF16)

    sums = jnp.zeros((1, 2 * channels), F32)
    squares = jnp.zeros((1, 2 * channels), F32)
    for y in (1, 2):
        rows = hidden_rows(y, 2, 4)
        h_ref[2:6, y] = rows.reshape(4, tokens, 2 * channels)
        values = rows.astype(F32)
        sums = sums + jnp.sum(values, axis=0, keepdims=True)
        squares = squares + jnp.sum(values * values, axis=0, keepdims=True)
    folded = jnp.concatenate(
        [sums[:, :channels] + sums[:, channels:], squares[:, :channels] + squares[:, channels:]], axis=-1
    )
    mine[...] = jnp.dot(
        folded, one_hot[...], preferred_element_type=F32, precision=lax.Precision.HIGHEST
    )

    pl.semaphore_wait(know_z.at[1], 2)
    tell(know_z.at[2], near(0, 4, False))
    tell(know_z.at[2], near(0, RING_Z - 4, False))
    pl.semaphore_wait(know_x, 2)

    plane = []
    for dx in (2, 1, 3, 0):
        for flip in (0, 1):
            if dx or flip:
                slot = 2 * dx + flip - 1
                plane.append(
                    pltpu.make_async_remote_copy(
                        mine, plane_in.at[slot], plane_send.at[slot], plane_recv.at[slot],
                        device_id=near(dx, 0, bool(flip)), device_id_type=MESH,
                    )
                )
    for copy in plane:
        copy.start()

    h_ref[0:6, 0] = hidden_rows(0, 0, 6).reshape(6, tokens, 2 * channels)
    h_ref[0:6, 3] = hidden_rows(3, 0, 6).reshape(6, tokens, 2 * channels)
    for y in (1, 2):
        h_ref[0:2, y] = hidden_rows(y, 0, 2).reshape(2, tokens, 2 * channels)

    for p in range(2):
        pltpu.make_async_copy(mid_hbm.at[p], mid.at[p], mid_sem.at[p]).start()
    total = mine[...]
    for copy in plane:
        copy.wait_recv()
    for slot in range(plane_in.shape[0]):
        total = total + plane_in[slot]
    plane_sum[...] = total

    pl.semaphore_wait(know_z.at[2], 2)
    ring = []
    for d in sorted(range(1, RING_Z), key=lambda d: -min(d, RING_Z - d)):
        ring.append(
            pltpu.make_async_remote_copy(
                plane_sum, ring_in.at[d - 1], ring_send.at[d - 1], ring_recv.at[d - 1],
                device_id=near(0, d, False), device_id_type=MESH,
            )
        )
    for copy in ring:
        copy.start()


    wide = main_ref.shape[2]
    rest = channels - wide

    def fetch(p):
        return pltpu.make_async_copy(mid_hbm.at[p], mid.at[p % 2], mid_sem.at[p % 2])

    def bank(tap_0, tap_1, tap_2):
        ends = tap_0 + tap_2
        return tap_0, 0.5 * (ends + tap_1), 0.5 * (ends - tap_1), tap_2

    for i in range(16):
        rest_ref[i, 3 * channels :, :rest] = jnp.zeros((channels, rest), BF16)
        rest_ref[i, :channels, rest:] = jnp.zeros((channels, rest), BF16)
    for p in range(3):
        fetch(p).wait()

        def transform(step, carry):
            at = pl.multiple_of(step * 16, 16)
            for part in range(channels // 128):
                lanes = slice(128 * part, 128 * part + 128)
                taps = [
                    [mid[p % 2, q, r, pl.ds(at, 16), lanes].astype(F32) for r in range(3)] for q in range(3)
                ]
                by_row = [bank(*[taps[q][r] for q in range(3)]) for r in range(3)]
                for i in range(4):
                    for k, value in enumerate(bank(*[by_row[r][i] for r in range(3)])):
                        value = value.astype(BF16)
                        if 128 * part < wide:
                            main_ref[4 * i + k, pl.ds(at + p * channels, 16), lanes] = value
                        else:
                            rest_ref[4 * i + k, pl.ds(at + p * channels, 16), :rest] = value
                            rest_ref[4 * i + k, pl.ds(at + (p + 1) * channels, 16), rest:] = value
            return carry

        lax.fori_loop(0, channels // 16, transform, 0)
        if p == 0:
            fetch(2).start()

    @pl.when(ha < n_ha - 1)
    def _():
        tokens_to(ha + 1, 1, 0, 0).wait_send()
        tokens_to(ha + 1, 0, 0, 1).wait_send()

    @pl.when(ha > 0)
    def _():
        tokens_to(ha - 1, 1, 2, 2).wait_send()
        tokens_to(ha - 1, 0, 2, 3).wait_send()

    @pl.when(ta == 0)
    def _():
        tokens_to(ha, 1, 1, 4).wait_send()

    @pl.when(ta == 1)
    def _():
        tokens_to(ha, 0, 1, 4).wait_send()

    for copy in plane:
        copy.wait_send()

    for copy in ring:
        copy.wait_recv()
    for slot in range(ring_in.shape[0]):
        total = total + ring_in[slot]
    for copy in ring:
        copy.wait_send()

    count = n_ha * lax.axis_size("ta") * 4 * 2 * 2 * tokens * members
    spread_out = jnp.dot(
        total * (1.0 / count), spread[...], preferred_element_type=F32, precision=lax.Precision.HIGHEST
    )
    mean, square = spread_out[:, :channels], spread_out[:, channels:]
    var = jnp.maximum(square - mean * mean, 0.0)
    scale = lax.rsqrt(var + EPS) * gain_ref[...].reshape(1, -1)
    stat_ref[0:1] = 0.5 * scale
    stat_ref[1:2] = 0.5 * (shift_ref[...].reshape(1, -1) - mean * scale)


def decode_kernel(h_ref, stat_ref, main_ref, rest_ref, b_ref, out_ref, planes, acc, rows_f32):
    ha, ta = lax.axis_index("ha"), lax.axis_index("ta")
    n_ha = lax.axis_size("ha")
    frames_in, rows_in, tokens, width = h_ref.shape
    channels = width // 2
    frames, rows = frames_in - 2, rows_in - 2
    wide = main_ref.shape[2]
    rest = channels - wide
    place = lax.broadcasted_iota(jnp.int32, (tokens, 128), 0)

    def activate(f, carry):
        inside = [
            (f >= 2 - 2 * ta) & (ha * rows + y >= 1) & (ha * rows + y <= n_ha * rows) for y in range(rows_in)
        ]
        for part in range(channels // 128):
            lanes = slice(128 * part, 128 * part + 128)
            scale, shift = stat_ref[0:1, lanes], stat_ref[1:2, lanes]
            by_column = []
            for y in range(rows_in):
                row_scale = jnp.where(inside[y], scale, 0.0)
                row_shift = jnp.where(inside[y], shift, 0.0)

                def active(b):
                    lo = b * channels + 128 * part
                    value = h_ref[f, y, :, lo : lo + 128].astype(F32) * row_scale + row_shift
                    return value + value * jnp.tanh(value)

                even, odd = active(0), active(1)
                before = jnp.where(place == 0, 0.0, pltpu.roll(odd, 1, 0)).astype(BF16)
                after = jnp.where(place == tokens - 1, 0.0, pltpu.roll(even, tokens - 1, 0)).astype(BF16)
                even, odd = even.astype(BF16), odd.astype(BF16)
                by_column.append((before - odd, even + odd, odd - even, even - after))
            for k in range(4):
                y0, y1, y2, y3 = [by_column[y][k] for y in range(4)]
                for i, value in enumerate((y0 - y2, y1 + y2, y2 - y1, y1 - y3)):
                    planes[4 * i + k, f, :, lanes] = value
        return carry

    lax.fori_loop(0, frames_in, activate, 0)

    signs = ((1, 1, 1, 0), (0, 1, -1, -1))
    first = [[True, True], [True, True]]
    for i in range(4):
        for k in range(4):
            at = 4 * i + k
            lhs = jnp.concatenate([planes[at, p : p + frames] for p in range(3)], axis=-1)
            lhs = lhs.reshape(frames * tokens, 3 * channels)
            product = jnp.dot(lhs, main_ref[at], preferred_element_type=F32)
            lhs = jnp.concatenate(
                [
                    jnp.concatenate([planes[at, t + p] for p in range(4)], axis=-1)
                    for t in range(0, frames, 2)
                ],
                axis=0,
            )
            other = jnp.dot(lhs, rest_ref[at], preferred_element_type=F32)
            for y in (0, 1):
                for b in (0, 1):
                    sign = signs[y][i] * signs[b][k]
                    if not sign:
                        continue
                    for f in range(frames):
                        one = product[f * tokens : (f + 1) * tokens]
                        two = other[f // 2 * tokens : (f // 2 + 1) * tokens, rest * (f % 2) : rest * (f % 2) + rest]
                        for value, lanes in ((one, slice(0, wide)), (two, slice(wide, channels))):
                            value = value if sign > 0 else -value
                            if not first[y][b]:
                                value = acc[y, b, f, :, lanes] + value
                            acc[y, b, f, :, lanes] = value
                    first[y][b] = False
    bias = b_ref[...].reshape(1, -1)
    for f in range(frames):
        for y in range(rows):
            for b in (0, 1):
                hidden = h_ref[f + 2, y + 1, :, b * channels : (b + 1) * channels].astype(F32)
                total = acc[y, b, f] + hidden + bias
                for part in range(channels // 128):
                    rows_f32[part, pl.ds(b, tokens, stride=2)] = total[:, 128 * part : 128 * part + 128]
            for part in range(channels // 128):
                out_ref[f, y, :, 128 * part : 128 * part + 128] = rows_f32[part].astype(BF16)


def keep(value):
    return pltpu.with_memory_space_constraint(value, pltpu.HBM)


def body(latent_tokens, w_in, b_in, gn_gain, gn_shift, w_mid, b_mid):
    frames_all, half, token_lanes = latent_tokens.shape
    channels = w_in.shape[-1]
    tokens = 2 * half
    wide = channels // 256 * 256
    rest = channels - wide
    vmem = pl.BlockSpec(memory_space=pltpu.VMEM)
    hbm = pl.BlockSpec(memory_space=pltpu.HBM)
    hidden, stats, main, other = pl.pallas_call(
        exchange_kernel,
        out_shape=(
            jax.ShapeDtypeStruct((6, 4, tokens, 2 * channels), BF16),
            jax.ShapeDtypeStruct((2, channels), F32),
            jax.ShapeDtypeStruct((16, 3 * channels, wide), BF16),
            jax.ShapeDtypeStruct((16, 4 * channels, 2 * rest), BF16),
        ),
        in_specs=[vmem, hbm, vmem, vmem, vmem, hbm],
        out_specs=(vmem, vmem, vmem, vmem),
        scratch_shapes=[
            pltpu.VMEM((4, half, 128), BF16),
            pltpu.VMEM((4, 3, tokens, 128), BF16),
            pltpu.VMEM((8, tokens, 384), BF16),
            pltpu.VMEM((2, 3, 4, 64, 2 * channels), BF16),
            pltpu.VMEM((2, 3, 3, channels, channels), BF16),
            pltpu.VMEM((1, 128), F32),
            pltpu.VMEM((7, 1, 128), F32),
            pltpu.VMEM((1, 128), F32),
            pltpu.VMEM((RING_Z - 1, 1, 128), F32),
            pltpu.VMEM((384, 256), BF16),
            pltpu.VMEM((2 * channels, 128), F32),
            pltpu.VMEM((128, 2 * channels), F32),
            pltpu.SemaphoreType.DMA((12,)),
            pltpu.SemaphoreType.DMA((2,)),
            pltpu.SemaphoreType.DMA((5,)),
            pltpu.SemaphoreType.DMA((3, 2)),
            pltpu.SemaphoreType.DMA((7,)),
            pltpu.SemaphoreType.DMA((7,)),
            pltpu.SemaphoreType.DMA((RING_Z - 1,)),
            pltpu.SemaphoreType.DMA((RING_Z - 1,)),
            pltpu.SemaphoreType.REGULAR,
            pltpu.SemaphoreType.REGULAR((3,)),
        ],
        compiler_params=pltpu.CompilerParams(
            collective_id=0, has_side_effects=True, vmem_limit_bytes=16 * 2**20
        ),
        name="exchange",
    )(keep(latent_tokens), keep(w_in.reshape(3, 3, -1, channels)), keep(b_in), keep(gn_gain), keep(gn_shift), keep(w_mid))
    return pl.pallas_call(
        decode_kernel,
        out_shape=jax.ShapeDtypeStruct((4, 2, 2 * tokens, channels), BF16),
        in_specs=[vmem, vmem, vmem, vmem, vmem],
        out_specs=vmem,
        scratch_shapes=[
            pltpu.VMEM((16, 6, tokens, channels), BF16),
            pltpu.VMEM((2, 2, 4, tokens, channels), F32),
            pltpu.VMEM((channels // 128, 2 * tokens, 128), F32),
        ],
        compiler_params=pltpu.CompilerParams(vmem_limit_bytes=16 * 2**20),
        name="decode",
    )(hidden, stats, main, other, b_mid)


def solution(mesh):
    return jax.shard_map(
        body,
        mesh=mesh,
        in_specs=(P("clip", ("ha", "ta"), None), P(), P(), P(), P(), P(), P()),
        out_specs=P(("clip", "ta"), "ha", None, None),
        check_vma=False,
    )
```

```python
import jax
import jax.numpy as jnp
from jax import lax
from jax.experimental import pallas as pl
from jax.experimental.pallas import tpu as pltpu
from jax.sharding import PartitionSpec as P

GROUPS = 32
RING_X = 4
RING_Z = 16
EPS = 1e-06
MESH = pl.DeviceIdType.MESH
BF16 = jnp.bfloat16
F32 = jnp.float32


def exchange_kernel(
    tok_hbm, w_hbm, b_hbm, gain_hbm, shift_hbm, b_mid_hbm, mid_hbm,
    h_ref, stat_ref, main_ref, rest_ref,
    tok, vectors, packed, field, patch, w_big, mid, mine, plane_in, plane_sum, ring_in, sel, member,
    tok_sem, vec_sem, w_sem, mid_sem, send_sem, recv_sem,
    plane_send, plane_recv, ring_send, ring_recv, know_x, know_all, know_first,
):
    ha, ta = lax.axis_index("ha"), lax.axis_index("ta")
    n_ha = lax.axis_size("ha")
    x, z = ha // RING_Z, ha % RING_Z
    channels = vectors.shape[1]
    members = channels // GROUPS
    parts = channels // 128

    def near(dx, dz, flip):
        hx = (x + dx) % RING_X
        hz = (z + dz) % RING_Z
        return {"ha": hx * RING_Z + hz, "ta": 1 - ta if flip else ta}
    barrier = pltpu.get_barrier_semaphore()

    def greet(device):
        pl.semaphore_signal(barrier, inc=1, device_id=device, device_id_type=MESH)

    last = RING_Z - 1

    @pl.when(ha < n_ha - 1)
    def _():
        for t in (0, 1):
            greet({"ha": ha + 1, "ta": t})

    @pl.when(ha > 0)
    def _():
        for t in (0, 1):
            greet({"ha": ha - 1, "ta": t})

    for flip in (False, True):
        for dx in (1, RING_X - 1):
            greet(near(dx, 0, flip))
    greet(near(0, 0, True))

    @pl.when(z == 0)
    def _():
        greet(near(0, last, False))

    for d in range(2, last):

        @pl.when((z >= 1) & (z + d <= last))
        def _():
            greet(near(0, d, False))

    tok_copy = pltpu.make_async_copy(tok_hbm, tok, tok_sem)
    tok_copy.start()
    w_copies = [
        pltpu.make_async_copy(
            w_hbm,
            w_big.at[high, :, pl.ds(high, 3), pl.ds(16 * b, 48), pl.ds(channels * b, channels)],
            w_sem.at[2 * high + b],
        )
        for high in (0, 1)
        for b in (0, 1)
    ]
    for copy in w_copies:
        copy.start()
    vector_copies = [
        pltpu.make_async_copy(ref, vectors.at[i], vec_sem.at[i])
        for i, ref in enumerate((b_hbm, gain_hbm, shift_hbm, b_mid_hbm))
    ]
    for copy in vector_copies:
        copy.start()

    wide = main_ref.shape[2]
    rest = channels - wide

    def fetch(p):
        return pltpu.make_async_copy(mid_hbm.at[p], mid.at[p], mid_sem.at[p])

    for p in range(3):
        fetch(p).start()

    def bank(tap_0, tap_1, tap_2):
        ends = tap_0 + tap_2
        return tap_0, 0.5 * (ends + tap_1), 0.5 * (ends - tap_1), tap_2

    def transform(p):
        fetch(p).wait()

        def rows(step, carry):
            at = pl.multiple_of(step * 16, 16)
            for part in range(parts):
                lanes = slice(128 * part, 128 * part + 128)
                taps = [[mid[p, q, r, pl.ds(at, 16), lanes].astype(F32) for r in range(3)] for q in range(3)]
                by_row = [bank(*[taps[q][r] for q in range(3)]) for r in range(3)]
                for i in range(4):
                    for k, value in enumerate(bank(*[by_row[r][i] for r in range(3)])):
                        value = value.astype(BF16)
                        if 128 * part < wide:
                            main_ref[4 * i + k, pl.ds(at + p * channels, 16), lanes] = value
                        else:
                            rest_ref[4 * i + k, pl.ds(at + p * channels, 16), :rest] = value
                            rest_ref[4 * i + k, pl.ds(at + (p + 1) * channels, 16), rest:] = value
            return carry

        lax.fori_loop(0, channels // 16, rows, 0)

    early = z < RING_Z // 2

    @pl.when(early)
    def _():
        transform(0)
        transform(1)
    tok_copy.wait()
    pairs = packed.shape[0]
    for g in range(pairs):
        packed[g] = jnp.concatenate([tok[2 * g].astype(F32), tok[2 * g + 1].astype(F32)], axis=-1).astype(BF16)
    half = packed.shape[1]
    own = pl.ds(ta * half, half)
    expected = (
        5
        + jnp.where(ha > 0, 2, 0)
        + jnp.where(ha < n_ha - 1, 2, 0)
        + jnp.maximum(z - 2, 0)
        + jnp.where(z == last, 1, 0)
    )
    pl.semaphore_wait(barrier, expected)
    def tokens_to(to_ha, to_ta, place, slot):
        if to_ta:
            src, dst = packed, field.at[pl.ds(0, 4), place, own]
        else:
            src, dst = packed.at[pl.ds(0, 2)], field.at[pl.ds(2, 2), place, own]
        return pltpu.make_async_remote_copy(
            src, dst, send_sem.at[slot], recv_sem.at[place, ta],
            device_id={"ha": to_ha, "ta": to_ta}, device_id_type=MESH,
        )

    def tokens_from(place, src_ta, frames_8):
        there = pl.ds(src_ta * half, half)
        if frames_8:
            src, dst = packed, field.at[pl.ds(0, 4), place, there]
        else:
            src, dst = packed.at[pl.ds(0, 2)], field.at[pl.ds(2, 2), place, there]
        return pltpu.make_async_remote_copy(
            src, dst, send_sem.at[0], recv_sem.at[place, src_ta],
            device_id={"ha": ha, "ta": ta}, device_id_type=MESH,
        )

    def each_token_copy(act):
        @pl.when(ha < n_ha - 1)
        def _():
            act(tokens_to(ha + 1, 1, 0, 0))
            act(tokens_to(ha + 1, 0, 0, 1))

        @pl.when(ha > 0)
        def _():
            act(tokens_to(ha - 1, 1, 2, 2))
            act(tokens_to(ha - 1, 0, 2, 3))

        @pl.when(ta == 0)
        def _():
            act(tokens_to(ha, 1, 1, 4))

        @pl.when(ta == 1)
        def _():
            act(tokens_to(ha, 0, 1, 4))

    each_token_copy(lambda copy: copy.start())

    def tell(sem, device):
        pl.semaphore_signal(sem, inc=1, device_id=device, device_id_type=MESH)

    tell(know_x, near(1, 0, False))
    tell(know_x, near(RING_X - 1, 0, False))

    def pass_first(where, onwards):
        @pl.when(where & (z >= 2))
        def _():
            pl.semaphore_wait(know_first, 1)

        @pl.when(where & (z >= 1) & onwards)
        def _():
            tell(know_first, near(0, 1, False))

    pass_first(early, True)
    middle = (z == RING_Z // 2) | (z == RING_Z // 2 + 1)

    @pl.when(z == last)
    def _():
        for d in range(1, RING_Z):
            tell(know_all, near(0, d, False))
    @pl.when(ta == 0)
    def _():
        field[0:2] = jnp.zeros_like(field[0:2])
        field[2:4, 1, own] = packed[0:2]

    @pl.when(ta == 1)
    def _():
        field[0:4, 1, own] = packed[0:4]

    @pl.when(ha == 0)
    def _():
        field[:, 0] = jnp.zeros_like(field[:, 0])

    @pl.when(ha == n_ha - 1)
    def _():
        field[:, 2] = jnp.zeros_like(field[:, 2])

    for high in (0, 1):
        w_big[high, :, 3 * (1 - high)] = jnp.zeros_like(w_big[high, :, 0])
        for p in range(3):
            for q in range(3):
                w_big[high, p, high + q, 48:64, :channels] = jnp.zeros((16, channels), BF16)
                w_big[high, p, high + q, 0:16, channels:] = jnp.zeros((16, channels), BF16)
    k = lax.broadcasted_iota(jnp.int32, sel.shape, 0)
    n = lax.broadcasted_iota(jnp.int32, sel.shape, 1)
    step, lane = k // 128, k % 128
    column = 2 * step + (lane // 16) % 2 - 1
    same = (lane // 32 == n // 64) & (lane % 16 == n % 16)
    sel[...] = jnp.where(same & (column == (n // 16) % 4), 1.0, 0.0).astype(BF16)
    k = lax.broadcasted_iota(jnp.int32, (channels, channels), 0)
    n = lax.broadcasted_iota(jnp.int32, (channels, channels), 1)
    member[...] = jnp.where(k // members == n // members, 1.0, 0.0).astype(BF16)
    for copy in vector_copies:
        copy.wait()
    for copy in w_copies:
        copy.wait()
    for frames_8 in (False, True):

        @pl.when(ta == int(frames_8))
        def _():
            tokens_from(1, int(not frames_8), frames_8).wait_recv()

            @pl.when(ha > 0)
            def _():
                for t in (0, 1):
                    tokens_from(0, t, frames_8).wait_recv()

            @pl.when(ha < n_ha - 1)
            def _():
                for t in (0, 1):
                    tokens_from(2, t, frames_8).wait_recv()
    tokens = field.shape[2]
    row = lax.broadcasted_iota(jnp.int32, (tokens, 128), 0)

    def patches(pairs_now):
        for i in range(3):
            stack = []
            for g in pairs_now:
                now = field[g, i].astype(F32)
                left = jnp.where(row == 0, 0.0, pltpu.roll(now, 1, 0))
                right = jnp.where(row == tokens - 1, 0.0, pltpu.roll(now, tokens - 1, 0))
                stack.append(jnp.concatenate([left, now, right], axis=-1).astype(BF16))
            moved = jnp.dot(jnp.concatenate(stack, axis=0), sel[...], preferred_element_type=F32)
            moved = moved.astype(BF16)
            for at, g in enumerate(pairs_now):
                for f in (0, 1):
                    patch[2 * g + f, i] = moved[at * tokens : (at + 1) * tokens, 128 * f : 128 * f + 128]

    patches((1, 2, 3))
    bias = vectors[0].reshape(1, -1)
    bias = jnp.concatenate([bias, bias], axis=-1)

    def hidden_rows(y, first, frames):
        low, high = y // 2, y % 2
        total = bias
        for p in range(3):
            lhs = [
                patch[first + p : first + p + frames, i].reshape(frames * tokens, 128) for i in (low, low + 1)
            ]
            lhs = jnp.concatenate(lhs, axis=-1)
            total = total + jnp.dot(
                lhs, w_big[high, p].reshape(256, 2 * channels), preferred_element_type=F32
            )
        total = total.astype(BF16).astype(F32)
        for n in range(2 * parts):
            part = total[:, 128 * n : 128 * n + 128]
            h_ref[first : first + frames, y, n] = part.reshape(frames, tokens, 128)
        return total

    sums = jnp.zeros((1, 2 * channels), F32)
    squares = jnp.zeros((1, 2 * channels), F32)
    for y in (1, 2):
        values = hidden_rows(y, 2, 4)
        sums = sums + jnp.sum(values, axis=0, keepdims=True)
        squares = squares + jnp.sum(values * values, axis=0, keepdims=True)
    for at, both in ((0, sums), (parts, squares)):
        one = both[:, :channels] + both[:, channels:]
        for part in range(parts):
            mine[at + part : at + part + 1] = one[:, 128 * part : 128 * part + 128]
    mine[2 * parts :] = jnp.zeros_like(mine[2 * parts :])
    pl.semaphore_wait(know_x, 2)
    plane = []
    for dx in (2, 1, 3, 0):
        for flip in (0, 1):
            if dx or flip:
                slot = 2 * dx + flip - 1
                plane.append(
                    pltpu.make_async_remote_copy(
                        mine, plane_in.at[slot], plane_send, plane_recv,
                        device_id=near(dx, 0, bool(flip)), device_id_type=MESH,
                    )
                )
    for copy in plane:
        copy.start()
    patches((0,))
    hidden_rows(0, 0, 6)
    hidden_rows(3, 0, 6)
    hidden_rows(1, 0, 2)
    hidden_rows(2, 0, 2)
    total = mine[...]
    all_plane = pltpu.make_async_remote_copy(
        plane_in, plane_in, plane_send, plane_recv, device_id=near(0, 0, True), device_id_type=MESH
    )
    all_plane.wait_recv()
    for slot in range(plane_in.shape[0]):
        total = total + plane_in[slot]
    plane_sum[...] = total
    def ring_copy(d):
        return pltpu.make_async_remote_copy(
            plane_sum, ring_in.at[d - 1], ring_send, ring_recv,
            device_id=near(0, d, False), device_id_type=MESH,
        )

    ring_copy(1).start()
    for d in range(2, RING_Z):

        @pl.when((z + d > RING_Z) | ((z == 1) & (d == last)))
        def _():
            ring_copy(d).start()

    pass_first(middle, z == RING_Z // 2)
    for d in range(2, last):

        @pl.when((early | middle) & (z + d == RING_Z))
        def _():
            ring_copy(d).start()
    for i in range(16):
        rest_ref[i, 3 * channels :, :rest] = jnp.zeros((channels, rest), BF16)
        rest_ref[i, :channels, rest:] = jnp.zeros((channels, rest), BF16)
    stat_ref[2:3] = vectors[3].reshape(1, -1)

    @pl.when(early)
    def _():
        transform(2)
    @pl.when(z < last)
    def _():
        pl.semaphore_wait(know_all, 1)

    for d in range(2, RING_Z):

        @pl.when((z + d <= last) | (jnp.logical_not(early | middle) & (z + d == RING_Z) & (z < last)))
        def _():
            ring_copy(d).start()
    @pl.when(jnp.logical_not(early))
    def _():
        for p in range(3):
            transform(p)
    each_token_copy(lambda copy: copy.wait_send())
    all_plane.wait_send()
    all_ring = pltpu.make_async_remote_copy(
        ring_in, ring_in, ring_send, ring_recv, device_id=near(0, 1, False), device_id_type=MESH
    )
    all_ring.wait_recv()
    for slot in range(ring_in.shape[0]):
        total = total + ring_in[slot]
    count = n_ha * lax.axis_size("ta") * 4 * 2 * 2 * tokens * members
    sums = jnp.concatenate([total[part : part + 1] for part in range(parts)], axis=-1)
    squares = jnp.concatenate([total[parts + part : parts + part + 1] for part in range(parts)], axis=-1)
    terms = []
    for value in (sums, squares):
        for _ in range(3):
            term = value.astype(BF16)
            terms.append(term.astype(F32))
            value = value - terms[-1]
    terms = jnp.concatenate(terms + [jnp.zeros((2, channels), F32)], axis=0).astype(BF16)
    shared = jnp.dot(terms, member[...], preferred_element_type=F32) * (1.0 / count)
    mean = shared[0:1] + shared[1:2] + shared[2:3]
    square = shared[3:4] + shared[4:5] + shared[5:6]
    var = jnp.maximum(square - mean * mean, 0.0)
    scale = lax.rsqrt(var + EPS) * vectors[1].reshape(1, -1)
    stat_ref[0:1] = 0.5 * scale
    stat_ref[1:2] = 0.5 * (vectors[2].reshape(1, -1) - mean * scale)
    all_ring.wait_send()


def decode_kernel(
    h_ref, stat_ref, main_ref, rest_ref, out_hbm,
    shifted, columns_wide, columns_rest, planes_wide, planes_rest, acc, rows_f32, out, out_sem,
):
    ha, ta = lax.axis_index("ha"), lax.axis_index("ta")
    n_ha = lax.axis_size("ha")
    frames_in, rows_in, pieces, tokens, _ = h_ref.shape
    parts = pieces // 2
    channels = 128 * parts
    frames, rows = frames_in - 2, rows_in - 2
    wide = main_ref.shape[2]
    rest = channels - wide
    for part in range(parts):
        for y in range(rows_in):
            shifted[part, y, 0, 8 + tokens :] = jnp.zeros((8, 128), F32)
            shifted[part, y, 1, :8] = jnp.zeros((8, 128), F32)

    def activate(f, carry):
        inside = [
            (f >= 2 - 2 * ta) & (ha * rows + y >= 1) & (ha * rows + y <= n_ha * rows) for y in range(rows_in)
        ]
        for y in range(rows_in):
            by_part = []
            for part in range(parts):
                lanes = slice(128 * part, 128 * part + 128)
                row_scale = jnp.where(inside[y], stat_ref[0:1, lanes], 0.0)
                row_shift = jnp.where(inside[y], stat_ref[1:2, lanes], 0.0)
                columns = []
                for b in (0, 1):
                    value = h_ref[f, y, b * parts + part] * row_scale + row_shift
                    value = value + value * jnp.tanh(value)
                    shifted[part, y, b, 8 : 8 + tokens] = value
                    columns.append(value)
                even, odd = columns
                before = shifted[part, y, 1, 7 : 7 + tokens]
                after = shifted[part, y, 0, 9 : 9 + tokens]
                by_part.append((before - odd, even + odd, odd - even, even - after))
            for k in range(4):
                value = jnp.concatenate([by_part[part][k] for part in range(wide // 128)], axis=-1)
                columns_wide[k, f, y] = value.astype(BF16)
                value = jnp.concatenate([by_part[part][k] for part in range(wide // 128, parts)], axis=-1)
                columns_rest[k, f, y] = value.astype(BF16)
        return carry

    lax.fori_loop(0, frames_in, activate, 0)

    def by_rows(i, k):
        one, two = ((0, 2), (1, 2), (2, 1), (1, 3))[i]
        for columns, planes in ((columns_wide, planes_wide), (columns_rest, planes_rest)):
            if i == 1:
                planes[k % 2] = columns[k, :, one] + columns[k, :, two]
            else:
                planes[k % 2] = columns[k, :, one] - columns[k, :, two]

    by_rows(0, 0)
    bias = stat_ref[2:3]
    copies = []

    def finish(y):
        for f in range(frames):
            for part in range(parts):
                lanes = slice(128 * part, 128 * part + 128)
                for b in (0, 1):
                    hidden = h_ref[f + 2, y + 1, b * parts + part]
                    rows_f32[y, f, part, pl.ds(b, tokens, stride=2)] = acc[y, b, f, part] + (
                        hidden + bias[:, lanes]
                    )
                out[f, y, :, lanes] = rows_f32[y, f, part].astype(BF16)
            copies.append(pltpu.make_async_copy(out.at[f, y], out_hbm.at[f, y], out_sem.at[frames * y + f]))
            copies[-1].start()

    signs = ((1, 1, 1, 0), (0, 1, -1, -1))
    first = [[True, True], [True, True]]
    for i in range(4):
        for k in range(4):
            at = 4 * i + k
            if at < 15:
                by_rows((at + 1) // 4, (at + 1) % 4)
            both = (planes_wide.at[k % 2], planes_rest.at[k % 2])
            lhs = [planes[p : p + frames] for p in range(3) for planes in both]
            lhs = jnp.concatenate(lhs, axis=-1).reshape(frames * tokens, 3 * channels)
            product = jnp.dot(lhs, main_ref[at], preferred_element_type=F32)
            lhs = [
                jnp.concatenate([planes[t + p] for p in range(4) for planes in both], axis=-1)
                for t in range(0, frames, 2)
            ]
            other = jnp.dot(jnp.concatenate(lhs, axis=0), rest_ref[at], preferred_element_type=F32)
            for y in (0, 1):
                for b in (0, 1):
                    sign = signs[y][i] * signs[b][k]
                    if not sign:
                        continue
                    for f in range(frames):
                        for part in range(parts):
                            if 128 * part < wide:
                                value = product[f * tokens : (f + 1) * tokens, 128 * part : 128 * part + 128]
                            else:
                                value = other[
                                    f // 2 * tokens : (f // 2 + 1) * tokens,
                                    rest * (f % 2) : rest * (f % 2) + rest,
                                ]
                            if first[y][b]:
                                acc[y, b, f, part] = value if sign > 0 else -value
                            elif sign > 0:
                                acc[y, b, f, part] = acc[y, b, f, part] + value
                            else:
                                acc[y, b, f, part] = acc[y, b, f, part] - value
                    first[y][b] = False
        if i == 2:
            finish(0)
    finish(1)
    for y in (0, 1):
        for f in range(frames):
            copies[frames * y + f].wait()


def keep(value):
    return pltpu.with_memory_space_constraint(value, pltpu.HBM)


def body(latent_tokens, w_in, b_in, gn_gain, gn_shift, w_mid, b_mid):
    half = latent_tokens.shape[1]
    channels = w_in.shape[-1]
    tokens = 2 * half
    wide = channels // 256 * 256
    rest = channels - wide
    parts = channels // 128
    vmem = pl.BlockSpec(memory_space=pltpu.VMEM)
    hbm = pl.BlockSpec(memory_space=pltpu.HBM)
    inputs = (latent_tokens, w_in.reshape(3, 3, -1, channels), b_in, gn_gain, gn_shift, b_mid, w_mid)
    prepared = pl.pallas_call(
        exchange_kernel,
        out_shape=(
            jax.ShapeDtypeStruct((6, 4, 2 * parts, tokens, 128), F32),
            jax.ShapeDtypeStruct((3, channels), F32),
            jax.ShapeDtypeStruct((16, 3 * channels, wide), BF16),
            jax.ShapeDtypeStruct((16, 4 * channels, 2 * rest), BF16),
        ),
        in_specs=[hbm] * len(inputs),
        out_specs=(vmem, vmem, vmem, vmem),
        scratch_shapes=[
            pltpu.VMEM(latent_tokens.shape, BF16),
            pltpu.VMEM((4, channels), F32),
            pltpu.VMEM((4, half, 128), BF16),
            pltpu.VMEM((4, 3, tokens, 128), BF16),
            pltpu.VMEM((8, 3, tokens, 128), BF16),
            pltpu.VMEM((2, 3, 4, 64, 2 * channels), BF16),
            pltpu.VMEM(w_mid.shape, BF16),
            pltpu.VMEM((8, 128), F32),
            pltpu.VMEM((7, 8, 128), F32),
            pltpu.VMEM((8, 128), F32),
            pltpu.VMEM((RING_Z - 1, 8, 128), F32),
            pltpu.VMEM((384, 256), BF16),
            pltpu.VMEM((channels, channels), BF16),
            pltpu.SemaphoreType.DMA,
            pltpu.SemaphoreType.DMA((4,)),
            pltpu.SemaphoreType.DMA((4,)),
            pltpu.SemaphoreType.DMA((3,)),
            pltpu.SemaphoreType.DMA((5,)),
            pltpu.SemaphoreType.DMA((3, 2)),
            pltpu.SemaphoreType.DMA,
            pltpu.SemaphoreType.DMA,
            pltpu.SemaphoreType.DMA,
            pltpu.SemaphoreType.DMA,
            pltpu.SemaphoreType.REGULAR,
            pltpu.SemaphoreType.REGULAR,
            pltpu.SemaphoreType.REGULAR,
        ],
        compiler_params=pltpu.CompilerParams(
            collective_id=0, has_side_effects=True, vmem_limit_bytes=20 * 2**20
        ),
        name="exchange",
    )(*[keep(value) for value in inputs])
    return pl.pallas_call(
        decode_kernel,
        out_shape=jax.ShapeDtypeStruct((4, 2, 2 * tokens, channels), BF16),
        in_specs=[vmem, vmem, vmem, vmem],
        out_specs=hbm,
        scratch_shapes=[
            pltpu.VMEM((parts, 4, 2, tokens + 16, 128), F32),
            pltpu.VMEM((4, 6, 4, tokens, wide), BF16),
            pltpu.VMEM((4, 6, 4, tokens, rest), BF16),
            pltpu.VMEM((2, 6, tokens, wide), BF16),
            pltpu.VMEM((2, 6, tokens, rest), BF16),
            pltpu.VMEM((2, 2, 4, parts, tokens, 128), F32),
            pltpu.VMEM((2, 4, parts, 2 * tokens, 128), F32),
            pltpu.VMEM((4, 2, 2 * tokens, channels), BF16),
            pltpu.SemaphoreType.DMA((8,)),
        ],
        compiler_params=pltpu.CompilerParams(vmem_limit_bytes=18 * 2**20),
        name="decode",
    )(*prepared)


def solution(mesh):
    return jax.shard_map(
        body,
        mesh=mesh,
        in_specs=(P("clip", ("ha", "ta"), None), P(), P(), P(), P(), P(), P()),
        out_specs=P(("clip", "ta"), "ha", None, None),
        check_vma=False,
    )
```

```python
import jax
import jax.numpy as jnp
from jax import lax
from jax.experimental import pallas as pl
from jax.experimental.pallas import tpu as pltpu
from jax.sharding import PartitionSpec as P

GROUPS = 32
RING_X = 4
RING_Z = 16
LATE = 4
EARLY = 4
EPS = 1e-06
MESH = pl.DeviceIdType.MESH
BF16 = jnp.bfloat16
F32 = jnp.float32


def exchange_kernel(
    tok_hbm, w_hbm, b_hbm, gain_hbm, shift_hbm, b_mid_hbm, mid_hbm,
    h_ref, stat_ref, main_ref, rest_ref,
    tok, vectors, packed, field, patch, w_big, mid, mine, plane_in, plane_sum, ring_in, direct_in,
    sel, gather, spread,
    tok_sem, vec_sem, w_sem, mid_sem, send_sem, recv_sem, later_sem,
    plane_send, plane_recv, ring_send, ring_recv, direct_send, direct_recv,
    know_x, know_all, know_first, know_plane,
):
    ha, ta = lax.axis_index("ha"), lax.axis_index("ta")
    n_ha = lax.axis_size("ha")
    x, z = ha // RING_Z, ha % RING_Z
    channels = vectors.shape[1]
    members = channels // GROUPS
    parts = channels // 128

    def near(dx, dz, flip):
        hx = (x + dx) % RING_X
        hz = (z + dz) % RING_Z
        return {"ha": hx * RING_Z + hz, "ta": 1 - ta if flip else ta}
    ring_in[...] = jnp.zeros_like(ring_in)
    direct_in[...] = jnp.zeros_like(direct_in)
    barrier = pltpu.get_barrier_semaphore()

    def greet(device):
        pl.semaphore_signal(barrier, inc=1, device_id=device, device_id_type=MESH)

    last = RING_Z - 1

    @pl.when(ha < n_ha - 1)
    def _():
        for t in (0, 1):
            greet({"ha": ha + 1, "ta": t})

    @pl.when(ha > 0)
    def _():
        for t in (0, 1):
            greet({"ha": ha - 1, "ta": t})

    for flip in (False, True):
        for dx in (1, RING_X - 1):
            greet(near(dx, 0, flip))
    greet(near(0, 0, True))

    @pl.when(z == 0)
    def _():
        greet(near(0, last, False))

    for d in range(2, last):

        @pl.when((z >= 1) & (z + d <= last))
        def _():
            greet(near(0, d, False))

    tok_copy = pltpu.make_async_copy(tok_hbm, tok, tok_sem)
    tok_copy.start()
    w_copies = [
        pltpu.make_async_copy(
            w_hbm,
            w_big.at[high, :, pl.ds(high, 3), pl.ds(16 * b, 48), pl.ds(channels * b, channels)],
            w_sem.at[2 * high + b],
        )
        for high in (0, 1)
        for b in (0, 1)
    ]
    for copy in w_copies:
        copy.start()
    vector_copies = [
        pltpu.make_async_copy(ref, vectors.at[i], vec_sem.at[i])
        for i, ref in enumerate((b_hbm, gain_hbm, shift_hbm, b_mid_hbm))
    ]
    for copy in vector_copies:
        copy.start()

    wide = main_ref.shape[2]
    rest = channels - wide

    def fetch(p):
        return pltpu.make_async_copy(mid_hbm.at[p], mid.at[p], mid_sem.at[p])

    for p in range(3):
        fetch(p).start()

    def bank(tap_0, tap_1, tap_2):
        ends = tap_0 + tap_2
        return tap_0, 0.5 * (ends + tap_1), 0.5 * (ends - tap_1), tap_2

    def transform(p):
        fetch(p).wait()

        def rows(step, carry):
            at = pl.multiple_of(step * 16, 16)
            for part in range(parts):
                lanes = slice(128 * part, 128 * part + 128)
                taps = [[mid[p, q, r, pl.ds(at, 16), lanes].astype(F32) for r in range(3)] for q in range(3)]
                by_row = [bank(*[taps[q][r] for q in range(3)]) for r in range(3)]
                for i in range(4):
                    for k, value in enumerate(bank(*[by_row[r][i] for r in range(3)])):
                        value = value.astype(BF16)
                        if 128 * part < wide:
                            main_ref[4 * i + k, pl.ds(at + p * channels, 16), lanes] = value
                        else:
                            rest_ref[4 * i + k, pl.ds(at + p * channels, 16), :rest] = value
                            rest_ref[4 * i + k, pl.ds(at + (p + 1) * channels, 16), rest:] = value
            return carry

        lax.fori_loop(0, channels // 16, rows, 0)

    early = z < 2
    lower = z < RING_Z // 2

    @pl.when(early)
    def _():
        transform(0)
        transform(1)
    tok_copy.wait()
    lanes = tok.shape[2] // 2
    for a in (0, 1):
        for h in (0, 1):
            packed[a, h] = jnp.concatenate(
                [tok[4 * h + f, :, a * lanes : (a + 1) * lanes].astype(F32) for f in range(4)], axis=-1
            ).astype(BF16)
    half = packed.shape[2]
    own = pl.ds(ta * half, half)
    expected = (
        5
        + jnp.where(ha > 0, 2, 0)
        + jnp.where(ha < n_ha - 1, 2, 0)
        + jnp.maximum(z - 2, 0)
        + jnp.where(z == last, 1, 0)
    )
    pl.semaphore_wait(barrier, expected)
    def tokens_copy(place, a, src_ta, to_ha, to_ta, slot, urgent):
        there = pl.ds(src_ta * half, half)
        frames = pl.ds(0, 2) if to_ta else pl.ds(1, 1)
        of = pl.ds(0, 2) if to_ta else pl.ds(0, 1)
        if a is None:
            src, dst = packed.at[:, of], field.at[place, :, frames, there]
        else:
            src, dst = packed.at[a, of], field.at[place, a, frames, there]
        sem = recv_sem.at[place, src_ta] if urgent else later_sem.at[place // 2, src_ta]
        return pltpu.make_async_remote_copy(
            src, dst, send_sem.at[slot], sem, device_id={"ha": to_ha, "ta": to_ta}, device_id_type=MESH
        )

    def each_token_copy(act, urgent):
        @pl.when(ha < n_ha - 1)
        def _():
            for t in (1, 0):
                act(tokens_copy(0, int(urgent), ta, ha + 1, t, 2 * (1 - int(urgent)) + t, urgent))

        @pl.when(ha > 0)
        def _():
            for t in (1, 0):
                act(tokens_copy(2, 1 - int(urgent), ta, ha - 1, t, 4 + 2 * (1 - int(urgent)) + t, urgent))

        if urgent:
            for t in (1, 0):

                @pl.when(ta == 1 - t)
                def _():
                    act(tokens_copy(1, None, ta, ha, t, 8, True))

    def each_token_arrival(act, urgent):
        for to_ta in (0, 1):

            @pl.when(ta == to_ta)
            def _():
                if urgent:
                    act(tokens_copy(1, None, 1 - to_ta, ha, to_ta, 8, True))

                @pl.when(ha > 0)
                def _():
                    for t in (0, 1):
                        act(tokens_copy(0, int(urgent), t, ha, to_ta, 0, urgent))

                @pl.when(ha < n_ha - 1)
                def _():
                    for t in (0, 1):
                        act(tokens_copy(2, 1 - int(urgent), t, ha, to_ta, 0, urgent))

    each_token_copy(lambda copy: copy.start(), True)
    each_token_copy(lambda copy: copy.start(), False)

    def tell(sem, device):
        pl.semaphore_signal(sem, inc=1, device_id=device, device_id_type=MESH)

    tell(know_x, near(1, 0, False))
    tell(know_x, near(RING_X - 1, 0, False))

    def pass_first(where, onwards):
        @pl.when(where)
        def _():
            pl.semaphore_wait(know_first, 1)

        @pl.when(where & onwards)
        def _():
            tell(know_first, near(0, 1, False))

    @pl.when(z == 1)
    def _():
        tell(know_first, near(0, 1, False))

    middle = (z == RING_Z // 2) | (z == RING_Z // 2 + 1)

    @pl.when(z == last)
    def _():
        for d in range(1, RING_Z):
            tell(know_all, near(0, d, False))
    @pl.when(ta == 0)
    def _():
        field[:, :, 0] = jnp.zeros_like(field[:, :, 0])
        field[1, :, 1, own] = packed[:, 0]

    @pl.when(ta == 1)
    def _():
        field[1, :, :, own] = packed[...]

    @pl.when(ha == 0)
    def _():
        field[0] = jnp.zeros_like(field[0])

    @pl.when(ha == n_ha - 1)
    def _():
        field[2] = jnp.zeros_like(field[2])

    for high in (0, 1):
        w_big[high, :, 3 * (1 - high)] = jnp.zeros_like(w_big[high, :, 0])
        for p in range(3):
            for q in range(3):
                w_big[high, p, high + q, 48:64, :channels] = jnp.zeros((16, channels), BF16)
                w_big[high, p, high + q, 0:16, channels:] = jnp.zeros((16, channels), BF16)
    for i in range(16):
        rest_ref[i, 3 * channels :, :rest] = jnp.zeros((channels, rest), BF16)
        rest_ref[i, :channels, rest:] = jnp.zeros((channels, rest), BF16)
    sel[...] = jnp.zeros_like(sel)
    k = lax.broadcasted_iota(jnp.int32, (lanes, 128), 0)
    n = lax.broadcasted_iota(jnp.int32, (lanes, 128), 1)
    for a in (0, 1):
        for step in range(3):
            column = 2 * step + k // 16 - 1
            block = (n // 64 == a) & (k % 16 == n % 16) & ((n // 16) % 4 == column)
            block = jnp.where(block, 1.0, 0.0).astype(BF16)
            for f in range(4):
                sel[384 * a + 128 * step + lanes * f : 384 * a + 128 * step + lanes * (f + 1), 128 * f : 128 * f + 128] = block
    k = lax.broadcasted_iota(jnp.int32, gather.shape, 0)
    n = lax.broadcasted_iota(jnp.int32, gather.shape, 1)
    gather[...] = jnp.where((k // members == n) & (n < 2 * GROUPS), 1.0, 0.0).astype(BF16)
    k = lax.broadcasted_iota(jnp.int32, spread.shape, 0)
    n = lax.broadcasted_iota(jnp.int32, spread.shape, 1)
    spread[...] = jnp.where((n // members == k) & (k < 2 * GROUPS), 1.0, 0.0).astype(BF16)
    for copy in vector_copies:
        copy.wait()
    stat_ref[2:3] = vectors[3].reshape(1, -1)
    for copy in w_copies:
        copy.wait()
    late = z >= RING_Z - LATE

    def tell_plane(z0):
        @pl.when(z == z0)
        def _():
            for to in range(RING_Z - LATE, RING_Z):
                tell(know_plane.at[z0], {"ha": x * RING_Z + to, "ta": ta})

    @pl.when(z <= 1)
    def _():
        pl.semaphore_wait(know_x, 2)
        pl.semaphore_wait(know_all, 1)

    tell_plane(0)
    tell_plane(1)
    pass_first((z == 2) | (z == 3), True)
    each_token_arrival(lambda copy: copy.wait_recv(), True)
    tokens = field.shape[3]
    row = lax.broadcasted_iota(jnp.int32, (tokens, 128), 0)

    def patches(i, sides):
        stack = []
        for h in (0, 1):
            pieces = []
            for a in sides:
                now = field[i, a, h].astype(F32)
                pieces.append(jnp.where(row == 0, 0.0, pltpu.roll(now, 1, 0)))
                pieces.append(now)
                pieces.append(jnp.where(row == tokens - 1, 0.0, pltpu.roll(now, tokens - 1, 0)))
            stack.append(jnp.concatenate(pieces, axis=-1).astype(BF16))
        chosen = sel[384 * sides[0] : 384 * (sides[-1] + 1)]
        moved = jnp.dot(jnp.concatenate(stack, axis=0), chosen, preferred_element_type=F32).astype(BF16)
        for h in (0, 1):
            for f in range(4):
                patch[4 * h + f, i] = moved[h * tokens : (h + 1) * tokens, 128 * f : 128 * f + 128]

    patches(0, (1,))
    patches(1, (0, 1))
    patches(2, (0,))
    bias = vectors[0].reshape(1, -1)
    bias = jnp.concatenate([bias, bias], axis=-1)

    def hidden_rows(y, first, frames):
        low, high = y // 2, y % 2
        total = bias
        for p in range(3):
            lhs = [
                patch[first + p : first + p + frames, i].reshape(frames * tokens, 128) for i in (low, low + 1)
            ]
            lhs = jnp.concatenate(lhs, axis=-1)
            total = total + jnp.dot(
                lhs, w_big[high, p].reshape(256, 2 * channels), preferred_element_type=F32
            )
        total = total.astype(BF16).astype(F32)
        for n in range(2 * parts):
            part = total[:, 128 * n : 128 * n + 128]
            h_ref[first : first + frames, y, n] = part.reshape(frames, tokens, 128)
        return total

    sums = jnp.zeros((1, 2 * channels), F32)
    squares = jnp.zeros((1, 2 * channels), F32)
    for y in (1, 2):
        values = hidden_rows(y, 2, 4)
        sums = sums + jnp.sum(values, axis=0, keepdims=True)
        squares = squares + jnp.sum(values * values, axis=0, keepdims=True)
    def product(value, matrix):
        terms = []
        for _ in range(3):
            term = value.astype(BF16)
            terms.append(term.astype(F32))
            value = value - terms[-1]
        terms = jnp.concatenate(terms + [jnp.zeros((5, value.shape[1]), F32)], axis=0).astype(BF16)
        result = jnp.dot(terms, matrix, preferred_element_type=F32)
        return result[0:1] + result[1:2] + result[2:3]

    folded = jnp.concatenate(
        [both[:, :channels] + both[:, channels:] for both in (sums, squares)], axis=-1
    )
    mine[...] = product(folded, gather[...])
    @pl.when(z > 1)
    def _():
        pl.semaphore_wait(know_x, 2)
    def direct_to(z0, where):
        @pl.when(late & where)
        def _():
            pl.semaphore_wait(know_plane.at[z0], 1)
            for dx in (2, 1, 3, 0):
                for flip in (1, 0):
                    to = {"ha": (x + dx) % RING_X * RING_Z + z0, "ta": 1 - ta if flip else ta}
                    pltpu.make_async_remote_copy(
                        mine, direct_in.at[(last - z) * 8 + 2 * dx + flip], direct_send, direct_recv,
                        device_id=to, device_id_type=MESH,
                    ).start()

    direct_to(0, z >= last - 1)
    plane = []
    for dx in (2, 1, 3, 0):
        for flip in (0, 1):
            if dx or flip:
                slot = 2 * dx + flip - 1
                plane.append(
                    pltpu.make_async_remote_copy(
                        mine, plane_in.at[slot], plane_send, plane_recv,
                        device_id=near(dx, 0, bool(flip)), device_id_type=MESH,
                    )
                )
    for copy in plane:
        copy.start()
    direct_to(0, z < last - 1)
    direct_to(1, True)
    pass_first(lower & (z >= 4), True)
    each_token_arrival(lambda copy: copy.wait_recv(), False)
    patches(0, (0, 1))
    patches(2, (0, 1))
    hidden_rows(0, 0, 6)
    hidden_rows(3, 0, 6)
    hidden_rows(1, 0, 2)
    hidden_rows(2, 0, 2)
    for z0 in range(2, EARLY):
        direct_to(z0, True)
    total = mine[...]
    all_plane = pltpu.make_async_remote_copy(
        plane_in, plane_in, plane_send, plane_recv, device_id=near(0, 0, True), device_id_type=MESH
    )
    all_plane.wait_recv()
    for slot in range(plane_in.shape[0]):
        total = total + plane_in[slot]
    plane_sum[...] = total
    def ring_copy(d):
        return pltpu.make_async_remote_copy(
            plane_sum, ring_in.at[d - 1], ring_send, ring_recv,
            device_id=near(0, d, False), device_id_type=MESH,
        )

    def straight(d):
        return late & (z + d >= RING_Z) & (z + d < RING_Z + EARLY)

    for d in range(1, RING_Z):

        @pl.when(jnp.logical_not(straight(d)) & ((d == 1) | (z + d > RING_Z) | ((z == 1) & (d == last))))
        def _():
            ring_copy(d).start()

    pass_first(middle, z == RING_Z // 2)
    for d in range(2, last):

        @pl.when((lower | middle) & (z + d == RING_Z))
        def _():
            ring_copy(d).start()
    @pl.when(early)
    def _():
        transform(2)
    @pl.when((z > 1) & (z < last))
    def _():
        pl.semaphore_wait(know_all, 1)

    for z0 in range(2, EARLY):
        tell_plane(z0)
    for d in range(2, RING_Z):

        @pl.when((z + d <= last) | (jnp.logical_not(lower | middle | late) & (z + d == RING_Z)))
        def _():
            ring_copy(d).start()
    @pl.when(jnp.logical_not(early))
    def _():
        for p in range(3):
            transform(p)
    each_token_copy(lambda copy: copy.wait_send(), True)
    each_token_copy(lambda copy: copy.wait_send(), False)
    all_plane.wait_send()
    def ring_copies(number):
        return pltpu.make_async_remote_copy(
            ring_in.at[pl.ds(0, number)], ring_in.at[pl.ds(0, number)], ring_send, ring_recv,
            device_id=near(0, 1, False), device_id_type=MESH,
        )

    def direct_copies(number):
        return pltpu.make_async_remote_copy(
            direct_in.at[pl.ds(0, number)], direct_in.at[pl.ds(0, number)], direct_send, direct_recv,
            device_id=near(0, 1, False), device_id_type=MESH,
        )

    @pl.when(z < EARLY)
    def _():
        ring_copies(last - LATE).wait_recv()
    @pl.when(z < EARLY)
    def _():
        direct_copies(8 * LATE).wait_recv()

    @pl.when(z >= EARLY)
    def _():
        ring_copies(last).wait_recv()

    for slot in range(ring_in.shape[0]):
        total = total + ring_in[slot]
    rows = [direct_in[slot] for slot in range(8 * LATE)]
    while len(rows) > 1:
        rows = [sum(rows[at + 1 : at + 2], rows[at]) for at in range(0, len(rows), 2)]
    total = total + rows[0]
    count = n_ha * lax.axis_size("ta") * 4 * 2 * 2 * tokens * members
    shared = product(total * (1.0 / count), spread[...])
    mean, square = shared[:, :channels], shared[:, channels:]
    var = jnp.maximum(square - mean * mean, 0.0)
    scale = lax.rsqrt(var + EPS) * vectors[1].reshape(1, -1)
    stat_ref[0:1] = 0.5 * scale
    stat_ref[1:2] = 0.5 * (vectors[2].reshape(1, -1) - mean * scale)

    @pl.when(late)
    def _():
        ring_copies(last - EARLY).wait_send()
        direct_copies(8 * EARLY).wait_send()

    @pl.when(jnp.logical_not(late))
    def _():
        ring_copies(last).wait_send()


def decode_kernel(
    h_ref, stat_ref, main_ref, rest_ref, out_hbm,
    shifted, columns_wide, columns_rest, planes_wide, planes_rest, acc, rows_f32, out, out_sem,
):
    ha, ta = lax.axis_index("ha"), lax.axis_index("ta")
    n_ha = lax.axis_size("ha")
    frames_in, rows_in, pieces, tokens, _ = h_ref.shape
    parts = pieces // 2
    channels = 128 * parts
    frames, rows = frames_in - 2, rows_in - 2
    wide = main_ref.shape[2]
    rest = channels - wide
    for slot in (0, 1):
        for part in range(parts):
            for y in range(rows_in):
                shifted[slot, part, y, 0, 8 + tokens :] = jnp.zeros((8, 128), F32)
                shifted[slot, part, y, 1, :8] = jnp.zeros((8, 128), F32)

    def activate(f):
        for y in range(rows_in):
            inside = (ha * rows + y >= 1) & (ha * rows + y <= n_ha * rows)
            if f < 2:
                inside = inside & (ta > 0)
            for part in range(parts):
                lanes = slice(128 * part, 128 * part + 128)
                row_scale = jnp.where(inside, stat_ref[0:1, lanes], 0.0)
                row_shift = jnp.where(inside, stat_ref[1:2, lanes], 0.0)
                for b in (0, 1):
                    value = h_ref[f, y, b * parts + part] * row_scale + row_shift
                    shifted[f % 2, part, y, b, 8 : 8 + tokens] = value + value * jnp.tanh(value)

    def by_columns(f):
        for y in range(rows_in):
            by_part = []
            for part in range(parts):
                even, odd = [shifted[f % 2, part, y, b, 8 : 8 + tokens] for b in (0, 1)]
                before = shifted[f % 2, part, y, 1, 7 : 7 + tokens]
                after = shifted[f % 2, part, y, 0, 9 : 9 + tokens]
                by_part.append((before - odd, even + odd, odd - even, even - after))
            for k in range(4):
                value = jnp.concatenate([by_part[part][k] for part in range(wide // 128)], axis=-1)
                columns_wide[k, f, y] = value.astype(BF16)
                value = jnp.concatenate([by_part[part][k] for part in range(wide // 128, parts)], axis=-1)
                columns_rest[k, f, y] = value.astype(BF16)

    activate(0)
    for f in range(frames_in):
        if f + 1 < frames_in:
            activate(f + 1)
        by_columns(f)

    def by_rows(i, k):
        one, two = ((0, 2), (1, 2), (2, 1), (1, 3))[i]
        for columns, planes in ((columns_wide, planes_wide), (columns_rest, planes_rest)):
            if i == 1:
                planes[k % 2] = columns[k, :, one] + columns[k, :, two]
            else:
                planes[k % 2] = columns[k, :, one] - columns[k, :, two]

    by_rows(0, 0)
    bias = stat_ref[2:3]
    copies = []

    def finish(y):
        for f in range(frames):
            for part in range(parts):
                lanes = slice(128 * part, 128 * part + 128)
                for b in (0, 1):
                    hidden = h_ref[f + 2, y + 1, b * parts + part]
                    rows_f32[y, f, part, pl.ds(b, tokens, stride=2)] = acc[y, b, f, part] + (
                        hidden + bias[:, lanes]
                    )
                out[f, y, :, lanes] = rows_f32[y, f, part].astype(BF16)
            copies.append(pltpu.make_async_copy(out.at[f, y], out_hbm.at[f, y], out_sem.at[frames * y + f]))
            copies[-1].start()

    signs = ((1, 1, 1, 0), (0, 1, -1, -1))
    first = [[True, True], [True, True]]
    for i in range(4):
        for k in range(4):
            at = 4 * i + k
            if at < 15:
                by_rows((at + 1) // 4, (at + 1) % 4)
            both = (planes_wide.at[k % 2], planes_rest.at[k % 2])
            lhs = [planes[p : p + frames] for p in range(3) for planes in both]
            lhs = jnp.concatenate(lhs, axis=-1).reshape(frames * tokens, 3 * channels)
            product = jnp.dot(lhs, main_ref[at], preferred_element_type=F32)
            lhs = [
                jnp.concatenate([planes[t + p] for p in range(4) for planes in both], axis=-1)
                for t in range(0, frames, 2)
            ]
            other = jnp.dot(jnp.concatenate(lhs, axis=0), rest_ref[at], preferred_element_type=F32)
            for y in (0, 1):
                for b in (0, 1):
                    sign = signs[y][i] * signs[b][k]
                    if not sign:
                        continue
                    for f in range(frames):
                        for part in range(parts):
                            if 128 * part < wide:
                                value = product[f * tokens : (f + 1) * tokens, 128 * part : 128 * part + 128]
                            else:
                                value = other[
                                    f // 2 * tokens : (f // 2 + 1) * tokens,
                                    rest * (f % 2) : rest * (f % 2) + rest,
                                ]
                            if first[y][b]:
                                acc[y, b, f, part] = value if sign > 0 else -value
                            elif sign > 0:
                                acc[y, b, f, part] = acc[y, b, f, part] + value
                            else:
                                acc[y, b, f, part] = acc[y, b, f, part] - value
                    first[y][b] = False
        if i == 2:
            finish(0)
    finish(1)
    for y in (0, 1):
        for f in range(frames):
            copies[frames * y + f].wait()


def keep(value):
    return pltpu.with_memory_space_constraint(value, pltpu.HBM)


def body(latent_tokens, w_in, b_in, gn_gain, gn_shift, w_mid, b_mid):
    half = latent_tokens.shape[1]
    channels = w_in.shape[-1]
    tokens = 2 * half
    wide = channels // 256 * 256
    rest = channels - wide
    parts = channels // 128
    vmem = pl.BlockSpec(memory_space=pltpu.VMEM)
    hbm = pl.BlockSpec(memory_space=pltpu.HBM)
    inputs = (latent_tokens, w_in.reshape(3, 3, -1, channels), b_in, gn_gain, gn_shift, b_mid, w_mid)
    prepared = pl.pallas_call(
        exchange_kernel,
        out_shape=(
            jax.ShapeDtypeStruct((6, 4, 2 * parts, tokens, 128), F32),
            jax.ShapeDtypeStruct((3, channels), F32),
            jax.ShapeDtypeStruct((16, 3 * channels, wide), BF16),
            jax.ShapeDtypeStruct((16, 4 * channels, 2 * rest), BF16),
        ),
        in_specs=[hbm] * len(inputs),
        out_specs=(vmem, vmem, vmem, vmem),
        scratch_shapes=[
            pltpu.VMEM(latent_tokens.shape, BF16),
            pltpu.VMEM((4, channels), F32),
            pltpu.VMEM((2, 2, half, 128), BF16),
            pltpu.VMEM((3, 2, 2, tokens, 128), BF16),
            pltpu.VMEM((8, 3, tokens, 128), BF16),
            pltpu.VMEM((2, 3, 4, 64, 2 * channels), BF16),
            pltpu.VMEM(w_mid.shape, BF16),
            pltpu.VMEM((1, 128), F32),
            pltpu.VMEM((7, 1, 128), F32),
            pltpu.VMEM((1, 128), F32),
            pltpu.VMEM((RING_Z - 1, 1, 128), F32),
            pltpu.VMEM((8 * max(LATE, EARLY), 1, 128), F32),
            pltpu.VMEM((2 * 384, 4 * 128), BF16),
            pltpu.VMEM((2 * channels, 128), BF16),
            pltpu.VMEM((128, 2 * channels), BF16),
            pltpu.SemaphoreType.DMA,
            pltpu.SemaphoreType.DMA((4,)),
            pltpu.SemaphoreType.DMA((4,)),
            pltpu.SemaphoreType.DMA((3,)),
            pltpu.SemaphoreType.DMA((9,)),
            pltpu.SemaphoreType.DMA((3, 2)),
            pltpu.SemaphoreType.DMA((2, 2)),
            pltpu.SemaphoreType.DMA,
            pltpu.SemaphoreType.DMA,
            pltpu.SemaphoreType.DMA,
            pltpu.SemaphoreType.DMA,
            pltpu.SemaphoreType.DMA,
            pltpu.SemaphoreType.DMA,
            pltpu.SemaphoreType.REGULAR,
            pltpu.SemaphoreType.REGULAR,
            pltpu.SemaphoreType.REGULAR,
            pltpu.SemaphoreType.REGULAR((EARLY,)),
        ],
        compiler_params=pltpu.CompilerParams(
            collective_id=0, has_side_effects=True, vmem_limit_bytes=20 * 2**20
        ),
        name="exchange",
    )(*[keep(value) for value in inputs])
    return pl.pallas_call(
        decode_kernel,
        out_shape=jax.ShapeDtypeStruct((4, 2, 2 * tokens, channels), BF16),
        in_specs=[vmem, vmem, vmem, vmem],
        out_specs=hbm,
        scratch_shapes=[
            pltpu.VMEM((2, parts, 4, 2, tokens + 16, 128), F32),
            pltpu.VMEM((4, 6, 4, tokens, wide), BF16),
            pltpu.VMEM((4, 6, 4, tokens, rest), BF16),
            pltpu.VMEM((2, 6, tokens, wide), BF16),
            pltpu.VMEM((2, 6, tokens, rest), BF16),
            pltpu.VMEM((2, 2, 4, parts, tokens, 128), F32),
            pltpu.VMEM((2, 4, parts, 2 * tokens, 128), F32),
            pltpu.VMEM((4, 2, 2 * tokens, channels), BF16),
            pltpu.SemaphoreType.DMA((8,)),
        ],
        compiler_params=pltpu.CompilerParams(vmem_limit_bytes=20 * 2**20),
        name="decode",
    )(*prepared)


def solution(mesh):
    return jax.shard_map(
        body,
        mesh=mesh,
        in_specs=(P("clip", ("ha", "ta"), None), P(), P(), P(), P(), P(), P()),
        out_specs=P(("clip", "ta"), "ha", None, None),
        check_vma=False,
    )
```

```python
import jax
import jax.numpy as jnp
from jax import lax
from jax.experimental import pallas as pl
from jax.experimental.pallas import tpu as pltpu
from jax.sharding import PartitionSpec as P

GROUPS = 32
RING_X = 4
RING_Z = 16
LATE = 4
EARLY = 4
EPS = 1e-06
MESH = pl.DeviceIdType.MESH
BF16 = jnp.bfloat16
F32 = jnp.float32


def exchange_kernel(
    tok_hbm, w_hbm, b_hbm, gain_hbm, shift_hbm, b_mid_hbm, mid_hbm,
    h_ref, stat_ref, main_ref, rest_ref,
    tok, vectors, packed, field, patch, partial, w_big, mid, mine, plane_in, plane_sum, ring_in, direct_in,
    sel, gather, spread,
    tok_sem, vec_sem, w_sem, mid_sem, send_sem, recv_sem, later_sem,
    plane_send, plane_recv, ring_send, ring_recv, direct_send, direct_recv,
    know_x, know_all, know_first, know_plane,
):
    ha, ta = lax.axis_index("ha"), lax.axis_index("ta")
    n_ha = lax.axis_size("ha")
    x, z = ha // RING_Z, ha % RING_Z
    channels = vectors.shape[1]
    members = channels // GROUPS
    parts = channels // 128

    def near(dx, dz, flip):
        hx = (x + dx) % RING_X
        hz = (z + dz) % RING_Z
        return {"ha": hx * RING_Z + hz, "ta": 1 - ta if flip else ta}
    ring_in[...] = jnp.zeros_like(ring_in)
    direct_in[...] = jnp.zeros_like(direct_in)
    barrier = pltpu.get_barrier_semaphore()

    def greet(device):
        pl.semaphore_signal(barrier, inc=1, device_id=device, device_id_type=MESH)

    last = RING_Z - 1

    @pl.when(ha < n_ha - 1)
    def _():
        for t in (0, 1):
            greet({"ha": ha + 1, "ta": t})

    @pl.when(ha > 0)
    def _():
        for t in (0, 1):
            greet({"ha": ha - 1, "ta": t})

    for flip in (False, True):
        for dx in (1, RING_X - 1):
            greet(near(dx, 0, flip))
    greet(near(0, 0, True))

    @pl.when(z == 0)
    def _():
        greet(near(0, last, False))

    for d in range(2, last):

        @pl.when((z >= 1) & (z + d <= last))
        def _():
            greet(near(0, d, False))

    tok_copy = pltpu.make_async_copy(tok_hbm, tok, tok_sem)
    tok_copy.start()
    w_copies = [
        pltpu.make_async_copy(
            w_hbm,
            w_big.at[high, :, pl.ds(high, 3), pl.ds(16 * b, 48), pl.ds(channels * b, channels)],
            w_sem.at[2 * high + b],
        )
        for high in (0, 1)
        for b in (0, 1)
    ]
    for copy in w_copies:
        copy.start()
    vector_copies = [
        pltpu.make_async_copy(ref, vectors.at[i], vec_sem.at[i])
        for i, ref in enumerate((b_hbm, gain_hbm, shift_hbm, b_mid_hbm))
    ]
    for copy in vector_copies:
        copy.start()

    wide = main_ref.shape[2]
    rest = channels - wide

    def fetch(p):
        return pltpu.make_async_copy(mid_hbm.at[p], mid.at[p], mid_sem.at[p])

    for p in range(3):
        fetch(p).start()

    def bank(tap_0, tap_1, tap_2):
        ends = tap_0 + tap_2
        return tap_0, 0.5 * (ends + tap_1), 0.5 * (ends - tap_1), tap_2

    def transform(p):
        fetch(p).wait()

        def rows(step, carry):
            at = pl.multiple_of(step * 16, 16)
            for part in range(parts):
                lanes = slice(128 * part, 128 * part + 128)
                taps = [[mid[p, q, r, pl.ds(at, 16), lanes].astype(F32) for r in range(3)] for q in range(3)]
                by_row = [bank(*[taps[q][r] for q in range(3)]) for r in range(3)]
                for i in range(4):
                    for k, value in enumerate(bank(*[by_row[r][i] for r in range(3)])):
                        value = value.astype(BF16)
                        if 128 * part < wide:
                            main_ref[4 * i + k, pl.ds(at + p * channels, 16), lanes] = value
                        else:
                            rest_ref[4 * i + k, pl.ds(at + p * channels, 16), :rest] = value
                            rest_ref[4 * i + k, pl.ds(at + (p + 1) * channels, 16), rest:] = value
            return carry

        lax.fori_loop(0, channels // 16, rows, 0)

    early = z < 2
    lower = z < RING_Z // 2

    @pl.when(early)
    def _():
        transform(0)

    first = (ha == 0) & (ta == 0)

    @pl.when(early & jnp.logical_not(first))
    def _():
        transform(1)
    tok_copy.wait()
    lanes = tok.shape[2] // 2
    for a in (0, 1):
        for h in (0, 1):
            packed[a, h] = jnp.concatenate(
                [tok[4 * h + f, :, a * lanes : (a + 1) * lanes].astype(F32) for f in range(4)], axis=-1
            ).astype(BF16)
    half = packed.shape[2]
    own = pl.ds(ta * half, half)
    expected = (
        5
        + jnp.where(ha > 0, 2, 0)
        + jnp.where(ha < n_ha - 1, 2, 0)
        + jnp.maximum(z - 2, 0)
        + jnp.where(z == last, 1, 0)
    )
    pl.semaphore_wait(barrier, expected)
    def tokens_copy(place, a, src_ta, to_ha, to_ta, slot, urgent):
        there = pl.ds(src_ta * half, half)
        frames = pl.ds(0, 2) if to_ta else pl.ds(1, 1)
        of = pl.ds(0, 2) if to_ta else pl.ds(0, 1)
        if a is None:
            src, dst = packed.at[:, of], field.at[place, :, frames, there]
        else:
            src, dst = packed.at[a, of], field.at[place, a, frames, there]
        sem = recv_sem.at[place, src_ta] if urgent else later_sem.at[place // 2, src_ta]
        return pltpu.make_async_remote_copy(
            src, dst, send_sem.at[slot], sem, device_id={"ha": to_ha, "ta": to_ta}, device_id_type=MESH
        )

    def each_token_copy(act, urgent):
        @pl.when(ha < n_ha - 1)
        def _():
            for t in (1, 0):
                act(tokens_copy(0, int(urgent), ta, ha + 1, t, 2 * (1 - int(urgent)) + t, urgent))

        @pl.when(ha > 0)
        def _():
            for t in (1, 0):
                act(tokens_copy(2, 1 - int(urgent), ta, ha - 1, t, 4 + 2 * (1 - int(urgent)) + t, urgent))

        if urgent:
            for t in (1, 0):

                @pl.when(ta == 1 - t)
                def _():
                    act(tokens_copy(1, None, ta, ha, t, 8, True))

    def each_token_arrival(act, urgent):
        for to_ta in (0, 1):

            @pl.when(ta == to_ta)
            def _():
                if urgent is None:
                    act(tokens_copy(1, None, 1 - to_ta, ha, to_ta, 8, True))
                    return

                @pl.when(ha > 0)
                def _():
                    for t in (0, 1):
                        act(tokens_copy(0, int(urgent), t, ha, to_ta, 0, urgent))

                @pl.when(ha < n_ha - 1)
                def _():
                    for t in (0, 1):
                        act(tokens_copy(2, 1 - int(urgent), t, ha, to_ta, 0, urgent))

    def tell(sem, device):
        pl.semaphore_signal(sem, inc=1, device_id=device, device_id_type=MESH)

    @pl.when(z == last)
    def _():
        for d in range(1, 1 + EARLY):
            tell(know_all, near(0, d, False))

    each_token_copy(lambda copy: copy.start(), True)

    tell(know_x, near(1, 0, False))
    tell(know_x, near(RING_X - 1, 0, False))

    def pass_first(where, onwards):
        @pl.when(where)
        def _():
            pl.semaphore_wait(know_first, 1)

        @pl.when(where & onwards)
        def _():
            tell(know_first, near(0, 1, False))

    @pl.when(z == 1)
    def _():
        tell(know_first, near(0, 1, False))

    middle = (z == RING_Z // 2) | (z == RING_Z // 2 + 1)

    @pl.when(z == last)
    def _():
        for d in range(1 + EARLY, RING_Z):
            tell(know_all, near(0, d, False))
    @pl.when(ta == 0)
    def _():
        field[:, :, 0] = jnp.zeros_like(field[:, :, 0])
        field[1, :, 1, own] = packed[:, 0]

    @pl.when(ta == 1)
    def _():
        field[1, :, :, own] = packed[...]

    @pl.when(ha == 0)
    def _():
        field[0] = jnp.zeros_like(field[0])

    @pl.when(ha == n_ha - 1)
    def _():
        field[2] = jnp.zeros_like(field[2])

    for high in (0, 1):
        w_big[high, :, 3 * (1 - high)] = jnp.zeros_like(w_big[high, :, 0])
        for p in range(3):
            for q in range(3):
                w_big[high, p, high + q, 48:64, :channels] = jnp.zeros((16, channels), BF16)
                w_big[high, p, high + q, 0:16, channels:] = jnp.zeros((16, channels), BF16)
    for i in range(16):
        rest_ref[i, 3 * channels :, :rest] = jnp.zeros((channels, rest), BF16)
        rest_ref[i, :channels, rest:] = jnp.zeros((channels, rest), BF16)
    sel[...] = jnp.zeros_like(sel)
    k = lax.broadcasted_iota(jnp.int32, (lanes, 128), 0)
    n = lax.broadcasted_iota(jnp.int32, (lanes, 128), 1)
    for a in (0, 1):
        for step in range(3):
            column = 2 * step + k // 16 - 1
            block = (n // 64 == a) & (k % 16 == n % 16) & ((n // 16) % 4 == column)
            block = jnp.where(block, 1.0, 0.0).astype(BF16)
            for f in range(4):
                sel[384 * a + 128 * step + lanes * f : 384 * a + 128 * step + lanes * (f + 1), 128 * f : 128 * f + 128] = block
    k = lax.broadcasted_iota(jnp.int32, gather.shape, 0)
    n = lax.broadcasted_iota(jnp.int32, gather.shape, 1)
    gather[...] = jnp.where((k // members == n) & (n < 2 * GROUPS), 1.0, 0.0).astype(BF16)
    k = lax.broadcasted_iota(jnp.int32, spread.shape, 0)
    n = lax.broadcasted_iota(jnp.int32, spread.shape, 1)
    spread[...] = jnp.where((n // members == k) & (k < 2 * GROUPS), 1.0, 0.0).astype(BF16)
    for copy in vector_copies:
        copy.wait()
    stat_ref[2:3] = vectors[3].reshape(1, -1)
    for copy in w_copies:
        copy.wait()
    each_token_copy(lambda copy: copy.start(), False)

    @pl.when(first)
    def _():
        transform(1)
    late = z >= RING_Z - LATE

    def tell_plane(z0):
        @pl.when(z == z0)
        def _():
            for to in range(RING_Z - LATE, RING_Z):
                tell(know_plane.at[z0], {"ha": x * RING_Z + to, "ta": ta})

    @pl.when(z <= 1)
    def _():
        pl.semaphore_wait(know_x, 2)
        pl.semaphore_wait(know_all, 1)

    tell_plane(0)
    tell_plane(1)
    pass_first((z == 2) | (z == 3), True)
    each_token_arrival(lambda copy: copy.wait_recv(), None)
    tokens = field.shape[3]
    row = lax.broadcasted_iota(jnp.int32, (tokens, 128), 0)

    def patches(i, sides):
        stack = []
        for h in (0, 1):
            pieces = []
            for a in sides:
                now = field[i, a, h].astype(F32)
                pieces.append(jnp.where(row == 0, 0.0, pltpu.roll(now, 1, 0)))
                pieces.append(now)
                pieces.append(jnp.where(row == tokens - 1, 0.0, pltpu.roll(now, tokens - 1, 0)))
            stack.append(jnp.concatenate(pieces, axis=-1).astype(BF16))
        chosen = sel[384 * sides[0] : 384 * (sides[-1] + 1)]
        moved = jnp.dot(jnp.concatenate(stack, axis=0), chosen, preferred_element_type=F32).astype(BF16)
        for h in (0, 1):
            for f in range(4):
                patch[4 * h + f, i] = moved[h * tokens : (h + 1) * tokens, 128 * f : 128 * f + 128]

    bias = vectors[0].reshape(1, -1)
    bias = jnp.concatenate([bias, bias], axis=-1)

    def keep_hidden(y, first, frames, total):
        for n in range(2 * parts):
            part = total[:, 128 * n : 128 * n + 128].astype(BF16).astype(F32)
            h_ref[first : first + frames, y, n] = part.reshape(frames, tokens, 128)

    def hidden_rows(y, first, frames):
        low, high = y // 2, y % 2
        total = bias
        for p in range(3):
            lhs = [
                patch[first + p : first + p + frames, i].reshape(frames * tokens, 128) for i in (low, low + 1)
            ]
            lhs = jnp.concatenate(lhs, axis=-1)
            total = total + jnp.dot(
                lhs, w_big[high, p].reshape(256, 2 * channels), preferred_element_type=F32
            )
        keep_hidden(y, first, frames, total)

    def part_of_own(y, i, start):
        low, high = y // 2, y % 2
        taps = [
            (
                patch[2 + p : 6 + p, i].reshape(4 * tokens, 128),
                w_big[high, p, 2 * (i - low) : 2 * (i - low) + 2].reshape(128, 2 * channels),
            )
            for p in range(3)
        ]
        lhs = jnp.concatenate([taps[0][0], taps[1][0]], axis=-1)
        rhs = jnp.concatenate([taps[0][1], taps[1][1]], axis=0)
        total = start + jnp.dot(lhs, rhs, preferred_element_type=F32)
        return total + jnp.dot(*taps[2], preferred_element_type=F32)

    patches(1, (0, 1))
    for y in (1, 2):
        partial[y - 1] = part_of_own(y, 1, bias)
    each_token_arrival(lambda copy: copy.wait_recv(), True)
    patches(0, (1,))
    patches(2, (0,))
    sums = jnp.zeros((1, 2 * channels), F32)
    squares = jnp.zeros((1, 2 * channels), F32)
    for y in (1, 2):
        values = part_of_own(y, 2 * (y - 1), partial[y - 1])
        keep_hidden(y, 2, 4, values)
        sums = sums + jnp.sum(values, axis=0, keepdims=True)
        squares = squares + jnp.sum(values * values, axis=0, keepdims=True)
    def product(value, matrix):
        terms = []
        for _ in range(3):
            term = value.astype(BF16)
            terms.append(term.astype(F32))
            value = value - terms[-1]
        terms = jnp.concatenate(terms + [jnp.zeros((5, value.shape[1]), F32)], axis=0).astype(BF16)
        result = jnp.dot(terms, matrix, preferred_element_type=F32)
        return result[0:1] + result[1:2] + result[2:3]

    folded = jnp.concatenate(
        [both[:, :channels] + both[:, channels:] for both in (sums, squares)], axis=-1
    )
    mine[...] = product(folded, gather[...])
    @pl.when(z > 1)
    def _():
        pl.semaphore_wait(know_x, 2)
    def direct_to(z0, where):
        @pl.when(late & where)
        def _():
            pl.semaphore_wait(know_plane.at[z0], 1)
            for dx in (2, 1, 3, 0):
                for flip in (1, 0):
                    to = {"ha": (x + dx) % RING_X * RING_Z + z0, "ta": 1 - ta if flip else ta}
                    pltpu.make_async_remote_copy(
                        mine, direct_in.at[(last - z) * 8 + 2 * dx + flip], direct_send, direct_recv,
                        device_id=to, device_id_type=MESH,
                    ).start()

    direct_to(0, z >= last - 1)
    plane = []
    for dx in (2, 1, 3, 0):
        for flip in (0, 1):
            if dx or flip:
                slot = 2 * dx + flip - 1
                plane.append(
                    pltpu.make_async_remote_copy(
                        mine, plane_in.at[slot], plane_send, plane_recv,
                        device_id=near(dx, 0, bool(flip)), device_id_type=MESH,
                    )
                )
    for copy in plane:
        copy.start()
    direct_to(0, z < last - 1)
    direct_to(1, True)
    pass_first(lower & (z >= 4), True)
    each_token_arrival(lambda copy: copy.wait_recv(), False)
    patches(0, (0, 1))
    patches(2, (0, 1))
    hidden_rows(0, 0, 6)
    direct_to(2, True)
    hidden_rows(3, 0, 6)
    hidden_rows(1, 0, 2)
    hidden_rows(2, 0, 2)
    for z0 in range(3, EARLY):
        direct_to(z0, True)
    total = mine[...]
    all_plane = pltpu.make_async_remote_copy(
        plane_in, plane_in, plane_send, plane_recv, device_id=near(0, 0, True), device_id_type=MESH
    )
    all_plane.wait_recv()
    for slot in range(plane_in.shape[0]):
        total = total + plane_in[slot]
    plane_sum[...] = total
    def ring_copy(d):
        return pltpu.make_async_remote_copy(
            plane_sum, ring_in.at[d - 1], ring_send, ring_recv,
            device_id=near(0, d, False), device_id_type=MESH,
        )

    def straight(d):
        return late & (z + d >= RING_Z) & (z + d < RING_Z + EARLY)

    pass_first(middle, z == RING_Z // 2)
    upper = (z > RING_Z // 2 + 1) & jnp.logical_not(late)

    @pl.when(upper)
    def _():
        pl.semaphore_wait(know_all, 1)

    for d in (*range(5, RING_Z), *range(1, 5)):

        @pl.when(jnp.logical_not(straight(d)) & ((d == 1) | (z + d >= RING_Z)))
        def _():
            ring_copy(d).start()
    @pl.when(early)
    def _():
        transform(2)
    @pl.when((z > 1) & (z < last) & jnp.logical_not(upper))
    def _():
        pl.semaphore_wait(know_all, 1)

    for z0 in range(2, EARLY):
        tell_plane(z0)
    for d in range(2, RING_Z):

        @pl.when(z + d <= last)
        def _():
            ring_copy(d).start()
    @pl.when(jnp.logical_not(early))
    def _():
        for p in range(3):
            transform(p)
    each_token_copy(lambda copy: copy.wait_send(), True)
    each_token_copy(lambda copy: copy.wait_send(), False)
    all_plane.wait_send()
    def ring_copies(number):
        return pltpu.make_async_remote_copy(
            ring_in.at[pl.ds(0, number)], ring_in.at[pl.ds(0, number)], ring_send, ring_recv,
            device_id=near(0, 1, False), device_id_type=MESH,
        )

    def direct_copies(number):
        return pltpu.make_async_remote_copy(
            direct_in.at[pl.ds(0, number)], direct_in.at[pl.ds(0, number)], direct_send, direct_recv,
            device_id=near(0, 1, False), device_id_type=MESH,
        )

    @pl.when(z < EARLY)
    def _():
        ring_copies(last - LATE).wait_recv()
    @pl.when(z < EARLY)
    def _():
        direct_copies(8 * LATE).wait_recv()

    @pl.when(z >= EARLY)
    def _():
        ring_copies(last).wait_recv()

    for slot in range(ring_in.shape[0]):
        total = total + ring_in[slot]
    rows = [direct_in[slot] for slot in range(8 * LATE)]
    while len(rows) > 1:
        rows = [sum(rows[at + 1 : at + 2], rows[at]) for at in range(0, len(rows), 2)]
    total = total + rows[0]
    count = n_ha * lax.axis_size("ta") * 4 * 2 * 2 * tokens * members
    shared = product(total * (1.0 / count), spread[...])
    mean, square = shared[:, :channels], shared[:, channels:]
    var = jnp.maximum(square - mean * mean, 0.0)
    scale = lax.rsqrt(var + EPS) * vectors[1].reshape(1, -1)
    stat_ref[0:1] = 0.5 * scale
    stat_ref[1:2] = 0.5 * (vectors[2].reshape(1, -1) - mean * scale)

    @pl.when(late)
    def _():
        ring_copies(last - EARLY).wait_send()
        direct_copies(8 * EARLY).wait_send()

    @pl.when(jnp.logical_not(late))
    def _():
        ring_copies(last).wait_send()


def decode_kernel(
    h_ref, stat_ref, main_ref, rest_ref, out_hbm,
    shifted, columns_wide, columns_rest, planes_wide, planes_rest, products, total, rows_f32, out, out_sem,
):
    ha, ta = lax.axis_index("ha"), lax.axis_index("ta")
    n_ha = lax.axis_size("ha")
    frames_in, rows_in, pieces, tokens, _ = h_ref.shape
    parts = pieces // 2
    channels = 128 * parts
    frames, rows = frames_in - 2, rows_in - 2
    wide = main_ref.shape[2]
    rest = channels - wide
    for f in range(frames_in):
        for part in range(parts):
            for y in range(rows_in):
                shifted[f, part, y, 0, 8 + tokens :] = jnp.zeros((8, 128), F32)
                shifted[f, part, y, 1, :8] = jnp.zeros((8, 128), F32)

    held = {}

    def activate(y, b):
        later = held.get("product", 0.0)
        for f in range(frames_in):
            inside = (ha * rows + y >= 1) & (ha * rows + y <= n_ha * rows)
            if f < 2:
                inside = inside & (ta > 0)
            for part in range(parts):
                lanes = slice(128 * part, 128 * part + 128)
                row_scale = jnp.where(inside, stat_ref[0:1, lanes], 0.0) + later
                row_shift = jnp.where(inside, stat_ref[1:2, lanes], 0.0)
                value = h_ref[f, y, b * parts + part] * row_scale + row_shift
                shifted[f, part, y, b, 8 : 8 + tokens] = value + value * jnp.tanh(value)

    def by_columns(y, k):
        def one(f, part):
            even, odd = [shifted.at[f, part, y, b] for b in (0, 1)]
            if k == 0:
                return odd[7 : 7 + tokens] - odd[8 : 8 + tokens]
            if k == 1:
                return even[8 : 8 + tokens] + odd[8 : 8 + tokens]
            if k == 2:
                return odd[8 : 8 + tokens] - even[8 : 8 + tokens]
            return even[8 : 8 + tokens] - even[9 : 9 + tokens]

        for f in range(frames_in):
            value = jnp.concatenate([one(f, part) for part in range(wide // 128)], axis=-1)
            columns_wide[k, f, y] = value.astype(BF16)
            value = jnp.concatenate([one(f, part) for part in range(wide // 128, parts)], axis=-1)
            columns_rest[k, f, y] = value.astype(BF16)

    def by_rows(i, k):
        one, two = ((0, 2), (1, 2), (2, 1), (1, 3))[i]
        for columns, planes in ((columns_wide, planes_wide), (columns_rest, planes_rest)):
            if i == 1:
                planes[k % 2] = columns[k, :, one] + columns[k, :, two]
            else:
                planes[k % 2] = columns[k, :, one] - columns[k, :, two]

    ahead = {
        0: [(activate, 0, 0), (activate, 2, 0), (by_columns, 0, 1), (by_columns, 2, 1)],
        1: [(by_columns, 0, 2), (by_columns, 2, 2), (activate, 1, 1)],
        2: [(by_columns, 0, 3), (by_columns, 2, 3), (activate, 1, 0)],
        3: [(by_columns, 1, 0), (by_columns, 1, 1)],
        4: [(by_columns, 1, 2), (by_columns, 1, 3)],
        5: [(activate, 3, 1)],
        6: [(activate, 3, 0)],
        7: [(by_columns, 3, 0)],
        8: [(by_columns, 3, 1)],
        9: [(by_columns, 3, 2)],
        10: [(by_columns, 3, 3)],
    }
    for y in (0, 2):
        activate(y, 1)
    for y in (0, 2):
        by_columns(y, 0)
    by_rows(0, 0)
    bias = stat_ref[2:3]
    copies = []

    def done(y, b, f, part, value):
        hidden = h_ref[f + 2, y + 1, b * parts + part] + bias[:, 128 * part : 128 * part + 128]
        rows_f32[y, f, part, pl.ds(b, tokens, stride=2)] = value + hidden

    def send(y, f):
        for part in range(parts):
            out[f, y, :, 128 * part : 128 * part + 128] = rows_f32[y, f, part].astype(BF16)
        copies.append(pltpu.make_async_copy(out.at[f, y], out_hbm.at[f, y], out_sem.at[frames * y + f]))
        copies[-1].start()

    def combine(i, f):
        for part in range(parts):
            m0, m1, m2, m3 = [products[i % 2, k, f, part] for k in range(4)]
            for b, value in ((0, m0 + m1 + m2), (1, m1 - m2 - m3)):
                if i == 0:
                    total[0, b, f, part] = value
                elif i == 1:
                    total[0, b, f, part] = total[0, b, f, part] + value
                    total[1, b, f, part] = value
                elif i == 2:
                    done(0, b, f, part, total[0, b, f, part] + value)
                    total[1, b, f, part] = total[1, b, f, part] - value
        if i == 2:
            send(0, f)

    def last_even(f):
        for part in range(parts):
            m0, m1, m2 = [products[1, k, f, part] for k in range(3)]
            done(1, 0, f, part, total[1, 0, f, part] - (m0 + m1 + m2))
            total[1, 1, f, part] = total[1, 1, f, part] - (m1 - m2)

    def last_odd(f):
        for part in range(parts):
            done(1, 1, f, part, total[1, 1, f, part] + products[1, 3, f, part])
        send(1, f)

    for i in range(4):
        for k in range(4):
            at = 4 * i + k
            for make, one, two in ahead.get(at, ()):
                make(one, two)
            if at < 15:
                by_rows((at + 1) // 4, (at + 1) % 4)
            if i and k < 2:
                combine(i - 1, 2 * k)
                combine(i - 1, 2 * k + 1)
            if at == 15:
                for f in range(frames):
                    last_even(f)
            both = (planes_wide.at[k % 2], planes_rest.at[k % 2])
            lhs = [planes[p : p + frames] for p in range(3) for planes in both]
            lhs = jnp.concatenate(lhs, axis=-1).reshape(frames * tokens, 3 * channels)
            product = jnp.dot(lhs, main_ref[at], preferred_element_type=F32)
            held["product"] = 0.0 * product[0:1, 0:128]
            for part in range(wide // 128):
                products[i % 2, k, :, part] = product[:, 128 * part : 128 * part + 128].reshape(frames, tokens, 128)
            lhs = [
                jnp.concatenate([planes[t + p] for p in range(4) for planes in both], axis=-1)
                for t in range(0, frames, 2)
            ]
            product = jnp.dot(jnp.concatenate(lhs, axis=0), rest_ref[at], preferred_element_type=F32)
            for f in range(frames):
                products[i % 2, k, f, wide // 128] = product[
                    f // 2 * tokens : (f // 2 + 1) * tokens, rest * (f % 2) : rest * (f % 2) + rest
                ]
    for f in range(frames):
        last_odd(f)
    for copy in copies:
        copy.wait()


def keep(value):
    return pltpu.with_memory_space_constraint(value, pltpu.HBM)


def body(latent_tokens, w_in, b_in, gn_gain, gn_shift, w_mid, b_mid):
    half = latent_tokens.shape[1]
    channels = w_in.shape[-1]
    tokens = 2 * half
    wide = channels // 256 * 256
    rest = channels - wide
    parts = channels // 128
    vmem = pl.BlockSpec(memory_space=pltpu.VMEM)
    hbm = pl.BlockSpec(memory_space=pltpu.HBM)
    inputs = (latent_tokens, w_in.reshape(3, 3, -1, channels), b_in, gn_gain, gn_shift, b_mid, w_mid)
    prepared = pl.pallas_call(
        exchange_kernel,
        out_shape=(
            jax.ShapeDtypeStruct((6, 4, 2 * parts, tokens, 128), F32),
            jax.ShapeDtypeStruct((3, channels), F32),
            jax.ShapeDtypeStruct((16, 3 * channels, wide), BF16),
            jax.ShapeDtypeStruct((16, 4 * channels, 2 * rest), BF16),
        ),
        in_specs=[hbm] * len(inputs),
        out_specs=(vmem, vmem, vmem, vmem),
        scratch_shapes=[
            pltpu.VMEM(latent_tokens.shape, BF16),
            pltpu.VMEM((4, channels), F32),
            pltpu.VMEM((2, 2, half, 128), BF16),
            pltpu.VMEM((3, 2, 2, tokens, 128), BF16),
            pltpu.VMEM((8, 3, tokens, 128), BF16),
            pltpu.VMEM((2, 4 * tokens, 2 * channels), F32),
            pltpu.VMEM((2, 3, 4, 64, 2 * channels), BF16),
            pltpu.VMEM(w_mid.shape, BF16),
            pltpu.VMEM((1, 128), F32),
            pltpu.VMEM((7, 1, 128), F32),
            pltpu.VMEM((1, 128), F32),
            pltpu.VMEM((RING_Z - 1, 1, 128), F32),
            pltpu.VMEM((8 * max(LATE, EARLY), 1, 128), F32),
            pltpu.VMEM((2 * 384, 4 * 128), BF16),
            pltpu.VMEM((2 * channels, 128), BF16),
            pltpu.VMEM((128, 2 * channels), BF16),
            pltpu.SemaphoreType.DMA,
            pltpu.SemaphoreType.DMA((4,)),
            pltpu.SemaphoreType.DMA((4,)),
            pltpu.SemaphoreType.DMA((3,)),
            pltpu.SemaphoreType.DMA((9,)),
            pltpu.SemaphoreType.DMA((3, 2)),
            pltpu.SemaphoreType.DMA((2, 2)),
            pltpu.SemaphoreType.DMA,
            pltpu.SemaphoreType.DMA,
            pltpu.SemaphoreType.DMA,
            pltpu.SemaphoreType.DMA,
            pltpu.SemaphoreType.DMA,
            pltpu.SemaphoreType.DMA,
            pltpu.SemaphoreType.REGULAR,
            pltpu.SemaphoreType.REGULAR,
            pltpu.SemaphoreType.REGULAR,
            pltpu.SemaphoreType.REGULAR((EARLY,)),
        ],
        compiler_params=pltpu.CompilerParams(
            collective_id=0, has_side_effects=True, vmem_limit_bytes=20 * 2**20
        ),
        name="exchange",
    )(*[keep(value) for value in inputs])
    return pl.pallas_call(
        decode_kernel,
        out_shape=jax.ShapeDtypeStruct((4, 2, 2 * tokens, channels), BF16),
        in_specs=[vmem, vmem, vmem, vmem],
        out_specs=hbm,
        scratch_shapes=[
            pltpu.VMEM((6, parts, 4, 2, tokens + 16, 128), F32),
            pltpu.VMEM((4, 6, 4, tokens, wide), BF16),
            pltpu.VMEM((4, 6, 4, tokens, rest), BF16),
            pltpu.VMEM((2, 6, tokens, wide), BF16),
            pltpu.VMEM((2, 6, tokens, rest), BF16),
            pltpu.VMEM((2, 4, 4, parts, tokens, 128), F32),
            pltpu.VMEM((2, 2, 4, parts, tokens, 128), F32),
            pltpu.VMEM((2, 4, parts, 2 * tokens, 128), F32),
            pltpu.VMEM((4, 2, 2 * tokens, channels), BF16),
            pltpu.SemaphoreType.DMA((8,)),
        ],
        compiler_params=pltpu.CompilerParams(vmem_limit_bytes=28 * 2**20),
        name="decode",
    )(*prepared)


def solution(mesh):
    return jax.shard_map(
        body,
        mesh=mesh,
        in_specs=(P("clip", ("ha", "ta"), None), P(), P(), P(), P(), P(), P()),
        out_specs=P(("clip", "ta"), "ha", None, None),
        check_vma=False,
    )
```

```python
import jax
import jax.numpy as jnp
from jax import lax
from jax.experimental import pallas as pl
from jax.experimental.pallas import tpu as pltpu
from jax.sharding import PartitionSpec as P

GROUPS = 32
RING_X = 4
RING_Z = 16
LATE = 4
EARLY = 4
EPS = 1e-06
MESH = pl.DeviceIdType.MESH
BF16 = jnp.bfloat16
F32 = jnp.float32


def exchange_kernel(
    tok_hbm, w_hbm, b_hbm, gain_hbm, shift_hbm, b_mid_hbm, mid_hbm,
    h_ref, stat_ref, main_ref, rest_ref,
    tok, vectors, packed, field, patch, partial, w_big, mid, mine, plane_in, plane_sum, ring_in, direct_in,
    sel, gather, spread,
    tok_sem, vec_sem, w_sem, mid_sem, send_sem, recv_sem,
    plane_send, plane_recv, ring_send, ring_recv, direct_send, direct_recv,
    know_x, know_all, know_first, know_plane,
):
    ha, ta = lax.axis_index("ha"), lax.axis_index("ta")
    n_ha = lax.axis_size("ha")
    x, z = ha // RING_Z, ha % RING_Z
    channels = vectors.shape[1]
    members = channels // GROUPS
    parts = channels // 128

    def near(dx, dz, flip):
        hx = (x + dx) % RING_X
        hz = (z + dz) % RING_Z
        return {"ha": hx * RING_Z + hz, "ta": 1 - ta if flip else ta}
    ring_in[...] = jnp.zeros_like(ring_in)
    direct_in[...] = jnp.zeros_like(direct_in)
    barrier = pltpu.get_barrier_semaphore()

    def greet(device):
        pl.semaphore_signal(barrier, inc=1, device_id=device, device_id_type=MESH)

    last = RING_Z - 1

    @pl.when(ha < n_ha - 1)
    def _():
        for t in (0, 1):
            greet({"ha": ha + 1, "ta": t})

    @pl.when(ha > 0)
    def _():
        for t in (0, 1):
            greet({"ha": ha - 1, "ta": t})

    for flip in (False, True):
        for dx in (1, RING_X - 1):
            greet(near(dx, 0, flip))
    greet(near(0, 0, True))

    @pl.when(z == 0)
    def _():
        greet(near(0, last, False))

    for d in range(2, last):

        @pl.when((z >= 1) & (z + d <= last))
        def _():
            greet(near(0, d, False))

    tok_copy = pltpu.make_async_copy(tok_hbm, tok, tok_sem)
    tok_copy.start()
    w_copies = [
        pltpu.make_async_copy(
            w_hbm,
            w_big.at[high, :, pl.ds(high, 3), pl.ds(16 * b, 48), pl.ds(channels * b, channels)],
            w_sem,
        )
        for high in (0, 1)
        for b in (0, 1)
    ]
    for copy in w_copies:
        copy.start()
    vector_copies = [
        pltpu.make_async_copy(ref, vectors.at[i], vec_sem)
        for i, ref in enumerate((b_hbm, gain_hbm, shift_hbm, b_mid_hbm))
    ]
    for copy in vector_copies:
        copy.start()

    wide = main_ref.shape[2]
    rest = channels - wide

    def fetch(p):
        return pltpu.make_async_copy(mid_hbm.at[p], mid.at[p], mid_sem.at[p])

    for p in range(3):
        fetch(p).start()

    def bank(tap_0, tap_1, tap_2):
        ends = tap_0 + tap_2
        return tap_0, 0.5 * (ends + tap_1), 0.5 * (ends - tap_1), tap_2

    def transform(p):
        fetch(p).wait()

        def rows(step, carry):
            at = pl.multiple_of(step * 16, 16)
            for part in range(parts):
                lanes = slice(128 * part, 128 * part + 128)
                taps = [[mid[p, q, r, pl.ds(at, 16), lanes].astype(F32) for r in range(3)] for q in range(3)]
                by_row = [bank(*[taps[q][r] for q in range(3)]) for r in range(3)]
                for i in range(4):
                    for k, value in enumerate(bank(*[by_row[r][i] for r in range(3)])):
                        value = value.astype(BF16)
                        if 128 * part < wide:
                            main_ref[4 * i + k, pl.ds(at + p * channels, 16), lanes] = value
                        else:
                            rest_ref[4 * i + k, pl.ds(at + p * channels, 16), :rest] = value
                            rest_ref[4 * i + k, pl.ds(at + (p + 1) * channels, 16), rest:] = value
            return carry

        lax.fori_loop(0, channels // 16, rows, 0)

    early = z < 2
    lower = z < RING_Z // 2

    @pl.when(early)
    def _():
        transform(0)

    first = (ha == 0) & (ta == 0)

    @pl.when(early & jnp.logical_not(first))
    def _():
        transform(1)
    tok_copy.wait()
    lanes = tok.shape[2] // 2
    for a in (0, 1):
        for h in (0, 1):
            packed[a, h] = jnp.concatenate(
                [tok[4 * h + f, :, a * lanes : (a + 1) * lanes].astype(F32) for f in range(4)], axis=-1
            ).astype(BF16)
    half = packed.shape[2]
    own = pl.ds(ta * half, half)
    expected = (
        5
        + jnp.where(ha > 0, 2, 0)
        + jnp.where(ha < n_ha - 1, 2, 0)
        + jnp.maximum(z - 2, 0)
        + jnp.where(z == last, 1, 0)
    )
    pl.semaphore_wait(barrier, expected)
    def tokens_copy(place, a, to_ha, to_ta, send, arrival):
        frames = pl.ds(0, 2) if to_ta else pl.ds(1, 1)
        of = pl.ds(0, 2) if to_ta else pl.ds(0, 1)
        if a is None:
            src, dst = packed.at[:, of], field.at[place, :, frames, own]
        else:
            src, dst = packed.at[a, of], field.at[place, a, frames, own]
        return pltpu.make_async_remote_copy(
            src, dst, send_sem.at[send], recv_sem.at[arrival],
            device_id={"ha": to_ha, "ta": to_ta}, device_id_type=MESH,
        )

    def send_tokens(urgent):
        @pl.when(ha < n_ha - 1)
        def _():
            for t in (1, 0):
                tokens_copy(0, int(urgent), ha + 1, t, 0 if urgent else 3, 0 if urgent else 3).start()

        @pl.when(ha > 0)
        def _():
            for t in (1, 0):
                tokens_copy(2, 1 - int(urgent), ha - 1, t, 1 if urgent else 4, 2 if urgent else 4).start()

        if urgent:
            for t in (1, 0):

                @pl.when(ta == 1 - t)
                def _():
                    tokens_copy(1, None, ha, t, 2, 1).start()

    def await_tokens(urgent):
        for to_ta in (0, 1):
            frames = pl.ds(0, 2) if to_ta else pl.ds(1, 1)

            def arrived(ref, arrival):
                pltpu.make_async_remote_copy(
                    ref, ref, send_sem.at[2], recv_sem.at[arrival],
                    device_id={"ha": ha, "ta": 1 - ta}, device_id_type=MESH,
                ).wait_recv()

            @pl.when(ta == to_ta)
            def _():
                if urgent is None:
                    arrived(field.at[1, :, frames, pl.ds((1 - to_ta) * half, half)], 1)
                    return

                @pl.when(ha > 0)
                def _():
                    arrived(field.at[0, int(urgent), frames], 0 if urgent else 3)

                @pl.when(ha < n_ha - 1)
                def _():
                    arrived(field.at[2, 1 - int(urgent), frames], 2 if urgent else 4)

    def tokens_left():
        three = field.at[pl.ds(0, 3), 0, 0, pl.ds(0, half)]

        def left(ref, send):
            pltpu.make_async_remote_copy(
                ref, ref, send_sem.at[send], recv_sem.at[1],
                device_id={"ha": ha, "ta": 1 - ta}, device_id_type=MESH,
            ).wait_send()

        @pl.when(ha < n_ha - 1)
        def _():
            left(three, 0)
            left(three, 3)

        @pl.when(ha > 0)
        def _():
            left(three, 1)
            left(three, 4)

        for t in (1, 0):

            @pl.when(ta == 1 - t)
            def _():
                tokens_copy(1, None, ha, t, 2, 1).wait_send()

    def tell(sem, device):
        pl.semaphore_signal(sem, inc=1, device_id=device, device_id_type=MESH)

    @pl.when(z == last)
    def _():
        for d in range(1, 1 + EARLY):
            tell(know_all, near(0, d, False))

    send_tokens(True)

    tell(know_x, near(1, 0, False))
    tell(know_x, near(RING_X - 1, 0, False))

    def pass_first(where, onwards):
        @pl.when(where)
        def _():
            pl.semaphore_wait(know_first, 1)

        @pl.when(where & onwards)
        def _():
            tell(know_first, near(0, 1, False))

    @pl.when(z == 1)
    def _():
        tell(know_first, near(0, 1, False))

    middle = (z == RING_Z // 2) | (z == RING_Z // 2 + 1)

    @pl.when(z == last)
    def _():
        for d in range(1 + EARLY, RING_Z):
            tell(know_all, near(0, d, False))
    @pl.when(ta == 0)
    def _():
        field[:, :, 0] = jnp.zeros_like(field[:, :, 0])
        field[1, :, 1, own] = packed[:, 0]

    @pl.when(ta == 1)
    def _():
        field[1, :, :, own] = packed[...]

    @pl.when(ha == 0)
    def _():
        field[0] = jnp.zeros_like(field[0])

    @pl.when(ha == n_ha - 1)
    def _():
        field[2] = jnp.zeros_like(field[2])

    for high in (0, 1):
        w_big[high, :, 3 * (1 - high)] = jnp.zeros_like(w_big[high, :, 0])
        for p in range(3):
            for q in range(3):
                w_big[high, p, high + q, 48:64, :channels] = jnp.zeros((16, channels), BF16)
                w_big[high, p, high + q, 0:16, channels:] = jnp.zeros((16, channels), BF16)
    for i in range(16):
        rest_ref[i, 3 * channels :, :rest] = jnp.zeros((channels, rest), BF16)
        rest_ref[i, :channels, rest:] = jnp.zeros((channels, rest), BF16)
    sel[...] = jnp.zeros_like(sel)
    k = lax.broadcasted_iota(jnp.int32, (lanes, 128), 0)
    n = lax.broadcasted_iota(jnp.int32, (lanes, 128), 1)
    for a in (0, 1):
        for step in range(3):
            column = 2 * step + k // 16 - 1
            block = (n // 64 == a) & (k % 16 == n % 16) & ((n // 16) % 4 == column)
            block = jnp.where(block, 1.0, 0.0).astype(BF16)
            for f in range(4):
                sel[384 * a + 128 * step + lanes * f : 384 * a + 128 * step + lanes * (f + 1), 128 * f : 128 * f + 128] = block
    k = lax.broadcasted_iota(jnp.int32, gather.shape, 0)
    n = lax.broadcasted_iota(jnp.int32, gather.shape, 1)
    gather[...] = jnp.where((k // members == n) & (n < 2 * GROUPS), 1.0, 0.0).astype(BF16)
    k = lax.broadcasted_iota(jnp.int32, spread.shape, 0)
    n = lax.broadcasted_iota(jnp.int32, spread.shape, 1)
    spread[...] = jnp.where((n // members == k) & (k < 2 * GROUPS), 1.0, 0.0).astype(BF16)
    pltpu.make_async_copy(vectors, vectors, vec_sem).wait()
    stat_ref[2:3] = vectors[3].reshape(1, -1)
    spread_over = w_big.at[:, :, pl.ds(0, 3), pl.ds(0, 48)]
    pltpu.make_async_copy(spread_over, spread_over, w_sem).wait()
    send_tokens(False)

    @pl.when(first)
    def _():
        transform(1)
    late = z >= RING_Z - LATE

    def tell_plane(z0):
        @pl.when(z == z0)
        def _():
            for to in range(RING_Z - LATE, RING_Z):
                tell(know_plane.at[z0], {"ha": x * RING_Z + to, "ta": ta})

    @pl.when(z <= 1)
    def _():
        pl.semaphore_wait(know_x, 2)
        pl.semaphore_wait(know_all, 1)

    tell_plane(0)
    tell_plane(1)
    pass_first((z == 2) | (z == 3), True)
    await_tokens(None)
    tokens = field.shape[3]
    row = lax.broadcasted_iota(jnp.int32, (tokens, 128), 0)

    def patches(i, sides):
        stack = []
        for h in (0, 1):
            pieces = []
            for a in sides:
                now = field[i, a, h].astype(F32)
                pieces.append(jnp.where(row == 0, 0.0, pltpu.roll(now, 1, 0)))
                pieces.append(now)
                pieces.append(jnp.where(row == tokens - 1, 0.0, pltpu.roll(now, tokens - 1, 0)))
            stack.append(jnp.concatenate(pieces, axis=-1).astype(BF16))
        chosen = sel[384 * sides[0] : 384 * (sides[-1] + 1)]
        moved = jnp.dot(jnp.concatenate(stack, axis=0), chosen, preferred_element_type=F32).astype(BF16)
        for h in (0, 1):
            for f in range(4):
                patch[4 * h + f, i] = moved[h * tokens : (h + 1) * tokens, 128 * f : 128 * f + 128]

    bias = vectors[0].reshape(1, -1)
    bias = jnp.concatenate([bias, bias], axis=-1)

    def keep_hidden(y, first, frames, total):
        for n in range(2 * parts):
            part = total[:, 128 * n : 128 * n + 128].astype(BF16).astype(F32)
            h_ref[first : first + frames, y, n] = part.reshape(frames, tokens, 128)

    def hidden_rows(y, first, frames):
        low, high = y // 2, y % 2
        total = bias
        for p in range(3):
            lhs = [
                patch[first + p : first + p + frames, i].reshape(frames * tokens, 128) for i in (low, low + 1)
            ]
            lhs = jnp.concatenate(lhs, axis=-1)
            total = total + jnp.dot(
                lhs, w_big[high, p].reshape(256, 2 * channels), preferred_element_type=F32
            )
        keep_hidden(y, first, frames, total)

    def part_of_own(y, i, start):
        low, high = y // 2, y % 2
        taps = [
            (
                patch[2 + p : 6 + p, i].reshape(4 * tokens, 128),
                w_big[high, p, 2 * (i - low) : 2 * (i - low) + 2].reshape(128, 2 * channels),
            )
            for p in range(3)
        ]
        lhs = jnp.concatenate([taps[0][0], taps[1][0]], axis=-1)
        rhs = jnp.concatenate([taps[0][1], taps[1][1]], axis=0)
        total = start + jnp.dot(lhs, rhs, preferred_element_type=F32)
        return total + jnp.dot(*taps[2], preferred_element_type=F32)

    patches(1, (0, 1))
    for y in (1, 2):
        partial[y - 1] = part_of_own(y, 1, bias)
    await_tokens(True)
    patches(0, (1,))
    patches(2, (0,))
    sums = jnp.zeros((1, 2 * channels), F32)
    squares = jnp.zeros((1, 2 * channels), F32)
    for y in (1, 2):
        values = part_of_own(y, 2 * (y - 1), partial[y - 1])
        keep_hidden(y, 2, 4, values)
        sums = sums + jnp.sum(values, axis=0, keepdims=True)
        squares = squares + jnp.sum(values * values, axis=0, keepdims=True)
    def product(value, matrix):
        terms = []
        for _ in range(3):
            term = value.astype(BF16)
            terms.append(term.astype(F32))
            value = value - terms[-1]
        terms = jnp.concatenate(terms + [jnp.zeros((5, value.shape[1]), F32)], axis=0).astype(BF16)
        result = jnp.dot(terms, matrix, preferred_element_type=F32)
        return result[0:1] + result[1:2] + result[2:3]

    folded = jnp.concatenate(
        [both[:, :channels] + both[:, channels:] for both in (sums, squares)], axis=-1
    )
    mine[...] = product(folded, gather[...])
    @pl.when(z > 1)
    def _():
        pl.semaphore_wait(know_x, 2)
    def direct_to(z0, where):
        @pl.when(late & where)
        def _():
            pl.semaphore_wait(know_plane.at[z0], 1)
            for to_x in range(RING_X):
                for to_ta in (1, 0):
                    slot = (last - z) * 8 + (to_x - x + RING_X) % RING_X * 2 + (to_ta + ta) % 2
                    pltpu.make_async_remote_copy(
                        mine, direct_in.at[slot], direct_send, direct_recv,
                        device_id={"ha": to_x * RING_Z + z0, "ta": to_ta}, device_id_type=MESH,
                    ).start()

    direct_to(0, z >= last - 1)
    plane = []
    for dx in (2, 1, 3, 0):
        for flip in (0, 1):
            if dx or flip:
                slot = 2 * dx + flip - 1
                plane.append(
                    pltpu.make_async_remote_copy(
                        mine, plane_in.at[slot], plane_send, plane_recv,
                        device_id=near(dx, 0, bool(flip)), device_id_type=MESH,
                    )
                )
    for copy in plane:
        copy.start()
    direct_to(0, z < last - 1)
    direct_to(1, True)
    pass_first(lower & (z >= 4), True)
    await_tokens(False)
    patches(0, (0, 1))
    patches(2, (0, 1))
    hidden_rows(0, 0, 6)
    direct_to(2, True)
    hidden_rows(3, 0, 6)
    hidden_rows(1, 0, 2)
    hidden_rows(2, 0, 2)
    for z0 in range(3, EARLY):
        direct_to(z0, True)
    total = mine[...]
    all_plane = pltpu.make_async_remote_copy(
        plane_in, plane_in, plane_send, plane_recv, device_id=near(0, 0, True), device_id_type=MESH
    )
    all_plane.wait_recv()
    for slot in range(plane_in.shape[0]):
        total = total + plane_in[slot]
    plane_sum[...] = total
    def ring_copy(d):
        return pltpu.make_async_remote_copy(
            plane_sum, ring_in.at[d - 1], ring_send, ring_recv,
            device_id=near(0, d, False), device_id_type=MESH,
        )

    def straight(d):
        return late & (z + d >= RING_Z) & (z + d < RING_Z + EARLY)

    pass_first(middle, z == RING_Z // 2)
    upper = (z > RING_Z // 2 + 1) & jnp.logical_not(late)

    @pl.when(upper)
    def _():
        pl.semaphore_wait(know_all, 1)

    for d in (*range(5, RING_Z), *range(1, 5)):

        @pl.when(jnp.logical_not(straight(d)) & ((d == 1) | (z + d >= RING_Z)))
        def _():
            ring_copy(d).start()
    @pl.when(early)
    def _():
        transform(2)
    @pl.when((z > 1) & (z < last) & jnp.logical_not(upper))
    def _():
        pl.semaphore_wait(know_all, 1)

    for z0 in range(2, EARLY):
        tell_plane(z0)
    for d in range(2, RING_Z):

        @pl.when(z + d <= last)
        def _():
            ring_copy(d).start()
    @pl.when(jnp.logical_not(early))
    def _():
        for p in range(3):
            transform(p)
    tokens_left()
    all_plane.wait_send()
    def ring_copies(number):
        return pltpu.make_async_remote_copy(
            ring_in.at[pl.ds(0, number)], ring_in.at[pl.ds(0, number)], ring_send, ring_recv,
            device_id=near(0, 1, False), device_id_type=MESH,
        )

    def direct_copies(number):
        return pltpu.make_async_remote_copy(
            direct_in.at[pl.ds(0, number)], direct_in.at[pl.ds(0, number)], direct_send, direct_recv,
            device_id=near(0, 1, False), device_id_type=MESH,
        )

    @pl.when(z < EARLY)
    def _():
        ring_copies(last - LATE).wait_recv()
    @pl.when(z < EARLY)
    def _():
        direct_copies(8 * LATE).wait_recv()

    @pl.when(z >= EARLY)
    def _():
        ring_copies(last).wait_recv()

    for slot in range(ring_in.shape[0]):
        total = total + ring_in[slot]
    rows = [direct_in[slot] for slot in range(8 * LATE)]
    while len(rows) > 1:
        rows = [sum(rows[at + 1 : at + 2], rows[at]) for at in range(0, len(rows), 2)]
    total = total + rows[0]
    count = n_ha * lax.axis_size("ta") * 4 * 2 * 2 * tokens * members
    shared = product(total * (1.0 / count), spread[...])
    mean, square = shared[:, :channels], shared[:, channels:]
    var = jnp.maximum(square - mean * mean, 0.0)
    scale = lax.rsqrt(var + EPS) * vectors[1].reshape(1, -1)
    stat_ref[0:1] = 0.5 * scale
    stat_ref[1:2] = 0.5 * (vectors[2].reshape(1, -1) - mean * scale)

    @pl.when(late)
    def _():
        ring_copies(last - EARLY).wait_send()
        direct_copies(8 * EARLY).wait_send()

    @pl.when(jnp.logical_not(late))
    def _():
        ring_copies(last).wait_send()


def decode_kernel(
    h_ref, stat_ref, main_ref, rest_ref, out_hbm,
    shifted, columns_wide, columns_rest, planes_wide, planes_rest, products, total, rows_f32, out, out_sem,
):
    ha, ta = lax.axis_index("ha"), lax.axis_index("ta")
    n_ha = lax.axis_size("ha")
    frames_in, rows_in, pieces, tokens, _ = h_ref.shape
    parts = pieces // 2
    channels = 128 * parts
    frames, rows = frames_in - 2, rows_in - 2
    wide = main_ref.shape[2]
    rest = channels - wide
    for f in range(frames_in):
        for part in range(parts):
            for y in range(rows_in):
                shifted[f, part, y, 0, 8 + tokens :] = jnp.zeros((8, 128), F32)
                shifted[f, part, y, 1, :8] = jnp.zeros((8, 128), F32)

    held = {}

    def activate(y, b):
        later = held.get("product", 0.0)
        for f in range(frames_in):
            inside = (ha * rows + y >= 1) & (ha * rows + y <= n_ha * rows)
            if f < 2:
                inside = inside & (ta > 0)
            for part in range(parts):
                lanes = slice(128 * part, 128 * part + 128)
                row_scale = jnp.where(inside, stat_ref[0:1, lanes], 0.0) + later
                row_shift = jnp.where(inside, stat_ref[1:2, lanes], 0.0)
                value = h_ref[f, y, b * parts + part] * row_scale + row_shift
                shifted[f, part, y, b, 8 : 8 + tokens] = value + value * jnp.tanh(value)

    def by_columns(y, k):
        def one(f, part):
            even, odd = [shifted.at[f, part, y, b] for b in (0, 1)]
            if k == 0:
                return odd[7 : 7 + tokens] - odd[8 : 8 + tokens]
            if k == 1:
                return even[8 : 8 + tokens] + odd[8 : 8 + tokens]
            if k == 2:
                return odd[8 : 8 + tokens] - even[8 : 8 + tokens]
            return even[8 : 8 + tokens] - even[9 : 9 + tokens]

        for f in range(frames_in):
            value = jnp.concatenate([one(f, part) for part in range(wide // 128)], axis=-1)
            columns_wide[k, f, y] = value.astype(BF16)
            value = jnp.concatenate([one(f, part) for part in range(wide // 128, parts)], axis=-1)
            columns_rest[k, f, y] = value.astype(BF16)

    def by_rows(i, k):
        one, two = ((0, 2), (1, 2), (2, 1), (1, 3))[i]
        for columns, planes in ((columns_wide, planes_wide), (columns_rest, planes_rest)):
            if i == 1:
                planes[k % 2] = columns[k, :, one] + columns[k, :, two]
            else:
                planes[k % 2] = columns[k, :, one] - columns[k, :, two]

    ahead = {
        0: [(activate, 0, 0), (activate, 2, 0), (by_columns, 0, 1), (by_columns, 2, 1)],
        1: [(by_columns, 0, 2), (by_columns, 2, 2), (activate, 1, 1)],
        2: [(by_columns, 0, 3), (by_columns, 2, 3), (activate, 1, 0)],
        3: [(by_columns, 1, 0), (by_columns, 1, 1)],
        4: [(by_columns, 1, 2), (by_columns, 1, 3)],
        5: [(activate, 3, 1)],
        6: [(activate, 3, 0)],
        7: [(by_columns, 3, 0)],
        8: [(by_columns, 3, 1)],
        9: [(by_columns, 3, 2)],
        10: [(by_columns, 3, 3)],
    }
    for y in (0, 2):
        activate(y, 1)
    for y in (0, 2):
        by_columns(y, 0)
    by_rows(0, 0)
    bias = stat_ref[2:3]
    copies = []

    def done(y, b, f, part, value):
        hidden = h_ref[f + 2, y + 1, b * parts + part] + bias[:, 128 * part : 128 * part + 128]
        rows_f32[y, f, part, pl.ds(b, tokens, stride=2)] = value + hidden

    def send(y, f):
        for part in range(parts):
            out[f, y, :, 128 * part : 128 * part + 128] = rows_f32[y, f, part].astype(BF16)
        copies.append(pltpu.make_async_copy(out.at[f, y], out_hbm.at[f, y], out_sem))
        copies[-1].start()

    def combine(i, f):
        for part in range(parts):
            m0, m1, m2, m3 = [products[i % 2, k, f, part] for k in range(4)]
            for b, value in ((0, m0 + m1 + m2), (1, m1 - m2 - m3)):
                if i == 0:
                    total[0, b, f, part] = value
                elif i == 1:
                    total[0, b, f, part] = total[0, b, f, part] + value
                    total[1, b, f, part] = value
                elif i == 2:
                    done(0, b, f, part, total[0, b, f, part] + value)
                    total[1, b, f, part] = total[1, b, f, part] - value
        if i == 2:
            send(0, f)

    def last_even(f):
        for part in range(parts):
            m0, m1, m2 = [products[1, k, f, part] for k in range(3)]
            done(1, 0, f, part, total[1, 0, f, part] - (m0 + m1 + m2))
            total[1, 1, f, part] = total[1, 1, f, part] - (m1 - m2)

    def last_odd(f):
        for part in range(parts):
            done(1, 1, f, part, total[1, 1, f, part] + products[1, 3, f, part])
        send(1, f)

    for i in range(4):
        for k in range(4):
            at = 4 * i + k
            for make, one, two in ahead.get(at, ()):
                make(one, two)
            if at < 15:
                by_rows((at + 1) // 4, (at + 1) % 4)
            if i and k < 2:
                combine(i - 1, 2 * k)
                combine(i - 1, 2 * k + 1)
            if at == 15:
                for f in range(frames):
                    last_even(f)
            both = (planes_wide.at[k % 2], planes_rest.at[k % 2])
            lhs = [planes[p : p + frames] for p in range(3) for planes in both]
            lhs = jnp.concatenate(lhs, axis=-1).reshape(frames * tokens, 3 * channels)
            product = jnp.dot(lhs, main_ref[at], preferred_element_type=F32)
            held["product"] = 0.0 * product[0:1, 0:128]
            for part in range(wide // 128):
                products[i % 2, k, :, part] = product[:, 128 * part : 128 * part + 128].reshape(frames, tokens, 128)
            lhs = [
                jnp.concatenate([planes[t + p] for p in range(4) for planes in both], axis=-1)
                for t in range(0, frames, 2)
            ]
            product = jnp.dot(jnp.concatenate(lhs, axis=0), rest_ref[at], preferred_element_type=F32)
            for f in range(frames):
                products[i % 2, k, f, wide // 128] = product[
                    f // 2 * tokens : (f // 2 + 1) * tokens, rest * (f % 2) : rest * (f % 2) + rest
                ]
    for f in range(frames):
        last_odd(f)
    pltpu.make_async_copy(out, out_hbm, out_sem).wait()


def keep(value):
    return pltpu.with_memory_space_constraint(value, pltpu.HBM)


def body(latent_tokens, w_in, b_in, gn_gain, gn_shift, w_mid, b_mid):
    half = latent_tokens.shape[1]
    channels = w_in.shape[-1]
    tokens = 2 * half
    wide = channels // 256 * 256
    rest = channels - wide
    parts = channels // 128
    vmem = pl.BlockSpec(memory_space=pltpu.VMEM)
    hbm = pl.BlockSpec(memory_space=pltpu.HBM)
    inputs = (latent_tokens, w_in.reshape(3, 3, -1, channels), b_in, gn_gain, gn_shift, b_mid, w_mid)
    prepared = pl.pallas_call(
        exchange_kernel,
        out_shape=(
            jax.ShapeDtypeStruct((6, 4, 2 * parts, tokens, 128), F32),
            jax.ShapeDtypeStruct((3, channels), F32),
            jax.ShapeDtypeStruct((16, 3 * channels, wide), BF16),
            jax.ShapeDtypeStruct((16, 4 * channels, 2 * rest), BF16),
        ),
        in_specs=[hbm] * len(inputs),
        out_specs=(vmem, vmem, vmem, vmem),
        scratch_shapes=[
            pltpu.VMEM(latent_tokens.shape, BF16),
            pltpu.VMEM((4, channels), F32),
            pltpu.VMEM((2, 2, half, 128), BF16),
            pltpu.VMEM((3, 2, 2, tokens, 128), BF16),
            pltpu.VMEM((8, 3, tokens, 128), BF16),
            pltpu.VMEM((2, 4 * tokens, 2 * channels), F32),
            pltpu.VMEM((2, 3, 4, 64, 2 * channels), BF16),
            pltpu.VMEM(w_mid.shape, BF16),
            pltpu.VMEM((1, 128), F32),
            pltpu.VMEM((7, 1, 128), F32),
            pltpu.VMEM((1, 128), F32),
            pltpu.VMEM((RING_Z - 1, 1, 128), F32),
            pltpu.VMEM((8 * max(LATE, EARLY), 1, 128), F32),
            pltpu.VMEM((2 * 384, 4 * 128), BF16),
            pltpu.VMEM((2 * channels, 128), BF16),
            pltpu.VMEM((128, 2 * channels), BF16),
            pltpu.SemaphoreType.DMA,
            pltpu.SemaphoreType.DMA,
            pltpu.SemaphoreType.DMA,
            pltpu.SemaphoreType.DMA((3,)),
            pltpu.SemaphoreType.DMA((5,)),
            pltpu.SemaphoreType.DMA((5,)),
            pltpu.SemaphoreType.DMA,
            pltpu.SemaphoreType.DMA,
            pltpu.SemaphoreType.DMA,
            pltpu.SemaphoreType.DMA,
            pltpu.SemaphoreType.DMA,
            pltpu.SemaphoreType.DMA,
            pltpu.SemaphoreType.REGULAR,
            pltpu.SemaphoreType.REGULAR,
            pltpu.SemaphoreType.REGULAR,
            pltpu.SemaphoreType.REGULAR((EARLY,)),
        ],
        compiler_params=pltpu.CompilerParams(
            collective_id=0, has_side_effects=True, vmem_limit_bytes=20 * 2**20
        ),
        name="exchange",
    )(*[keep(value) for value in inputs])
    return pl.pallas_call(
        decode_kernel,
        out_shape=jax.ShapeDtypeStruct((4, 2, 2 * tokens, channels), BF16),
        in_specs=[vmem, vmem, vmem, vmem],
        out_specs=hbm,
        scratch_shapes=[
            pltpu.VMEM((6, parts, 4, 2, tokens + 16, 128), F32),
            pltpu.VMEM((4, 6, 4, tokens, wide), BF16),
            pltpu.VMEM((4, 6, 4, tokens, rest), BF16),
            pltpu.VMEM((2, 6, tokens, wide), BF16),
            pltpu.VMEM((2, 6, tokens, rest), BF16),
            pltpu.VMEM((2, 4, 4, parts, tokens, 128), F32),
            pltpu.VMEM((2, 2, 4, parts, tokens, 128), F32),
            pltpu.VMEM((2, 4, parts, 2 * tokens, 128), F32),
            pltpu.VMEM((4, 2, 2 * tokens, channels), BF16),
            pltpu.SemaphoreType.DMA,
        ],
        compiler_params=pltpu.CompilerParams(vmem_limit_bytes=28 * 2**20),
        name="decode",
    )(*prepared)


def solution(mesh):
    return jax.shard_map(
        body,
        mesh=mesh,
        in_specs=(P("clip", ("ha", "ta"), None), P(), P(), P(), P(), P(), P()),
        out_specs=P(("clip", "ta"), "ha", None, None),
        check_vma=False,
    )
```

```python
import jax
import jax.numpy as jnp
from jax import lax
from jax.experimental import pallas as pl
from jax.experimental.pallas import tpu as pltpu
from jax.sharding import PartitionSpec as P

GROUPS = 32
RING_X = 4
RING_Z = 16
LATE = 4
EARLY = 4
EPS = 1e-06
MESH = pl.DeviceIdType.MESH
BF16 = jnp.bfloat16
F32 = jnp.float32


def exchange_kernel(
    tok_hbm, w_hbm, b_hbm, gain_hbm, shift_hbm, b_mid_hbm, mid_hbm,
    h_ref, stat_ref, main_ref, rest_ref,
    tok, vectors, packed, field, patch, partial, w_big, mid, mine, plane_in, plane_sum, ring_in, direct_in,
    sel, gather, spread,
    tok_sem, vec_sem, w_sem, mid_sem, send_sem, recv_sem,
    plane_send, plane_recv, ring_send, ring_recv, direct_send, direct_recv,
    know_x, know_all, know_first, know_plane,
):
    ha, ta = lax.axis_index("ha"), lax.axis_index("ta")
    n_ha = lax.axis_size("ha")
    x, z = ha // RING_Z, ha % RING_Z
    channels = vectors.shape[1]
    members = channels // GROUPS
    parts = channels // 128

    def near(dx, dz, flip):
        hx = (x + dx) % RING_X
        hz = (z + dz) % RING_Z
        return {"ha": hx * RING_Z + hz, "ta": 1 - ta if flip else ta}
    ring_in[...] = jnp.zeros_like(ring_in)
    direct_in[...] = jnp.zeros_like(direct_in)
    barrier = pltpu.get_barrier_semaphore()

    def greet(device):
        pl.semaphore_signal(barrier, inc=1, device_id=device, device_id_type=MESH)

    last = RING_Z - 1

    @pl.when(ha < n_ha - 1)
    def _():
        for t in (0, 1):
            greet({"ha": ha + 1, "ta": t})

    @pl.when(ha > 0)
    def _():
        for t in (0, 1):
            greet({"ha": ha - 1, "ta": t})

    for flip in (False, True):
        for dx in (1, RING_X - 1):
            greet(near(dx, 0, flip))
    greet(near(0, 0, True))

    @pl.when(z == 0)
    def _():
        greet(near(0, last, False))

    for d in range(2, last):

        @pl.when((z >= 1) & (z + d <= last))
        def _():
            greet(near(0, d, False))

    tok_copy = pltpu.make_async_copy(tok_hbm, tok, tok_sem)
    tok_copy.start()
    w_copies = [
        pltpu.make_async_copy(
            w_hbm,
            w_big.at[high, :, pl.ds(high, 3), pl.ds(16 * b, 48), pl.ds(channels * b, channels)],
            w_sem,
        )
        for high in (0, 1)
        for b in (0, 1)
    ]
    for copy in w_copies:
        copy.start()
    vector_copies = [
        pltpu.make_async_copy(ref, vectors.at[i], vec_sem)
        for i, ref in enumerate((b_hbm, gain_hbm, shift_hbm, b_mid_hbm))
    ]
    for copy in vector_copies:
        copy.start()

    wide = main_ref.shape[2]
    rest = channels - wide

    def fetch(p):
        return pltpu.make_async_copy(mid_hbm.at[p], mid.at[p], mid_sem.at[p])

    for p in range(3):
        fetch(p).start()

    def bank(tap_0, tap_1, tap_2):
        ends = tap_0 + tap_2
        return tap_0, 0.5 * (ends + tap_1), 0.5 * (ends - tap_1), tap_2

    def transform(p):
        fetch(p).wait()

        def rows(step, carry):
            at = pl.multiple_of(step * 16, 16)
            for part in range(parts):
                lanes = slice(128 * part, 128 * part + 128)
                taps = [[mid[p, q, r, pl.ds(at, 16), lanes].astype(F32) for r in range(3)] for q in range(3)]
                by_row = [bank(*[taps[q][r] for q in range(3)]) for r in range(3)]
                for i in range(4):
                    for k, value in enumerate(bank(*[by_row[r][i] for r in range(3)])):
                        value = value.astype(BF16)
                        if 128 * part < wide:
                            main_ref[4 * i + k, pl.ds(at + p * channels, 16), lanes] = value
                        else:
                            rest_ref[4 * i + k, pl.ds(at + p * channels, 16), :rest] = value
                            rest_ref[4 * i + k, pl.ds(at + (p + 1) * channels, 16), rest:] = value
            return carry

        lax.fori_loop(0, channels // 16, rows, 0)

    early = z < 2
    lower = z < RING_Z // 2

    @pl.when(early)
    def _():
        transform(0)

    first = (ha == 0) & (ta == 0)

    @pl.when(early & jnp.logical_not(first))
    def _():
        transform(1)
    tok_copy.wait()
    lanes = tok.shape[2] // 2
    for a in (0, 1):
        for h in (0, 1):
            packed[a, h] = jnp.concatenate(
                [tok[4 * h + f, :, a * lanes : (a + 1) * lanes].astype(F32) for f in range(4)], axis=-1
            ).astype(BF16)
    half = packed.shape[2]
    own = pl.ds(ta * half, half)
    expected = (
        5
        + jnp.where(ha > 0, 2, 0)
        + jnp.where(ha < n_ha - 1, 2, 0)
        + jnp.maximum(z - 2, 0)
        + jnp.where(z == last, 1, 0)
    )
    pl.semaphore_wait(barrier, expected)
    def tokens_copy(place, a, to_ha, to_ta, send, arrival):
        frames = pl.ds(0, 2) if to_ta else pl.ds(1, 1)
        of = pl.ds(0, 2) if to_ta else pl.ds(0, 1)
        if a is None:
            src, dst = packed.at[:, of], field.at[place, :, frames, own]
        else:
            src, dst = packed.at[a, of], field.at[place, a, frames, own]
        return pltpu.make_async_remote_copy(
            src, dst, send_sem.at[send], recv_sem.at[arrival],
            device_id={"ha": to_ha, "ta": to_ta}, device_id_type=MESH,
        )

    def send_tokens(urgent):
        @pl.when(ha < n_ha - 1)
        def _():
            for t in (0, 1):
                tokens_copy(0, int(urgent), ha + 1, t, 0 if urgent else 3, 0 if urgent else 3).start()

        @pl.when(ha > 0)
        def _():
            for t in (0, 1):
                tokens_copy(2, 1 - int(urgent), ha - 1, t, 1 if urgent else 4, 2 if urgent else 4).start()

        if urgent:
            for t in (1, 0):

                @pl.when(ta == 1 - t)
                def _():
                    tokens_copy(1, None, ha, t, 2, 1).start()

    def await_tokens(urgent):
        for to_ta in (0, 1):
            frames = pl.ds(0, 2) if to_ta else pl.ds(1, 1)

            def arrived(ref, arrival):
                pltpu.make_async_remote_copy(
                    ref, ref, send_sem.at[2], recv_sem.at[arrival],
                    device_id={"ha": ha, "ta": 1 - ta}, device_id_type=MESH,
                ).wait_recv()

            @pl.when(ta == to_ta)
            def _():
                if urgent is None:
                    arrived(field.at[1, :, frames, pl.ds((1 - to_ta) * half, half)], 1)
                    return

                @pl.when(ha > 0)
                def _():
                    arrived(field.at[0, int(urgent), frames], 0 if urgent else 3)

                @pl.when(ha < n_ha - 1)
                def _():
                    arrived(field.at[2, 1 - int(urgent), frames], 2 if urgent else 4)

    def tokens_left():
        three = field.at[pl.ds(0, 3), 0, 0, pl.ds(0, half)]

        def left(ref, send):
            pltpu.make_async_remote_copy(
                ref, ref, send_sem.at[send], recv_sem.at[1],
                device_id={"ha": ha, "ta": 1 - ta}, device_id_type=MESH,
            ).wait_send()

        @pl.when(ha < n_ha - 1)
        def _():
            left(three, 0)
            left(three, 3)

        @pl.when(ha > 0)
        def _():
            left(three, 1)
            left(three, 4)

        for t in (1, 0):

            @pl.when(ta == 1 - t)
            def _():
                tokens_copy(1, None, ha, t, 2, 1).wait_send()

    def tell(sem, device):
        pl.semaphore_signal(sem, inc=1, device_id=device, device_id_type=MESH)

    @pl.when(z == last)
    def _():
        for d in range(1, 1 + EARLY):
            tell(know_all, near(0, d, False))

    send_tokens(True)

    tell(know_x, near(1, 0, False))
    tell(know_x, near(RING_X - 1, 0, False))

    def pass_first(where, onwards):
        @pl.when(where)
        def _():
            pl.semaphore_wait(know_first, 1)

        @pl.when(where & onwards)
        def _():
            tell(know_first, near(0, 1, False))

    @pl.when(z == 1)
    def _():
        tell(know_first, near(0, 1, False))

    middle = (z == RING_Z // 2) | (z == RING_Z // 2 + 1)

    @pl.when(z == last)
    def _():
        for d in range(1 + EARLY, RING_Z):
            tell(know_all, near(0, d, False))
    @pl.when(ta == 0)
    def _():
        field[:, :, 0] = jnp.zeros_like(field[:, :, 0])
        field[1, :, 1, own] = packed[:, 0]

    @pl.when(ta == 1)
    def _():
        field[1, :, :, own] = packed[...]

    @pl.when(ha == 0)
    def _():
        field[0] = jnp.zeros_like(field[0])

    @pl.when(ha == n_ha - 1)
    def _():
        field[2] = jnp.zeros_like(field[2])

    for high in (0, 1):
        w_big[high, :, 3 * (1 - high)] = jnp.zeros_like(w_big[high, :, 0])
        for p in range(3):
            for q in range(3):
                w_big[high, p, high + q, 48:64, :channels] = jnp.zeros((16, channels), BF16)
                w_big[high, p, high + q, 0:16, channels:] = jnp.zeros((16, channels), BF16)
    for i in range(16):
        rest_ref[i, 3 * channels :, :rest] = jnp.zeros((channels, rest), BF16)
        rest_ref[i, :channels, rest:] = jnp.zeros((channels, rest), BF16)
    sel[...] = jnp.zeros_like(sel)
    k = lax.broadcasted_iota(jnp.int32, (lanes, 128), 0)
    n = lax.broadcasted_iota(jnp.int32, (lanes, 128), 1)
    for a in (0, 1):
        for step in range(3):
            column = 2 * step + k // 16 - 1
            block = (n // 64 == a) & (k % 16 == n % 16) & ((n // 16) % 4 == column)
            block = jnp.where(block, 1.0, 0.0).astype(BF16)
            for f in range(4):
                sel[384 * a + 128 * step + lanes * f : 384 * a + 128 * step + lanes * (f + 1), 128 * f : 128 * f + 128] = block
    k = lax.broadcasted_iota(jnp.int32, gather.shape, 0)
    n = lax.broadcasted_iota(jnp.int32, gather.shape, 1)
    gather[...] = jnp.where((k // members == n) & (n < 2 * GROUPS), 1.0, 0.0).astype(BF16)
    k = lax.broadcasted_iota(jnp.int32, spread.shape, 0)
    n = lax.broadcasted_iota(jnp.int32, spread.shape, 1)
    spread[...] = jnp.where((n // members == k) & (k < 2 * GROUPS), 1.0, 0.0).astype(BF16)
    pltpu.make_async_copy(vectors, vectors, vec_sem).wait()
    stat_ref[2:3] = vectors[3].reshape(1, -1)
    spread_over = w_big.at[:, :, pl.ds(0, 3), pl.ds(0, 48)]
    pltpu.make_async_copy(spread_over, spread_over, w_sem).wait()
    send_tokens(False)

    @pl.when(first)
    def _():
        transform(1)
    late = z >= RING_Z - LATE

    def tell_plane(z0):
        @pl.when(z == z0)
        def _():
            for to in range(RING_Z - LATE, RING_Z):
                tell(know_plane.at[z0], {"ha": x * RING_Z + to, "ta": ta})

    @pl.when(z <= 1)
    def _():
        pl.semaphore_wait(know_x, 2)
        pl.semaphore_wait(know_all, 1)

    tell_plane(0)
    tell_plane(1)
    pass_first((z == 2) | (z == 3), True)
    await_tokens(None)
    tokens = field.shape[3]
    row = lax.broadcasted_iota(jnp.int32, (tokens, 128), 0)

    def patches(i, sides):
        stack = []
        for h in (0, 1):
            pieces = []
            for a in sides:
                now = field[i, a, h].astype(F32)
                pieces.append(jnp.where(row == 0, 0.0, pltpu.roll(now, 1, 0)))
                pieces.append(now)
                pieces.append(jnp.where(row == tokens - 1, 0.0, pltpu.roll(now, tokens - 1, 0)))
            stack.append(jnp.concatenate(pieces, axis=-1).astype(BF16))
        chosen = sel[384 * sides[0] : 384 * (sides[-1] + 1)]
        moved = jnp.dot(jnp.concatenate(stack, axis=0), chosen, preferred_element_type=F32).astype(BF16)
        for h in (0, 1):
            for f in range(4):
                patch[4 * h + f, i] = moved[h * tokens : (h + 1) * tokens, 128 * f : 128 * f + 128]

    bias = vectors[0].reshape(1, -1)
    bias = jnp.concatenate([bias, bias], axis=-1)

    def keep_hidden(y, first, frames, total):
        for n in range(2 * parts):
            part = total[:, 128 * n : 128 * n + 128].astype(BF16).astype(F32)
            h_ref[first : first + frames, y, n] = part.reshape(frames, tokens, 128)

    def hidden_rows(y, first, frames):
        low, high = y // 2, y % 2
        total = bias
        for p in range(3):
            lhs = [
                patch[first + p : first + p + frames, i].reshape(frames * tokens, 128) for i in (low, low + 1)
            ]
            lhs = jnp.concatenate(lhs, axis=-1)
            total = total + jnp.dot(
                lhs, w_big[high, p].reshape(256, 2 * channels), preferred_element_type=F32
            )
        keep_hidden(y, first, frames, total)

    def part_of_own(y, i, start):
        low, high = y // 2, y % 2
        taps = [
            (
                patch[2 + p : 6 + p, i].reshape(4 * tokens, 128),
                w_big[high, p, 2 * (i - low) : 2 * (i - low) + 2].reshape(128, 2 * channels),
            )
            for p in range(3)
        ]
        lhs = jnp.concatenate([taps[0][0], taps[1][0]], axis=-1)
        rhs = jnp.concatenate([taps[0][1], taps[1][1]], axis=0)
        total = start + jnp.dot(lhs, rhs, preferred_element_type=F32)
        return total + jnp.dot(*taps[2], preferred_element_type=F32)

    patches(1, (0, 1))
    for y in (1, 2):
        partial[y - 1] = part_of_own(y, 1, bias)
    await_tokens(True)
    patches(0, (1,))
    patches(2, (0,))
    sums = jnp.zeros((1, 2 * channels), F32)
    squares = jnp.zeros((1, 2 * channels), F32)
    for y in (1, 2):
        values = part_of_own(y, 2 * (y - 1), partial[y - 1])
        keep_hidden(y, 2, 4, values)
        sums = sums + jnp.sum(values, axis=0, keepdims=True)
        squares = squares + jnp.sum(values * values, axis=0, keepdims=True)
    def product(value, matrix):
        terms = []
        for _ in range(3):
            term = value.astype(BF16)
            terms.append(term.astype(F32))
            value = value - terms[-1]
        terms = jnp.concatenate(terms + [jnp.zeros((5, value.shape[1]), F32)], axis=0).astype(BF16)
        result = jnp.dot(terms, matrix, preferred_element_type=F32)
        return result[0:1] + result[1:2] + result[2:3]

    folded = jnp.concatenate(
        [both[:, :channels] + both[:, channels:] for both in (sums, squares)], axis=-1
    )
    mine[...] = product(folded, gather[...])
    @pl.when(z > 1)
    def _():
        pl.semaphore_wait(know_x, 2)
    def direct_to(z0, where):
        @pl.when(late & where)
        def _():
            pl.semaphore_wait(know_plane.at[z0], 1)
            for to_x in range(RING_X):
                for to_ta in (1, 0):
                    slot = (last - z) * 8 + (to_x - x + RING_X) % RING_X * 2 + (to_ta + ta) % 2
                    pltpu.make_async_remote_copy(
                        mine, direct_in.at[slot], direct_send, direct_recv,
                        device_id={"ha": to_x * RING_Z + z0, "ta": to_ta}, device_id_type=MESH,
                    ).start()

    direct_to(0, z >= last - 1)
    plane = []
    for dx in (2, 1, 3, 0):
        for flip in (0, 1):
            if dx or flip:
                slot = 2 * dx + flip - 1
                plane.append(
                    pltpu.make_async_remote_copy(
                        mine, plane_in.at[slot], plane_send, plane_recv,
                        device_id=near(dx, 0, bool(flip)), device_id_type=MESH,
                    )
                )
    for copy in plane:
        copy.start()
    direct_to(0, z < last - 1)
    direct_to(1, True)
    pass_first(lower & (z >= 4), True)
    await_tokens(False)
    patches(0, (0, 1))
    patches(2, (0, 1))
    hidden_rows(0, 0, 6)
    direct_to(2, True)
    hidden_rows(3, 0, 6)
    hidden_rows(1, 0, 2)
    hidden_rows(2, 0, 2)
    for z0 in range(3, EARLY):
        direct_to(z0, True)
    total = mine[...]
    all_plane = pltpu.make_async_remote_copy(
        plane_in, plane_in, plane_send, plane_recv, device_id=near(0, 0, True), device_id_type=MESH
    )
    all_plane.wait_recv()
    for slot in range(plane_in.shape[0]):
        total = total + plane_in[slot]
    plane_sum[...] = total
    def ring_copy(d):
        return pltpu.make_async_remote_copy(
            plane_sum, ring_in.at[d - 1], ring_send, ring_recv,
            device_id=near(0, d, False), device_id_type=MESH,
        )

    def straight(d):
        return late & (z + d >= RING_Z) & (z + d < RING_Z + EARLY)

    pass_first(middle, z == RING_Z // 2)
    upper = (z > RING_Z // 2 + 1) & jnp.logical_not(late)

    @pl.when(upper)
    def _():
        pl.semaphore_wait(know_all, 1)

    for d in (*range(5, RING_Z), *range(1, 5)):

        @pl.when(jnp.logical_not(straight(d)) & ((d == 1) | (z + d >= RING_Z)))
        def _():
            ring_copy(d).start()
    @pl.when(early)
    def _():
        transform(2)
    @pl.when((z > 1) & (z < last) & jnp.logical_not(upper))
    def _():
        pl.semaphore_wait(know_all, 1)

    for z0 in range(2, EARLY):
        tell_plane(z0)
    for d in range(2, RING_Z):

        @pl.when(z + d <= last)
        def _():
            ring_copy(d).start()
    @pl.when(jnp.logical_not(early))
    def _():
        for p in range(3):
            transform(p)
    tokens_left()
    all_plane.wait_send()
    def ring_copies(number):
        return pltpu.make_async_remote_copy(
            ring_in.at[pl.ds(0, number)], ring_in.at[pl.ds(0, number)], ring_send, ring_recv,
            device_id=near(0, 1, False), device_id_type=MESH,
        )

    def direct_copies(number):
        return pltpu.make_async_remote_copy(
            direct_in.at[pl.ds(0, number)], direct_in.at[pl.ds(0, number)], direct_send, direct_recv,
            device_id=near(0, 1, False), device_id_type=MESH,
        )

    @pl.when(z < EARLY)
    def _():
        ring_copies(last - LATE).wait_recv()
    @pl.when(z < EARLY)
    def _():
        direct_copies(8 * LATE).wait_recv()

    @pl.when(z >= EARLY)
    def _():
        ring_copies(last).wait_recv()

    for slot in range(ring_in.shape[0]):
        total = total + ring_in[slot]
    rows = [direct_in[slot] for slot in range(8 * LATE)]
    while len(rows) > 1:
        rows = [sum(rows[at + 1 : at + 2], rows[at]) for at in range(0, len(rows), 2)]
    total = total + rows[0]
    count = n_ha * lax.axis_size("ta") * 4 * 2 * 2 * tokens * members
    shared = product(total * (1.0 / count), spread[...])
    mean, square = shared[:, :channels], shared[:, channels:]
    var = jnp.maximum(square - mean * mean, 0.0)
    scale = lax.rsqrt(var + EPS) * vectors[1].reshape(1, -1)
    stat_ref[0:1] = 0.5 * scale
    stat_ref[1:2] = 0.5 * (vectors[2].reshape(1, -1) - mean * scale)

    @pl.when(late)
    def _():
        ring_copies(last - EARLY).wait_send()
        direct_copies(8 * EARLY).wait_send()

    @pl.when(jnp.logical_not(late))
    def _():
        ring_copies(last).wait_send()


def decode_kernel(
    h_ref, stat_ref, main_ref, rest_ref, out_hbm,
    shifted, columns_wide, columns_rest, planes_wide, planes_rest, products, total, rows_f32, out, out_sem,
):
    ha, ta = lax.axis_index("ha"), lax.axis_index("ta")
    n_ha = lax.axis_size("ha")
    frames_in, rows_in, pieces, tokens, _ = h_ref.shape
    parts = pieces // 2
    channels = 128 * parts
    frames, rows = frames_in - 2, rows_in - 2
    wide = main_ref.shape[2]
    rest = channels - wide
    for f in range(frames_in):
        for part in range(parts):
            for y in range(rows_in):
                shifted[f, part, y, 0, 8 + tokens :] = jnp.zeros((8, 128), F32)
                shifted[f, part, y, 1, :8] = jnp.zeros((8, 128), F32)

    held = {}

    def activate(y, b):
        later = held.get("product", 0.0)
        for f in range(frames_in):
            inside = (ha * rows + y >= 1) & (ha * rows + y <= n_ha * rows)
            if f < 2:
                inside = inside & (ta > 0)
            for part in range(parts):
                lanes = slice(128 * part, 128 * part + 128)
                row_scale = jnp.where(inside, stat_ref[0:1, lanes], 0.0) + later
                row_shift = jnp.where(inside, stat_ref[1:2, lanes], 0.0)
                value = h_ref[f, y, b * parts + part] * row_scale + row_shift
                shifted[f, part, y, b, 8 : 8 + tokens] = value + value * jnp.tanh(value)

    def by_columns(y, k):
        def one(f, part):
            even, odd = [shifted.at[f, part, y, b] for b in (0, 1)]
            if k == 0:
                return odd[7 : 7 + tokens] - odd[8 : 8 + tokens]
            if k == 1:
                return even[8 : 8 + tokens] + odd[8 : 8 + tokens]
            if k == 2:
                return odd[8 : 8 + tokens] - even[8 : 8 + tokens]
            return even[8 : 8 + tokens] - even[9 : 9 + tokens]

        for f in range(frames_in):
            value = jnp.concatenate([one(f, part) for part in range(wide // 128)], axis=-1)
            columns_wide[k, f, y] = value.astype(BF16)
            value = jnp.concatenate([one(f, part) for part in range(wide // 128, parts)], axis=-1)
            columns_rest[k, f, y] = value.astype(BF16)

    def by_rows(i, k):
        one, two = ((0, 2), (1, 2), (2, 1), (1, 3))[i]
        for columns, planes in ((columns_wide, planes_wide), (columns_rest, planes_rest)):
            if i == 1:
                planes[k % 2] = columns[k, :, one] + columns[k, :, two]
            else:
                planes[k % 2] = columns[k, :, one] - columns[k, :, two]

    ahead = {
        0: [(activate, 0, 0), (activate, 2, 0), (by_columns, 0, 1), (by_columns, 2, 1)],
        1: [(by_columns, 0, 2), (by_columns, 2, 2), (activate, 1, 1)],
        2: [(by_columns, 0, 3), (by_columns, 2, 3), (activate, 1, 0)],
        3: [(by_columns, 1, 0), (by_columns, 1, 1)],
        4: [(by_columns, 1, 2), (by_columns, 1, 3)],
        5: [(activate, 3, 1)],
        6: [(activate, 3, 0)],
        7: [(by_columns, 3, 0)],
        8: [(by_columns, 3, 1)],
        9: [(by_columns, 3, 2)],
        10: [(by_columns, 3, 3)],
    }
    for y in (0, 2):
        activate(y, 1)
    for y in (0, 2):
        by_columns(y, 0)
    by_rows(0, 0)
    bias = stat_ref[2:3]
    copies = []

    def done(y, b, f, part, value):
        hidden = h_ref[f + 2, y + 1, b * parts + part] + bias[:, 128 * part : 128 * part + 128]
        rows_f32[y, f, part, pl.ds(b, tokens, stride=2)] = value + hidden

    def send(y, f):
        for part in range(parts):
            out[f, y, :, 128 * part : 128 * part + 128] = rows_f32[y, f, part].astype(BF16)
        copies.append(pltpu.make_async_copy(out.at[f, y], out_hbm.at[f, y], out_sem))
        copies[-1].start()

    def combine(i, f):
        for part in range(parts):
            m0, m1, m2, m3 = [products[i % 2, k, f, part] for k in range(4)]
            for b, value in ((0, m0 + m1 + m2), (1, m1 - m2 - m3)):
                if i == 0:
                    total[0, b, f, part] = value
                elif i == 1:
                    total[0, b, f, part] = total[0, b, f, part] + value
                    total[1, b, f, part] = value
                elif i == 2:
                    done(0, b, f, part, total[0, b, f, part] + value)
                    total[1, b, f, part] = total[1, b, f, part] - value
        if i == 2:
            send(0, f)

    def last_even(f):
        for part in range(parts):
            m0, m1, m2 = [products[1, k, f, part] for k in range(3)]
            done(1, 0, f, part, total[1, 0, f, part] - (m0 + m1 + m2))
            total[1, 1, f, part] = total[1, 1, f, part] - (m1 - m2)

    def last_odd(f):
        for part in range(parts):
            done(1, 1, f, part, total[1, 1, f, part] + products[1, 3, f, part])
        send(1, f)

    for i in range(4):
        for k in range(4):
            at = 4 * i + k
            for make, one, two in ahead.get(at, ()):
                make(one, two)
            if at < 15:
                by_rows((at + 1) // 4, (at + 1) % 4)
            if i and k < 2:
                combine(i - 1, 2 * k)
                combine(i - 1, 2 * k + 1)
            if at == 15:
                for f in range(frames):
                    last_even(f)
            both = (planes_wide.at[k % 2], planes_rest.at[k % 2])
            lhs = [planes[p : p + frames] for p in range(3) for planes in both]
            lhs = jnp.concatenate(lhs, axis=-1).reshape(frames * tokens, 3 * channels)
            product = jnp.dot(lhs, main_ref[at], preferred_element_type=F32)
            held["product"] = 0.0 * product[0:1, 0:128]
            for part in range(wide // 128):
                products[i % 2, k, :, part] = product[:, 128 * part : 128 * part + 128].reshape(frames, tokens, 128)
            lhs = [
                jnp.concatenate([planes[t + p] for p in range(4) for planes in both], axis=-1)
                for t in range(0, frames, 2)
            ]
            product = jnp.dot(jnp.concatenate(lhs, axis=0), rest_ref[at], preferred_element_type=F32)
            for f in range(frames):
                products[i % 2, k, f, wide // 128] = product[
                    f // 2 * tokens : (f // 2 + 1) * tokens, rest * (f % 2) : rest * (f % 2) + rest
                ]
    for f in range(frames):
        last_odd(f)
    pltpu.make_async_copy(out, out_hbm, out_sem).wait()


def keep(value):
    return pltpu.with_memory_space_constraint(value, pltpu.HBM)


def body(latent_tokens, w_in, b_in, gn_gain, gn_shift, w_mid, b_mid):
    half = latent_tokens.shape[1]
    channels = w_in.shape[-1]
    tokens = 2 * half
    wide = channels // 256 * 256
    rest = channels - wide
    parts = channels // 128
    vmem = pl.BlockSpec(memory_space=pltpu.VMEM)
    hbm = pl.BlockSpec(memory_space=pltpu.HBM)
    inputs = (latent_tokens, w_in.reshape(3, 3, -1, channels), b_in, gn_gain, gn_shift, b_mid, w_mid)
    prepared = pl.pallas_call(
        exchange_kernel,
        out_shape=(
            jax.ShapeDtypeStruct((6, 4, 2 * parts, tokens, 128), F32),
            jax.ShapeDtypeStruct((3, channels), F32),
            jax.ShapeDtypeStruct((16, 3 * channels, wide), BF16),
            jax.ShapeDtypeStruct((16, 4 * channels, 2 * rest), BF16),
        ),
        in_specs=[hbm] * len(inputs),
        out_specs=(vmem, vmem, vmem, vmem),
        scratch_shapes=[
            pltpu.VMEM(latent_tokens.shape, BF16),
            pltpu.VMEM((4, channels), F32),
            pltpu.VMEM((2, 2, half, 128), BF16),
            pltpu.VMEM((3, 2, 2, tokens, 128), BF16),
            pltpu.VMEM((8, 3, tokens, 128), BF16),
            pltpu.VMEM((2, 4 * tokens, 2 * channels), F32),
            pltpu.VMEM((2, 3, 4, 64, 2 * channels), BF16),
            pltpu.VMEM(w_mid.shape, BF16),
            pltpu.VMEM((1, 128), F32),
            pltpu.VMEM((7, 1, 128), F32),
            pltpu.VMEM((1, 128), F32),
            pltpu.VMEM((RING_Z - 1, 1, 128), F32),
            pltpu.VMEM((8 * max(LATE, EARLY), 1, 128), F32),
            pltpu.VMEM((2 * 384, 4 * 128), BF16),
            pltpu.VMEM((2 * channels, 128), BF16),
            pltpu.VMEM((128, 2 * channels), BF16),
            pltpu.SemaphoreType.DMA,
            pltpu.SemaphoreType.DMA,
            pltpu.SemaphoreType.DMA,
            pltpu.SemaphoreType.DMA((3,)),
            pltpu.SemaphoreType.DMA((5,)),
            pltpu.SemaphoreType.DMA((5,)),
            pltpu.SemaphoreType.DMA,
            pltpu.SemaphoreType.DMA,
            pltpu.SemaphoreType.DMA,
            pltpu.SemaphoreType.DMA,
            pltpu.SemaphoreType.DMA,
            pltpu.SemaphoreType.DMA,
            pltpu.SemaphoreType.REGULAR,
            pltpu.SemaphoreType.REGULAR,
            pltpu.SemaphoreType.REGULAR,
            pltpu.SemaphoreType.REGULAR((EARLY,)),
        ],
        compiler_params=pltpu.CompilerParams(
            collective_id=0, has_side_effects=True, vmem_limit_bytes=20 * 2**20
        ),
        name="exchange",
    )(*[keep(value) for value in inputs])
    return pl.pallas_call(
        decode_kernel,
        out_shape=jax.ShapeDtypeStruct((4, 2, 2 * tokens, channels), BF16),
        in_specs=[vmem, vmem, vmem, vmem],
        out_specs=hbm,
        scratch_shapes=[
            pltpu.VMEM((6, parts, 4, 2, tokens + 16, 128), F32),
            pltpu.VMEM((4, 6, 4, tokens, wide), BF16),
            pltpu.VMEM((4, 6, 4, tokens, rest), BF16),
            pltpu.VMEM((2, 6, tokens, wide), BF16),
            pltpu.VMEM((2, 6, tokens, rest), BF16),
            pltpu.VMEM((2, 4, 4, parts, tokens, 128), F32),
            pltpu.VMEM((2, 2, 4, parts, tokens, 128), F32),
            pltpu.VMEM((2, 4, parts, 2 * tokens, 128), F32),
            pltpu.VMEM((4, 2, 2 * tokens, channels), BF16),
            pltpu.SemaphoreType.DMA,
        ],
        compiler_params=pltpu.CompilerParams(vmem_limit_bytes=28 * 2**20),
        name="decode",
    )(*prepared)


def solution(mesh):
    return jax.shard_map(
        body,
        mesh=mesh,
        in_specs=(P("clip", ("ha", "ta"), None), P(), P(), P(), P(), P(), P()),
        out_specs=P(("clip", "ta"), "ha", None, None),
        check_vma=False,
    )
```

```python
import jax
import jax.numpy as jnp
from jax import lax
from jax.experimental import pallas as pl
from jax.experimental.pallas import tpu as pltpu
from jax.sharding import PartitionSpec as P

GROUPS = 32
RING_X = 4
RING_Z = 16
LATE = 4
EARLY = 4
EPS = 1e-06
MESH = pl.DeviceIdType.MESH
BF16 = jnp.bfloat16
F32 = jnp.float32


def exchange_kernel(
    tok_hbm, w_hbm, b_hbm, gain_hbm, shift_hbm, b_mid_hbm, mid_hbm,
    h_ref, stat_ref, main_ref, rest_ref,
    tok, vectors, packed, field, patch, partial, w_big, mid, mine, plane_in, plane_sum, ring_in, direct_in,
    sel, gather, spread,
    tok_sem, vec_sem, w_sem, mid_sem, send_sem, recv_sem,
    plane_send, plane_recv, ring_send, ring_recv, direct_send, direct_recv,
    know_x, know_all, know_first, know_plane,
):
    ha, ta = lax.axis_index("ha"), lax.axis_index("ta")
    n_ha = lax.axis_size("ha")
    x, z = ha // RING_Z, ha % RING_Z
    channels = vectors.shape[1]
    members = channels // GROUPS
    parts = channels // 128

    def near(dx, dz, flip):
        hx = (x + dx) % RING_X
        hz = (z + dz) % RING_Z
        return {"ha": hx * RING_Z + hz, "ta": 1 - ta if flip else ta}
    ring_in[...] = jnp.zeros_like(ring_in)
    direct_in[...] = jnp.zeros_like(direct_in)
    barrier = pltpu.get_barrier_semaphore()

    def greet(device):
        pl.semaphore_signal(barrier, inc=1, device_id=device, device_id_type=MESH)

    last = RING_Z - 1

    @pl.when(ha < n_ha - 1)
    def _():
        for t in (0, 1):
            greet({"ha": ha + 1, "ta": t})

    @pl.when(ha > 0)
    def _():
        for t in (0, 1):
            greet({"ha": ha - 1, "ta": t})

    for flip in (False, True):
        for dx in (1, RING_X - 1):
            greet(near(dx, 0, flip))
    greet(near(0, 0, True))

    @pl.when(z == 0)
    def _():
        greet(near(0, last, False))

    for d in range(2, last):

        @pl.when((z >= 1) & (z + d <= last))
        def _():
            greet(near(0, d, False))

    tok_copy = pltpu.make_async_copy(tok_hbm, tok, tok_sem)
    tok_copy.start()
    w_copies = [
        pltpu.make_async_copy(
            w_hbm,
            w_big.at[high, :, pl.ds(high, 3), pl.ds(16 * b, 48), pl.ds(channels * b, channels)],
            w_sem,
        )
        for high in (0, 1)
        for b in (0, 1)
    ]
    for copy in w_copies:
        copy.start()
    vector_copies = [
        pltpu.make_async_copy(ref, vectors.at[i], vec_sem)
        for i, ref in enumerate((b_hbm, gain_hbm, shift_hbm, b_mid_hbm))
    ]
    for copy in vector_copies:
        copy.start()

    wide = main_ref.shape[2]
    rest = channels - wide

    def fetch(p):
        return pltpu.make_async_copy(mid_hbm.at[p], mid.at[p], mid_sem.at[p])

    for p in range(3):
        fetch(p).start()

    def bank(tap_0, tap_1, tap_2):
        ends = tap_0 + tap_2
        return tap_0, 0.5 * (ends + tap_1), 0.5 * (ends - tap_1), tap_2

    def transform(p):
        fetch(p).wait()

        def rows(step, carry):
            at = pl.multiple_of(step * 16, 16)
            for part in range(parts):
                lanes = slice(128 * part, 128 * part + 128)
                taps = [[mid[p, q, r, pl.ds(at, 16), lanes].astype(F32) for r in range(3)] for q in range(3)]
                by_row = [bank(*[taps[q][r] for q in range(3)]) for r in range(3)]
                for i in range(4):
                    for k, value in enumerate(bank(*[by_row[r][i] for r in range(3)])):
                        value = value.astype(BF16)
                        if 128 * part < wide:
                            main_ref[4 * i + k, pl.ds(at + p * channels, 16), lanes] = value
                        else:
                            rest_ref[4 * i + k, pl.ds(at + p * channels, 16), :rest] = value
                            rest_ref[4 * i + k, pl.ds(at + (p + 1) * channels, 16), rest:] = value
            return carry

        lax.fori_loop(0, channels // 16, rows, 0)

    early = z < 2
    lower = z < RING_Z // 2

    @pl.when(early)
    def _():
        transform(0)

    first = (ha == 0) & (ta == 0)

    @pl.when(early & jnp.logical_not(first))
    def _():
        transform(1)
    tok_copy.wait()
    lanes = tok.shape[2] // 2
    for a in (0, 1):
        for h in (0, 1):
            packed[a, h] = jnp.concatenate(
                [tok[4 * h + f, :, a * lanes : (a + 1) * lanes].astype(F32) for f in range(4)], axis=-1
            ).astype(BF16)
    half = packed.shape[2]
    own = pl.ds(ta * half, half)
    expected = (
        5
        + jnp.where(ha > 0, 2, 0)
        + jnp.where(ha < n_ha - 1, 2, 0)
        + jnp.maximum(z - 2, 0)
        + jnp.where(z == last, 1, 0)
    )
    pl.semaphore_wait(barrier, expected)
    def tokens_copy(place, a, to_ha, to_ta, send, arrival):
        frames = pl.ds(0, 2) if to_ta else pl.ds(1, 1)
        of = pl.ds(0, 2) if to_ta else pl.ds(0, 1)
        if a is None:
            src, dst = packed.at[:, of], field.at[place, :, frames, own]
        else:
            src, dst = packed.at[a, of], field.at[place, a, frames, own]
        return pltpu.make_async_remote_copy(
            src, dst, send_sem.at[send], recv_sem.at[arrival],
            device_id={"ha": to_ha, "ta": to_ta}, device_id_type=MESH,
        )

    def send_tokens(urgent):
        @pl.when(ha < n_ha - 1)
        def _():
            for t in (1, 0):
                tokens_copy(0, int(urgent), ha + 1, t, 0 if urgent else 3, 0 if urgent else 3).start()

        @pl.when(ha > 0)
        def _():
            for t in (1, 0):
                tokens_copy(2, 1 - int(urgent), ha - 1, t, 1 if urgent else 4, 2 if urgent else 4).start()

        if urgent:
            for t in (1, 0):

                @pl.when(ta == 1 - t)
                def _():
                    tokens_copy(1, None, ha, t, 2, 1).start()

    def await_tokens(urgent):
        for to_ta in (0, 1):
            frames = pl.ds(0, 2) if to_ta else pl.ds(1, 1)

            def arrived(ref, arrival):
                pltpu.make_async_remote_copy(
                    ref, ref, send_sem.at[2], recv_sem.at[arrival],
                    device_id={"ha": ha, "ta": 1 - ta}, device_id_type=MESH,
                ).wait_recv()

            @pl.when(ta == to_ta)
            def _():
                if urgent is None:
                    arrived(field.at[1, :, frames, pl.ds((1 - to_ta) * half, half)], 1)
                    return

                @pl.when(ha > 0)
                def _():
                    arrived(field.at[0, int(urgent), frames], 0 if urgent else 3)

                @pl.when(ha < n_ha - 1)
                def _():
                    arrived(field.at[2, 1 - int(urgent), frames], 2 if urgent else 4)

    def tokens_left():
        three = field.at[pl.ds(0, 3), 0, 0, pl.ds(0, half)]

        def left(ref, send):
            pltpu.make_async_remote_copy(
                ref, ref, send_sem.at[send], recv_sem.at[1],
                device_id={"ha": ha, "ta": 1 - ta}, device_id_type=MESH,
            ).wait_send()

        @pl.when(ha < n_ha - 1)
        def _():
            left(three, 0)
            left(three, 3)

        @pl.when(ha > 0)
        def _():
            left(three, 1)
            left(three, 4)

        for t in (1, 0):

            @pl.when(ta == 1 - t)
            def _():
                tokens_copy(1, None, ha, t, 2, 1).wait_send()

    def tell(sem, device):
        pl.semaphore_signal(sem, inc=1, device_id=device, device_id_type=MESH)

    @pl.when(z == last)
    def _():
        for d in range(1, 1 + EARLY):
            tell(know_all, near(0, d, False))

    send_tokens(True)

    tell(know_x, near(1, 0, False))
    tell(know_x, near(RING_X - 1, 0, False))

    def pass_first(where, onwards):
        @pl.when(where)
        def _():
            pl.semaphore_wait(know_first, 1)

        @pl.when(where & onwards)
        def _():
            tell(know_first, near(0, 1, False))

    @pl.when(z == 1)
    def _():
        tell(know_first, near(0, 1, False))

    middle = (z == RING_Z // 2) | (z == RING_Z // 2 + 1)

    @pl.when(z == last)
    def _():
        for d in range(1 + EARLY, RING_Z):
            tell(know_all, near(0, d, False))
    @pl.when(ta == 0)
    def _():
        field[:, :, 0] = jnp.zeros_like(field[:, :, 0])
        field[1, :, 1, own] = packed[:, 0]

    @pl.when(ta == 1)
    def _():
        field[1, :, :, own] = packed[...]

    @pl.when(ha == 0)
    def _():
        field[0] = jnp.zeros_like(field[0])

    @pl.when(ha == n_ha - 1)
    def _():
        field[2] = jnp.zeros_like(field[2])

    for high in (0, 1):
        w_big[high, :, 3 * (1 - high)] = jnp.zeros_like(w_big[high, :, 0])
        for p in range(3):
            for q in range(3):
                w_big[high, p, high + q, 48:64, :channels] = jnp.zeros((16, channels), BF16)
                w_big[high, p, high + q, 0:16, channels:] = jnp.zeros((16, channels), BF16)
    for i in range(16):
        rest_ref[i, 3 * channels :, :rest] = jnp.zeros((channels, rest), BF16)
        rest_ref[i, :channels, rest:] = jnp.zeros((channels, rest), BF16)
    sel[...] = jnp.zeros_like(sel)
    k = lax.broadcasted_iota(jnp.int32, (lanes, 128), 0)
    n = lax.broadcasted_iota(jnp.int32, (lanes, 128), 1)
    for a in (0, 1):
        for step in range(3):
            column = 2 * step + k // 16 - 1
            block = (n // 64 == a) & (k % 16 == n % 16) & ((n // 16) % 4 == column)
            block = jnp.where(block, 1.0, 0.0).astype(BF16)
            for f in range(4):
                sel[384 * a + 128 * step + lanes * f : 384 * a + 128 * step + lanes * (f + 1), 128 * f : 128 * f + 128] = block
    k = lax.broadcasted_iota(jnp.int32, gather.shape, 0)
    n = lax.broadcasted_iota(jnp.int32, gather.shape, 1)
    gather[...] = jnp.where((k // members == n) & (n < 2 * GROUPS), 1.0, 0.0).astype(BF16)
    k = lax.broadcasted_iota(jnp.int32, spread.shape, 0)
    n = lax.broadcasted_iota(jnp.int32, spread.shape, 1)
    spread[...] = jnp.where((n // members == k) & (k < 2 * GROUPS), 1.0, 0.0).astype(BF16)
    pltpu.make_async_copy(vectors, vectors, vec_sem).wait()
    stat_ref[2:3] = vectors[3].reshape(1, -1)
    spread_over = w_big.at[:, :, pl.ds(0, 3), pl.ds(0, 48)]
    pltpu.make_async_copy(spread_over, spread_over, w_sem).wait()
    send_tokens(False)

    @pl.when(first)
    def _():
        transform(1)
    late = z >= RING_Z - LATE

    def tell_plane(z0):
        @pl.when(z == z0)
        def _():
            for to in range(RING_Z - LATE, RING_Z):
                tell(know_plane.at[z0], {"ha": x * RING_Z + to, "ta": ta})

    @pl.when(z <= 1)
    def _():
        pl.semaphore_wait(know_x, 2)
        pl.semaphore_wait(know_all, 1)

    tell_plane(0)
    tell_plane(1)
    pass_first((z == 2) | (z == 3), True)
    await_tokens(None)
    tokens = field.shape[3]
    row = lax.broadcasted_iota(jnp.int32, (tokens, 128), 0)

    def patches(i, sides):
        stack = []
        for h in (0, 1):
            pieces = []
            for a in sides:
                now = field[i, a, h].astype(F32)
                pieces.append(jnp.where(row == 0, 0.0, pltpu.roll(now, 1, 0)))
                pieces.append(now)
                pieces.append(jnp.where(row == tokens - 1, 0.0, pltpu.roll(now, tokens - 1, 0)))
            stack.append(jnp.concatenate(pieces, axis=-1).astype(BF16))
        chosen = sel[384 * sides[0] : 384 * (sides[-1] + 1)]
        moved = jnp.dot(jnp.concatenate(stack, axis=0), chosen, preferred_element_type=F32).astype(BF16)
        for h in (0, 1):
            for f in range(4):
                patch[4 * h + f, i] = moved[h * tokens : (h + 1) * tokens, 128 * f : 128 * f + 128]

    bias = vectors[0].reshape(1, -1)
    bias = jnp.concatenate([bias, bias], axis=-1)

    def keep_hidden(y, first, frames, total):
        for n in range(2 * parts):
            part = total[:, 128 * n : 128 * n + 128].astype(BF16).astype(F32)
            h_ref[first : first + frames, y, n] = part.reshape(frames, tokens, 128)

    def hidden_rows(y, first, frames):
        low, high = y // 2, y % 2
        total = bias
        for p in range(3):
            lhs = [
                patch[first + p : first + p + frames, i].reshape(frames * tokens, 128) for i in (low, low + 1)
            ]
            lhs = jnp.concatenate(lhs, axis=-1)
            total = total + jnp.dot(
                lhs, w_big[high, p].reshape(256, 2 * channels), preferred_element_type=F32
            )
        keep_hidden(y, first, frames, total)

    def part_of_own(y, i, start):
        low, high = y // 2, y % 2
        taps = [
            (
                patch[2 + p : 6 + p, i].reshape(4 * tokens, 128),
                w_big[high, p, 2 * (i - low) : 2 * (i - low) + 2].reshape(128, 2 * channels),
            )
            for p in range(3)
        ]
        lhs = jnp.concatenate([taps[0][0], taps[1][0]], axis=-1)
        rhs = jnp.concatenate([taps[0][1], taps[1][1]], axis=0)
        total = start + jnp.dot(lhs, rhs, preferred_element_type=F32)
        return total + jnp.dot(*taps[2], preferred_element_type=F32)

    patches(1, (0, 1))
    for y in (1, 2):
        partial[y - 1] = part_of_own(y, 1, bias)
    await_tokens(True)
    patches(0, (1,))
    patches(2, (0,))
    sums = jnp.zeros((1, 2 * channels), F32)
    squares = jnp.zeros((1, 2 * channels), F32)
    for y in (1, 2):
        values = part_of_own(y, 2 * (y - 1), partial[y - 1])
        keep_hidden(y, 2, 4, values)
        sums = sums + jnp.sum(values, axis=0, keepdims=True)
        squares = squares + jnp.sum(values * values, axis=0, keepdims=True)
    def product(value, matrix):
        terms = []
        for _ in range(3):
            term = value.astype(BF16)
            terms.append(term.astype(F32))
            value = value - terms[-1]
        terms = jnp.concatenate(terms + [jnp.zeros((5, value.shape[1]), F32)], axis=0).astype(BF16)
        result = jnp.dot(terms, matrix, preferred_element_type=F32)
        return result[0:1] + result[1:2] + result[2:3]

    folded = jnp.concatenate(
        [both[:, :channels] + both[:, channels:] for both in (sums, squares)], axis=-1
    )
    mine[...] = product(folded, gather[...])
    @pl.when(z > 1)
    def _():
        pl.semaphore_wait(know_x, 2)
    def direct_to(z0, where):
        @pl.when(late & where)
        def _():
            pl.semaphore_wait(know_plane.at[z0], 1)
            for to_x in range(RING_X):
                for to_ta in (1, 0):
                    slot = (last - z) * 8 + (to_x - x + RING_X) % RING_X * 2 + (to_ta + ta) % 2
                    pltpu.make_async_remote_copy(
                        mine, direct_in.at[slot], direct_send, direct_recv,
                        device_id={"ha": to_x * RING_Z + z0, "ta": to_ta}, device_id_type=MESH,
                    ).start()

    direct_to(0, z >= last - 1)
    plane = []
    for dx in (2, 1, 3, 0):
        for flip in (0, 1):
            if dx or flip:
                slot = 2 * dx + flip - 1
                plane.append(
                    pltpu.make_async_remote_copy(
                        mine, plane_in.at[slot], plane_send, plane_recv,
                        device_id=near(dx, 0, bool(flip)), device_id_type=MESH,
                    )
                )
    for copy in plane:
        copy.start()
    direct_to(0, z < last - 1)
    direct_to(1, True)
    pass_first(lower & (z >= 4), True)
    await_tokens(False)
    patches(0, (0, 1))
    patches(2, (0, 1))
    hidden_rows(0, 0, 6)
    direct_to(2, True)
    hidden_rows(3, 0, 6)
    hidden_rows(1, 0, 2)
    hidden_rows(2, 0, 2)
    for z0 in range(3, EARLY):
        direct_to(z0, True)
    total = mine[...]
    all_plane = pltpu.make_async_remote_copy(
        plane_in, plane_in, plane_send, plane_recv, device_id=near(0, 0, True), device_id_type=MESH
    )
    all_plane.wait_recv()
    for slot in range(plane_in.shape[0]):
        total = total + plane_in[slot]
    plane_sum[...] = total
    def ring_copy(d):
        return pltpu.make_async_remote_copy(
            plane_sum, ring_in.at[d - 1], ring_send, ring_recv,
            device_id=near(0, d, False), device_id_type=MESH,
        )

    def straight(d):
        return late & (z + d >= RING_Z) & (z + d < RING_Z + EARLY)

    pass_first(middle, z == RING_Z // 2)
    upper = (z > RING_Z // 2 + 1) & jnp.logical_not(late)

    @pl.when(upper)
    def _():
        pl.semaphore_wait(know_all, 1)

    for d in (*range(5, RING_Z), *range(1, 5)):

        @pl.when(jnp.logical_not(straight(d)) & ((d == 1) | (z + d >= RING_Z)))
        def _():
            ring_copy(d).start()
    @pl.when(early)
    def _():
        transform(2)
    @pl.when((z > 1) & (z < last) & jnp.logical_not(upper))
    def _():
        pl.semaphore_wait(know_all, 1)

    for z0 in range(2, EARLY):
        tell_plane(z0)
    for d in range(2, RING_Z):

        @pl.when(z + d <= last)
        def _():
            ring_copy(d).start()
    @pl.when(jnp.logical_not(early))
    def _():
        for p in range(3):
            transform(p)
    tokens_left()
    all_plane.wait_send()
    def ring_copies(number):
        return pltpu.make_async_remote_copy(
            ring_in.at[pl.ds(0, number)], ring_in.at[pl.ds(0, number)], ring_send, ring_recv,
            device_id=near(0, 1, False), device_id_type=MESH,
        )

    def direct_copies(number):
        return pltpu.make_async_remote_copy(
            direct_in.at[pl.ds(0, number)], direct_in.at[pl.ds(0, number)], direct_send, direct_recv,
            device_id=near(0, 1, False), device_id_type=MESH,
        )

    @pl.when(z < EARLY)
    def _():
        ring_copies(last - LATE).wait_recv()
    @pl.when(z < EARLY)
    def _():
        direct_copies(8 * LATE).wait_recv()

    @pl.when(z >= EARLY)
    def _():
        ring_copies(last).wait_recv()

    for slot in range(ring_in.shape[0]):
        total = total + ring_in[slot]
    rows = [direct_in[slot] for slot in range(8 * LATE)]
    while len(rows) > 1:
        rows = [sum(rows[at + 1 : at + 2], rows[at]) for at in range(0, len(rows), 2)]
    total = total + rows[0]
    count = n_ha * lax.axis_size("ta") * 4 * 2 * 2 * tokens * members
    shared = product(total * (1.0 / count), spread[...])
    mean, square = shared[:, :channels], shared[:, channels:]
    var = jnp.maximum(square - mean * mean, 0.0)
    scale = lax.rsqrt(var + EPS) * vectors[1].reshape(1, -1)
    stat_ref[0:1] = 0.5 * scale
    stat_ref[1:2] = 0.5 * (vectors[2].reshape(1, -1) - mean * scale)

    @pl.when(late)
    def _():
        ring_copies(last - EARLY).wait_send()
        direct_copies(8 * EARLY).wait_send()

    @pl.when(jnp.logical_not(late))
    def _():
        ring_copies(last).wait_send()


def decode_kernel(
    h_ref, stat_ref, main_ref, rest_ref, out_hbm,
    shifted, columns_wide, columns_rest, planes_wide, planes_rest, products, total, rows_f32, out, out_sem,
):
    ha, ta = lax.axis_index("ha"), lax.axis_index("ta")
    n_ha = lax.axis_size("ha")
    frames_in, rows_in, pieces, tokens, _ = h_ref.shape
    parts = pieces // 2
    channels = 128 * parts
    frames, rows = frames_in - 2, rows_in - 2
    wide = main_ref.shape[2]
    rest = channels - wide
    for f in range(frames_in):
        for part in range(parts):
            for y in range(rows_in):
                shifted[f, part, y, 0, 8 + tokens :] = jnp.zeros((8, 128), F32)
                shifted[f, part, y, 1, :8] = jnp.zeros((8, 128), F32)

    held = {}

    def activate(y, b):
        later = held.get("product", 0.0)
        for f in range(frames_in):
            inside = (ha * rows + y >= 1) & (ha * rows + y <= n_ha * rows)
            if f < 2:
                inside = inside & (ta > 0)
            for part in range(parts):
                lanes = slice(128 * part, 128 * part + 128)
                row_scale = jnp.where(inside, stat_ref[0:1, lanes], 0.0) + later
                row_shift = jnp.where(inside, stat_ref[1:2, lanes], 0.0)
                value = h_ref[f, y, b * parts + part] * row_scale + row_shift
                shifted[f, part, y, b, 8 : 8 + tokens] = value + value * jnp.tanh(value)

    def by_columns(y, k):
        def one(f, part):
            even, odd = [shifted.at[f, part, y, b] for b in (0, 1)]
            if k == 0:
                return odd[7 : 7 + tokens] - odd[8 : 8 + tokens]
            if k == 1:
                return even[8 : 8 + tokens] + odd[8 : 8 + tokens]
            if k == 2:
                return odd[8 : 8 + tokens] - even[8 : 8 + tokens]
            return even[8 : 8 + tokens] - even[9 : 9 + tokens]

        for f in range(frames_in):
            value = jnp.concatenate([one(f, part) for part in range(wide // 128)], axis=-1)
            columns_wide[k, f, y] = value.astype(BF16)
        for f in range(0, frames_in, 2):
            value = jnp.concatenate([one(f, parts - 1), one(f + 1, parts - 1)], axis=-1)
            columns_rest[k, f // 2, y] = value.astype(BF16)

    def by_rows(i, k):
        one, two = ((0, 2), (1, 2), (2, 1), (1, 3))[i]
        for columns, planes in ((columns_wide, planes_wide), (columns_rest, planes_rest)):
            if i == 1:
                planes[k % 2] = columns[k, :, one] + columns[k, :, two]
            else:
                planes[k % 2] = columns[k, :, one] - columns[k, :, two]

    ahead = {
        0: [(activate, 0, 0), (activate, 2, 0), (by_columns, 0, 1), (by_columns, 2, 1)],
        1: [(by_columns, 0, 2), (by_columns, 2, 2), (activate, 1, 1)],
        2: [(by_columns, 0, 3), (by_columns, 2, 3), (activate, 1, 0)],
        3: [(by_columns, 1, 0), (by_columns, 1, 1)],
        4: [(by_columns, 1, 2), (by_columns, 1, 3)],
        5: [(activate, 3, 1)],
        6: [(activate, 3, 0)],
        7: [(by_columns, 3, 0)],
        8: [(by_columns, 3, 1)],
        9: [(by_columns, 3, 2)],
        10: [(by_columns, 3, 3)],
    }
    for y in (0, 2):
        activate(y, 1)
    for y in (0, 2):
        by_columns(y, 0)
    by_rows(0, 0)
    bias = stat_ref[2:3]
    copies = []

    def done(y, b, f, part, value):
        hidden = h_ref[f + 2, y + 1, b * parts + part] + bias[:, 128 * part : 128 * part + 128]
        rows_f32[y, f, part, pl.ds(b, tokens, stride=2)] = value + hidden

    def send(y, f):
        for part in range(parts):
            out[f, y, :, 128 * part : 128 * part + 128] = rows_f32[y, f, part].astype(BF16)
        copies.append(pltpu.make_async_copy(out.at[f, y], out_hbm.at[f, y], out_sem))
        copies[-1].start()

    def combine(i, f):
        for part in range(parts):
            m0, m1, m2, m3 = [products[i % 2, k, f, part] for k in range(4)]
            for b, value in ((0, m0 + m1 + m2), (1, m1 - m2 - m3)):
                if i == 0:
                    total[0, b, f, part] = value
                elif i == 1:
                    total[0, b, f, part] = total[0, b, f, part] + value
                    total[1, b, f, part] = value
                elif i == 2:
                    done(0, b, f, part, total[0, b, f, part] + value)
                    total[1, b, f, part] = total[1, b, f, part] - value
        if i == 2:
            send(0, f)

    def last_even(f):
        for part in range(parts):
            m0, m1, m2 = [products[1, k, f, part] for k in range(3)]
            done(1, 0, f, part, total[1, 0, f, part] - (m0 + m1 + m2))
            total[1, 1, f, part] = total[1, 1, f, part] - (m1 - m2)

    def last_odd(f):
        for part in range(parts):
            done(1, 1, f, part, total[1, 1, f, part] + products[1, 3, f, part])
        send(1, f)

    for i in range(4):
        for k in range(4):
            at = 4 * i + k
            for make, one, two in ahead.get(at, ()):
                make(one, two)
            if at < 15:
                by_rows((at + 1) // 4, (at + 1) % 4)
            if i and k < 2:
                combine(i - 1, 2 * k)
                combine(i - 1, 2 * k + 1)
            if at == 15:
                for f in range(frames):
                    last_even(f)
            def plane(f):
                last = planes_rest[k % 2, f // 2, :, rest * (f % 2) : rest * (f % 2) + rest]
                return jnp.concatenate([planes_wide[k % 2, f], last], axis=-1)

            lhs = [jnp.concatenate([plane(f + p) for p in range(3)], axis=-1) for f in range(frames)]
            lhs = jnp.concatenate(lhs, axis=0)
            product = jnp.dot(lhs, main_ref[at], preferred_element_type=F32)
            held["product"] = 0.0 * product[0:1, 0:128]
            for part in range(wide // 128):
                products[i % 2, k, :, part] = product[:, 128 * part : 128 * part + 128].reshape(frames, tokens, 128)
            lhs = [
                jnp.concatenate([plane(t + p) for p in range(4)], axis=-1)
                for t in range(0, frames, 2)
            ]
            product = jnp.dot(jnp.concatenate(lhs, axis=0), rest_ref[at], preferred_element_type=F32)
            for f in range(frames):
                products[i % 2, k, f, wide // 128] = product[
                    f // 2 * tokens : (f // 2 + 1) * tokens, rest * (f % 2) : rest * (f % 2) + rest
                ]
    for f in range(frames):
        last_odd(f)
    pltpu.make_async_copy(out, out_hbm, out_sem).wait()


def keep(value):
    return pltpu.with_memory_space_constraint(value, pltpu.HBM)


def body(latent_tokens, w_in, b_in, gn_gain, gn_shift, w_mid, b_mid):
    half = latent_tokens.shape[1]
    channels = w_in.shape[-1]
    tokens = 2 * half
    wide = channels // 256 * 256
    rest = channels - wide
    parts = channels // 128
    vmem = pl.BlockSpec(memory_space=pltpu.VMEM)
    hbm = pl.BlockSpec(memory_space=pltpu.HBM)
    inputs = (latent_tokens, w_in.reshape(3, 3, -1, channels), b_in, gn_gain, gn_shift, b_mid, w_mid)
    prepared = pl.pallas_call(
        exchange_kernel,
        out_shape=(
            jax.ShapeDtypeStruct((6, 4, 2 * parts, tokens, 128), F32),
            jax.ShapeDtypeStruct((3, channels), F32),
            jax.ShapeDtypeStruct((16, 3 * channels, wide), BF16),
            jax.ShapeDtypeStruct((16, 4 * channels, 2 * rest), BF16),
        ),
        in_specs=[hbm] * len(inputs),
        out_specs=(vmem, vmem, vmem, vmem),
        scratch_shapes=[
            pltpu.VMEM(latent_tokens.shape, BF16),
            pltpu.VMEM((4, channels), F32),
            pltpu.VMEM((2, 2, half, 128), BF16),
            pltpu.VMEM((3, 2, 2, tokens, 128), BF16),
            pltpu.VMEM((8, 3, tokens, 128), BF16),
            pltpu.VMEM((2, 4 * tokens, 2 * channels), F32),
            pltpu.VMEM((2, 3, 4, 64, 2 * channels), BF16),
            pltpu.VMEM(w_mid.shape, BF16),
            pltpu.VMEM((1, 128), F32),
            pltpu.VMEM((7, 1, 128), F32),
            pltpu.VMEM((1, 128), F32),
            pltpu.VMEM((RING_Z - 1, 1, 128), F32),
            pltpu.VMEM((8 * max(LATE, EARLY), 1, 128), F32),
            pltpu.VMEM((2 * 384, 4 * 128), BF16),
            pltpu.VMEM((2 * channels, 128), BF16),
            pltpu.VMEM((128, 2 * channels), BF16),
            pltpu.SemaphoreType.DMA,
            pltpu.SemaphoreType.DMA,
            pltpu.SemaphoreType.DMA,
            pltpu.SemaphoreType.DMA((3,)),
            pltpu.SemaphoreType.DMA((5,)),
            pltpu.SemaphoreType.DMA((5,)),
            pltpu.SemaphoreType.DMA,
            pltpu.SemaphoreType.DMA,
            pltpu.SemaphoreType.DMA,
            pltpu.SemaphoreType.DMA,
            pltpu.SemaphoreType.DMA,
            pltpu.SemaphoreType.DMA,
            pltpu.SemaphoreType.REGULAR,
            pltpu.SemaphoreType.REGULAR,
            pltpu.SemaphoreType.REGULAR,
            pltpu.SemaphoreType.REGULAR((EARLY,)),
        ],
        compiler_params=pltpu.CompilerParams(
            collective_id=0, has_side_effects=True, vmem_limit_bytes=20 * 2**20
        ),
        name="exchange",
    )(*[keep(value) for value in inputs])
    return pl.pallas_call(
        decode_kernel,
        out_shape=jax.ShapeDtypeStruct((4, 2, 2 * tokens, channels), BF16),
        in_specs=[vmem, vmem, vmem, vmem],
        out_specs=hbm,
        scratch_shapes=[
            pltpu.VMEM((6, parts, 4, 2, tokens + 16, 128), F32),
            pltpu.VMEM((4, 6, 4, tokens, wide), BF16),
            pltpu.VMEM((4, 3, 4, tokens, 2 * rest), BF16),
            pltpu.VMEM((2, 6, tokens, wide), BF16),
            pltpu.VMEM((2, 3, tokens, 2 * rest), BF16),
            pltpu.VMEM((2, 4, 4, parts, tokens, 128), F32),
            pltpu.VMEM((2, 2, 4, parts, tokens, 128), F32),
            pltpu.VMEM((2, 4, parts, 2 * tokens, 128), F32),
            pltpu.VMEM((4, 2, 2 * tokens, channels), BF16),
            pltpu.SemaphoreType.DMA,
        ],
        compiler_params=pltpu.CompilerParams(vmem_limit_bytes=28 * 2**20),
        name="decode",
    )(*prepared)


def solution(mesh):
    return jax.shard_map(
        body,
        mesh=mesh,
        in_specs=(P("clip", ("ha", "ta"), None), P(), P(), P(), P(), P(), P()),
        out_specs=P(("clip", "ta"), "ha", None, None),
        check_vma=False,
    )
```

```python
import functools

import jax
import jax.numpy as jnp
from jax import lax
from jax.experimental import pallas as pl
from jax.experimental.pallas import tpu as pltpu
from jax.sharding import PartitionSpec as P

GROUPS = 32
RING_X = 4
RING_Z = 16
LATE = 4
EARLY = 4
EPS = 1e-06
MESH = pl.DeviceIdType.MESH
BF16 = jnp.bfloat16
F32 = jnp.float32


def exchange_kernel(
    tok_hbm, w_hbm, b_hbm, gain_hbm, shift_hbm, b_mid_hbm, mid_hbm,
    h_ref, stat_ref, main_ref, rest_ref,
    tok, vectors, packed, field, patch, partial, w_big, mid, mine, plane_in, plane_sum, ring_in, direct_in,
    sel, gather, spread,
    tok_sem, vec_sem, w_sem, mid_sem, send_sem, recv_sem,
    sums_send, plane_recv, ring_recv, direct_recv,
    know_x, know_all, know_first, know_plane,
):
    ha, ta = lax.axis_index("ha"), lax.axis_index("ta")
    n_ha = lax.axis_size("ha")
    x, z = ha // RING_Z, ha % RING_Z
    channels = vectors.shape[1]
    members = channels // GROUPS
    parts = channels // 128

    def near(dx, dz, flip):
        hx = (x + dx) % RING_X
        hz = (z + dz) % RING_Z
        return {"ha": hx * RING_Z + hz, "ta": 1 - ta if flip else ta}
    ring_in[...] = jnp.zeros_like(ring_in)
    direct_in[0 : 8 * LATE] = jnp.zeros_like(direct_in[0 : 8 * LATE])
    barrier = pltpu.get_barrier_semaphore()

    def greet(device):
        pl.semaphore_signal(barrier, inc=1, device_id=device, device_id_type=MESH)

    last = RING_Z - 1

    @pl.when(ha < n_ha - 1)
    def _():
        for t in (0, 1):
            greet({"ha": ha + 1, "ta": t})

    @pl.when(ha > 0)
    def _():
        for t in (0, 1):
            greet({"ha": ha - 1, "ta": t})

    for flip in (False, True):
        for dx in (1, RING_X - 1):
            greet(near(dx, 0, flip))
    greet(near(0, 0, True))

    @pl.when(z == 0)
    def _():
        greet(near(0, last, False))

    for d in range(2, last):

        @pl.when((z >= 1) & (z + d <= last))
        def _():
            greet(near(0, d, False))

    tok_copy = pltpu.make_async_copy(tok_hbm, tok, tok_sem)
    tok_copy.start()
    w_copies = [
        pltpu.make_async_copy(
            w_hbm,
            w_big.at[high, :, pl.ds(high, 3), pl.ds(16 * b, 48), pl.ds(channels * b, channels)],
            w_sem,
        )
        for high in (0, 1)
        for b in (0, 1)
    ]
    for copy in w_copies:
        copy.start()
    vector_copies = [
        pltpu.make_async_copy(ref, vectors.at[i], vec_sem)
        for i, ref in enumerate((b_hbm, gain_hbm, shift_hbm, b_mid_hbm))
    ]
    for copy in vector_copies:
        copy.start()

    wide = main_ref.shape[2]
    rest = channels - wide

    def fetch(p):
        return pltpu.make_async_copy(mid_hbm.at[p], mid.at[p], mid_sem.at[p])

    for p in range(3):
        fetch(p).start()

    def bank(tap_0, tap_1, tap_2):
        ends = tap_0 + tap_2
        return tap_0, 0.5 * (ends + tap_1), 0.5 * (ends - tap_1), tap_2

    def transform(p):
        fetch(p).wait()

        def rows(moved, step, carry):
            at = pl.multiple_of(step * 16, 16)
            for part in range(parts):
                lanes = slice(128 * part, 128 * part + 128)
                taps = [[mid[p, q, r, pl.ds(at, 16), lanes].astype(F32) for r in range(3)] for q in range(3)]
                by_row = [bank(*[taps[q][r] for q in range(3)]) for r in range(3)]
                for i in range(4):
                    for k, value in enumerate(bank(*[by_row[r][i] for r in range(3)])):
                        value = value.astype(BF16)
                        if 128 * part >= wide:
                            rest_ref[4 * i + k, pl.ds(at + p * channels, 16), :rest] = value
                            rest_ref[4 * i + k, pl.ds(at + (p + 1) * channels, 16), rest:] = value
                        elif moved and i and k == 2:
                            for other in (0, 3):
                                main_ref[4 * i + other, pl.ds(at + 3 * channels - wide, 16), lanes] = value
                        else:
                            main_ref[4 * i + k, pl.ds(at + p * channels, 16), lanes] = value
            return carry

        end = wide // 16 if p == 2 else channels // 16
        lax.fori_loop(0, end, functools.partial(rows, False), 0)
        if p == 2:
            lax.fori_loop(end, channels // 16, functools.partial(rows, True), 0)

    early = z < 2
    lower = z < RING_Z // 2

    @pl.when(early)
    def _():
        transform(0)

    first = (ha == 0) & (ta == 0)

    @pl.when(early & jnp.logical_not(first))
    def _():
        transform(1)
    tok_copy.wait()
    lanes = tok.shape[2] // 2
    for a in (0, 1):
        for h in (0, 1):
            packed[a, h] = jnp.concatenate(
                [tok[4 * h + f, :, a * lanes : (a + 1) * lanes].astype(F32) for f in range(4)], axis=-1
            ).astype(BF16)
    half = packed.shape[2]
    own = pl.ds(ta * half, half)
    expected = (
        5
        + jnp.where(ha > 0, 2, 0)
        + jnp.where(ha < n_ha - 1, 2, 0)
        + jnp.maximum(z - 2, 0)
        + jnp.where(z == last, 1, 0)
    )
    pl.semaphore_wait(barrier, expected)
    def tokens_copy(place, a, to_ha, to_ta, arrival):
        frames = pl.ds(0, 2) if to_ta else pl.ds(1, 1)
        of = pl.ds(0, 2) if to_ta else pl.ds(0, 1)
        if a is None:
            src, dst = packed.at[:, of], field.at[place, :, frames, own]
        else:
            src, dst = packed.at[a, of], field.at[place, a, frames, own]
        return pltpu.make_async_remote_copy(
            src, dst, send_sem, recv_sem.at[arrival],
            device_id={"ha": to_ha, "ta": to_ta}, device_id_type=MESH,
        )

    def send_tokens(urgent):
        @pl.when(ha < n_ha - 1)
        def _():
            for t in (1, 0):
                tokens_copy(0, int(urgent), ha + 1, t, 1 if urgent else 2).start()

        @pl.when(ha > 0)
        def _():
            for t in (1, 0):
                tokens_copy(2, 1 - int(urgent), ha - 1, t, 1 if urgent else 2).start()

        if urgent:
            for t in (1, 0):

                @pl.when(ta == 1 - t)
                def _():
                    tokens_copy(1, None, ha, t, 0).start()

    inner = (ha > 0) & (ha < n_ha - 1)

    def await_tokens(urgent):
        for to_ta in (0, 1):
            frames = pl.ds(0, 2) if to_ta else pl.ds(1, 1)

            def arrived(ref, arrival):
                pltpu.make_async_remote_copy(
                    ref, ref, send_sem, recv_sem.at[arrival],
                    device_id={"ha": ha, "ta": 1 - ta}, device_id_type=MESH,
                ).wait_recv()

            if urgent is None:

                @pl.when(ta == to_ta)
                def _():
                    arrived(field.at[1, :, frames, pl.ds((1 - to_ta) * half, half)], 0)

            else:

                @pl.when((ta == to_ta) & inner)
                def _():
                    arrived(field.at[0, :, frames], 1 if urgent else 2)

                @pl.when((ta == to_ta) & jnp.logical_not(inner))
                def _():
                    arrived(field.at[0, 0, frames], 1 if urgent else 2)

    def tokens_left():
        for to_ta, blocks, where in ((1, 16, inner), (0, 14, inner)) + tuple(
            (t, n, jnp.logical_not(inner)) for t, n in ((1, 10), (0, 8))
        ):

            @pl.when(where & (ta == 1 - to_ta))
            def _():
                gone = patch.at[pl.ds(0, blocks // 2), 0]
                pltpu.make_async_remote_copy(
                    gone, gone, send_sem, recv_sem.at[0],
                    device_id={"ha": ha, "ta": 1 - ta}, device_id_type=MESH,
                ).wait_send()

    def tell(sem, device):
        pl.semaphore_signal(sem, inc=1, device_id=device, device_id_type=MESH)

    @pl.when(z == last)
    def _():
        for d in range(1, 1 + EARLY):
            tell(know_all, near(0, d, False))

    send_tokens(True)

    tell(know_x, near(1, 0, False))
    tell(know_x, near(RING_X - 1, 0, False))

    def pass_first(where, onwards):
        @pl.when(where)
        def _():
            pl.semaphore_wait(know_first, 1)

        @pl.when(where & onwards)
        def _():
            tell(know_first, near(0, 1, False))

    @pl.when(z == 1)
    def _():
        tell(know_first, near(0, 1, False))

    middle = (z == RING_Z // 2) | (z == RING_Z // 2 + 1)

    @pl.when(z == last)
    def _():
        for d in range(1 + EARLY, RING_Z):
            tell(know_all, near(0, d, False))
    @pl.when(ta == 0)
    def _():
        field[:, :, 0] = jnp.zeros_like(field[:, :, 0])
        field[1, :, 1, own] = packed[:, 0]

    @pl.when(ta == 1)
    def _():
        field[1, :, :, own] = packed[...]

    @pl.when(ha == 0)
    def _():
        field[0] = jnp.zeros_like(field[0])

    @pl.when(ha == n_ha - 1)
    def _():
        field[2] = jnp.zeros_like(field[2])

    for high in (0, 1):
        w_big[high, :, 3 * (1 - high)] = jnp.zeros_like(w_big[high, :, 0])
        for p in range(3):
            for q in range(3):
                w_big[high, p, high + q, 48:64, :channels] = jnp.zeros((16, channels), BF16)
                w_big[high, p, high + q, 0:16, channels:] = jnp.zeros((16, channels), BF16)
    for i in range(16):
        rest_ref[i, 3 * channels :, :rest] = jnp.zeros((channels, rest), BF16)
        rest_ref[i, :channels, rest:] = jnp.zeros((channels, rest), BF16)
    sel[...] = jnp.zeros_like(sel)
    k = lax.broadcasted_iota(jnp.int32, (lanes, 128), 0)
    n = lax.broadcasted_iota(jnp.int32, (lanes, 128), 1)
    for a in (0, 1):
        for step in range(3):
            column = 2 * step + k // 16 - 1
            block = (n // 64 == a) & (k % 16 == n % 16) & ((n // 16) % 4 == column)
            block = jnp.where(block, 1.0, 0.0).astype(BF16)
            for f in range(4):
                sel[384 * a + 128 * step + lanes * f : 384 * a + 128 * step + lanes * (f + 1), 128 * f : 128 * f + 128] = block
    k = lax.broadcasted_iota(jnp.int32, gather.shape, 0)
    n = lax.broadcasted_iota(jnp.int32, gather.shape, 1)
    gather[...] = jnp.where((k // members == n % GROUPS) & (n < 2 * GROUPS), 1.0, 0.0).astype(BF16)
    k = lax.broadcasted_iota(jnp.int32, spread.shape, 0)
    n = lax.broadcasted_iota(jnp.int32, spread.shape, 1)
    spread[...] = jnp.where((n // members == k % GROUPS) & (k < 2 * GROUPS), 1.0, 0.0).astype(BF16)
    pltpu.make_async_copy(vectors, vectors, vec_sem).wait()
    stat_ref[2:3] = vectors[3].reshape(1, -1)
    spread_over = w_big.at[:, :, pl.ds(0, 3), pl.ds(0, 48)]
    pltpu.make_async_copy(spread_over, spread_over, w_sem).wait()
    send_tokens(False)

    @pl.when(first)
    def _():
        transform(1)
    late = z >= RING_Z - LATE

    def tell_plane(z0):
        @pl.when(z == z0)
        def _():
            for to in range(RING_Z - LATE, RING_Z):
                tell(know_plane.at[z0], {"ha": x * RING_Z + to, "ta": ta})

    @pl.when(z <= 1)
    def _():
        pl.semaphore_wait(know_x, 2)
        pl.semaphore_wait(know_all, 1)

    tell_plane(0)
    tell_plane(1)
    pass_first((z == 2) | (z == 3), True)
    await_tokens(None)
    tokens = field.shape[3]
    row = lax.broadcasted_iota(jnp.int32, (tokens, 128), 0)

    def patches(i, sides):
        stack = []
        for h in (0, 1):
            pieces = []
            for a in sides:
                now = field[i, a, h].astype(F32)
                pieces.append(jnp.where(row == 0, 0.0, pltpu.roll(now, 1, 0)))
                pieces.append(now)
                pieces.append(jnp.where(row == tokens - 1, 0.0, pltpu.roll(now, tokens - 1, 0)))
            stack.append(jnp.concatenate(pieces, axis=-1).astype(BF16))
        chosen = sel[384 * sides[0] : 384 * (sides[-1] + 1)]
        moved = jnp.dot(jnp.concatenate(stack, axis=0), chosen, preferred_element_type=F32).astype(BF16)
        for h in (0, 1):
            for f in range(4):
                patch[4 * h + f, i] = moved[h * tokens : (h + 1) * tokens, 128 * f : 128 * f + 128]

    bias = vectors[0].reshape(1, -1)
    bias = jnp.concatenate([bias, bias], axis=-1)

    def keep_hidden(y, first, frames, total):
        for n in range(2 * parts):
            part = total[:, 128 * n : 128 * n + 128].astype(BF16).astype(F32)
            h_ref[first : first + frames, y, n] = part.reshape(frames, tokens, 128)

    def hidden_rows(y, first, frames):
        low, high = y // 2, y % 2
        total = bias
        for p in range(3):
            lhs = [
                patch[first + p : first + p + frames, i].reshape(frames * tokens, 128) for i in (low, low + 1)
            ]
            lhs = jnp.concatenate(lhs, axis=-1)
            total = total + jnp.dot(
                lhs, w_big[high, p].reshape(256, 2 * channels), preferred_element_type=F32
            )
        keep_hidden(y, first, frames, total)

    def part_of_own(y, i, start):
        low, high = y // 2, y % 2
        taps = [
            (
                patch[2 + p : 6 + p, i].reshape(4 * tokens, 128),
                w_big[high, p, 2 * (i - low) : 2 * (i - low) + 2].reshape(128, 2 * channels),
            )
            for p in range(3)
        ]
        lhs = jnp.concatenate([taps[0][0], taps[1][0]], axis=-1)
        rhs = jnp.concatenate([taps[0][1], taps[1][1]], axis=0)
        total = start + jnp.dot(lhs, rhs, preferred_element_type=F32)
        return total + jnp.dot(*taps[2], preferred_element_type=F32)

    patches(1, (0, 1))
    for y in (1, 2):
        partial[y - 1] = part_of_own(y, 1, bias)
    await_tokens(True)
    patches(0, (1,))
    patches(2, (0,))
    sums = jnp.zeros((1, 2 * channels), F32)
    squares = jnp.zeros((1, 2 * channels), F32)
    for y in (1, 2):
        values = part_of_own(y, 2 * (y - 1), partial[y - 1])
        keep_hidden(y, 2, 4, values)
        sums = sums + jnp.sum(values, axis=0, keepdims=True)
        squares = squares + jnp.sum(values * values, axis=0, keepdims=True)
    def product(values, matrix):
        terms = []
        for value in values:
            for _ in range(3):
                term = value.astype(BF16)
                terms.append(term.astype(F32))
                value = value - terms[-1]
        terms = jnp.concatenate(terms + [jnp.zeros((2, values[0].shape[1]), F32)], axis=0).astype(BF16)
        result = jnp.dot(terms, matrix, preferred_element_type=F32)
        return [result[at : at + 1] + result[at + 1 : at + 2] + result[at + 2 : at + 3] for at in (0, 3)]

    folded = [both[:, :channels] + both[:, channels:] for both in (sums, squares)]
    of_sums = lax.broadcasted_iota(jnp.int32, (1, 128), 1) < GROUPS
    mine[...] = jnp.where(of_sums, *product(folded, gather[...]))
    @pl.when(z > 1)
    def _():
        pl.semaphore_wait(know_x, 2)
    def direct_to(z0, where):
        @pl.when(late & where)
        def _():
            pl.semaphore_wait(know_plane.at[z0], 1)
            for to_x in range(RING_X):
                for to_ta in (1, 0):
                    slot = (last - z) * 8 + (to_x - x + RING_X) % RING_X * 2 + (to_ta + ta) % 2
                    pltpu.make_async_remote_copy(
                        mine, direct_in.at[slot], sums_send, direct_recv,
                        device_id={"ha": to_x * RING_Z + z0, "ta": to_ta}, device_id_type=MESH,
                    ).start()

    direct_to(0, z >= last - 1)
    plane = []
    for dx in (2, 1, 3, 0):
        for flip in (0, 1):
            if dx or flip:
                slot = 2 * dx + flip - 1
                plane.append(
                    pltpu.make_async_remote_copy(
                        mine, plane_in.at[slot], sums_send, plane_recv,
                        device_id=near(dx, 0, bool(flip)), device_id_type=MESH,
                    )
                )
    for copy in plane:
        copy.start()
    direct_to(0, z < last - 1)
    direct_to(1, True)
    pass_first(lower & (z >= 4), True)
    await_tokens(False)
    patches(0, (0, 1))
    patches(2, (0, 1))
    hidden_rows(0, 0, 6)
    direct_to(2, True)
    hidden_rows(3, 0, 6)
    hidden_rows(1, 0, 2)
    hidden_rows(2, 0, 2)
    for z0 in range(3, EARLY):
        direct_to(z0, True)
    total = mine[...]
    all_plane = pltpu.make_async_remote_copy(
        plane_in, plane_in, sums_send, plane_recv, device_id=near(0, 0, True), device_id_type=MESH
    )
    all_plane.wait_recv()
    for slot in range(plane_in.shape[0]):
        total = total + plane_in[slot]
    plane_sum[...] = total
    def ring_copy(d):
        return pltpu.make_async_remote_copy(
            plane_sum, ring_in.at[d - 1], sums_send, ring_recv,
            device_id=near(0, d, False), device_id_type=MESH,
        )

    def straight(d):
        return late & (z + d >= RING_Z) & (z + d < RING_Z + EARLY)

    pass_first(middle, z == RING_Z // 2)
    upper = (z > RING_Z // 2 + 1) & jnp.logical_not(late)

    @pl.when(upper)
    def _():
        pl.semaphore_wait(know_all, 1)

    for d in (*range(5, RING_Z), *range(1, 5)):

        @pl.when(jnp.logical_not(straight(d)) & ((d == 1) | (z + d >= RING_Z)))
        def _():
            ring_copy(d).start()
    @pl.when(early)
    def _():
        transform(2)
    @pl.when((z > 1) & (z < last) & jnp.logical_not(upper))
    def _():
        pl.semaphore_wait(know_all, 1)

    for z0 in range(2, EARLY):
        tell_plane(z0)
    for d in range(2, RING_Z):

        @pl.when(z + d <= last)
        def _():
            ring_copy(d).start()
    @pl.when(jnp.logical_not(early))
    def _():
        for p in range(3):
            transform(p)
    tokens_left()
    def ring_copies(number):
        return pltpu.make_async_remote_copy(
            ring_in.at[pl.ds(0, number)], ring_in.at[pl.ds(0, number)], sums_send, ring_recv,
            device_id=near(0, 1, False), device_id_type=MESH,
        )

    def direct_copies(number):
        return pltpu.make_async_remote_copy(
            direct_in.at[pl.ds(0, number)], direct_in.at[pl.ds(0, number)], sums_send, direct_recv,
            device_id=near(0, 1, False), device_id_type=MESH,
        )

    @pl.when(z < EARLY)
    def _():
        ring_copies(last - LATE).wait_recv()
    @pl.when(z < EARLY)
    def _():
        direct_copies(8 * LATE).wait_recv()

    @pl.when(z >= EARLY)
    def _():
        ring_copies(last).wait_recv()

    for slot in range(ring_in.shape[0]):
        total = total + ring_in[slot]
    rows = [direct_in[slot] for slot in range(8 * LATE)]
    while len(rows) > 1:
        rows = [sum(rows[at + 1 : at + 2], rows[at]) for at in range(0, len(rows), 2)]
    total = total + rows[0]
    count = n_ha * lax.axis_size("ta") * 4 * 2 * 2 * tokens * members
    total = total * (1.0 / count)
    mean, square = product((jnp.where(of_sums, total, 0.0), jnp.where(of_sums, 0.0, total)), spread[...])
    var = jnp.maximum(square - mean * mean, 0.0)
    scale = lax.rsqrt(var + EPS) * vectors[1].reshape(1, -1)
    stat_ref[0:1] = 0.5 * scale
    stat_ref[1:2] = 0.5 * (vectors[2].reshape(1, -1) - mean * scale)

    by_late = len(plane) + last - EARLY + 8 * EARLY

    @pl.when(late)
    def _():
        direct_copies(by_late).wait_send()

    @pl.when(jnp.logical_not(late))
    def _():
        direct_copies(len(plane) + last).wait_send()


def decode_kernel(
    h_ref, stat_ref, main_ref, rest_ref, out_hbm,
    shifted, columns_wide, columns_rest, planes_wide, planes_rest, products, total, rows_f32, out, out_sem,
):
    ha, ta = lax.axis_index("ha"), lax.axis_index("ta")
    n_ha = lax.axis_size("ha")
    frames_in, rows_in, pieces, tokens, _ = h_ref.shape
    parts = pieces // 2
    channels = 128 * parts
    frames, rows = frames_in - 2, rows_in - 2
    wide = main_ref.shape[2]
    rest = channels - wide
    for f in range(frames_in):
        for part in range(parts):
            for y in range(rows_in):
                shifted[f, part, y, 0, 8 + tokens :] = jnp.zeros((8, 128), F32)
                shifted[f, part, y, 1, :8] = jnp.zeros((8, 128), F32)

    held = {}

    def activate(y, b):
        later = held.get("product", 0.0)
        for f in range(frames_in):
            inside = (ha * rows + y >= 1) & (ha * rows + y <= n_ha * rows)
            if f < 2:
                inside = inside & (ta > 0)
            for part in range(parts):
                lanes = slice(128 * part, 128 * part + 128)
                row_scale = jnp.where(inside, stat_ref[0:1, lanes], 0.0) + later
                row_shift = jnp.where(inside, stat_ref[1:2, lanes], 0.0)
                value = h_ref[f, y, b * parts + part] * row_scale + row_shift
                shifted[f, part, y, b, 8 : 8 + tokens] = value + value * jnp.tanh(value)

    def by_columns(y, k):
        def one(f, part):
            even, odd = [shifted.at[f, part, y, b] for b in (0, 1)]
            if k == 0:
                return odd[7 : 7 + tokens] - odd[8 : 8 + tokens]
            if k == 1:
                return even[8 : 8 + tokens] + odd[8 : 8 + tokens]
            if k == 2:
                return odd[8 : 8 + tokens] - even[8 : 8 + tokens]
            return even[8 : 8 + tokens] - even[9 : 9 + tokens]

        for f in range(frames_in):
            value = jnp.concatenate([one(f, part) for part in range(wide // 128)], axis=-1)
            columns_wide[k, f, y] = value.astype(BF16)
        for f in range(0, frames_in, 2):
            value = jnp.concatenate([one(f, parts - 1), one(f + 1, parts - 1)], axis=-1)
            columns_rest[k, f // 2, y] = value.astype(BF16)

    order = [(i, k) for i in range(4) for k in ((1, 2, 0, 3) if i else range(4))]
    slot_of = {pair: step % 2 for step, pair in enumerate(order)}

    def by_rows(i, k):
        one, two = ((0, 2), (1, 2), (2, 1), (1, 3))[i]
        for columns, planes, slot in ((columns_wide, planes_wide, slot_of[i, k]), (columns_rest, planes_rest, k)):
            if i == 1:
                planes[slot] = columns[k, :, one] + columns[k, :, two]
            else:
                planes[slot] = columns[k, :, one] - columns[k, :, two]

    ahead = {
        0: [(activate, 0, 0), (activate, 2, 0), (by_columns, 0, 1), (by_columns, 2, 1)],
        1: [(by_columns, 0, 2), (by_columns, 2, 2), (activate, 1, 1)],
        2: [(by_columns, 0, 3), (by_columns, 2, 3), (activate, 1, 0)],
        3: [(by_columns, 1, 0), (by_columns, 1, 1)],
        4: [(by_columns, 1, 2), (by_columns, 1, 3)],
        5: [(activate, 3, 1)],
        6: [(activate, 3, 0)],
        7: [(by_columns, 3, 0)],
        8: [(by_columns, 3, 1)],
        9: [(by_columns, 3, 2)],
        10: [(by_columns, 3, 3)],
    }
    for y in (0, 2):
        activate(y, 1)
    for y in (0, 2):
        by_columns(y, 0)
    by_rows(0, 0)
    bias = stat_ref[2:3]
    copies = []

    def done(y, b, f, part, value):
        hidden = h_ref[f + 2, y + 1, b * parts + part] + bias[:, 128 * part : 128 * part + 128]
        rows_f32[y, f, part, pl.ds(b, tokens, stride=2)] = value + hidden

    def send(y, f):
        for part in range(parts):
            out[f, y, :, 128 * part : 128 * part + 128] = rows_f32[y, f, part].astype(BF16)
        copies.append(pltpu.make_async_copy(out.at[f, y], out_hbm.at[f, y], out_sem))
        copies[-1].start()

    def combine(i, f):
        for part in range(parts):
            m0, m1, m2, m3 = [products[i % 2, k, f, part] for k in range(4)]
            for b, value in ((0, m0 + m1 + m2), (1, m1 - m2 - m3)):
                if i == 0:
                    total[0, b, f, part] = value
                elif i == 1:
                    total[0, b, f, part] = total[0, b, f, part] + value
                    total[1, b, f, part] = value
                elif i == 2:
                    done(0, b, f, part, total[0, b, f, part] + value)
                    total[1, b, f, part] = total[1, b, f, part] - value
        if i == 2:
            send(0, f)

    def last_even(f):
        for part in range(parts):
            m0, m1, m2 = [products[1, k, f, part] for k in range(3)]
            done(1, 0, f, part, total[1, 0, f, part] - (m0 + m1 + m2))
            total[1, 1, f, part] = total[1, 1, f, part] - (m1 - m2)

    def last_odd(f):
        for part in range(parts):
            done(1, 1, f, part, total[1, 1, f, part] + products[1, 3, f, part])
        send(1, f)

    for step, (i, k) in enumerate(order):
            at = 4 * i + k
            for make, one, two in ahead.get(step, ()):
                make(one, two)
            if step < 15:
                by_rows(*order[step + 1])
            if i and step % 4 < 2:
                combine(i - 1, 2 * (step % 4))
                combine(i - 1, 2 * (step % 4) + 1)
            if step == 15:
                for f in range(frames):
                    last_even(f)

            def last_channels(f, k):
                return planes_rest[k, f // 2, :, rest * (f % 2) : rest * (f % 2) + rest]

            def plane(f):
                return jnp.concatenate([planes_wide[slot_of[i, k], f], last_channels(f, k)], axis=-1)

            lhs = [[plane(f + p) for p in range(3)] for f in range(frames)]
            if i and k in (0, 3):
                lhs = [taps + [last_channels(f + 2, 2)] for f, taps in enumerate(lhs)]
            lhs = jnp.concatenate([jnp.concatenate(taps, axis=-1) for taps in lhs], axis=0)
            if i and k == 2:
                lhs = lhs[:, : 3 * channels - rest]
            product = jnp.dot(lhs, main_ref[at, : lhs.shape[1]], preferred_element_type=F32)
            held["product"] = 0.0 * product[0:1, 0:128]
            for part in range(wide // 128):
                products[i % 2, k, :, part] = product[:, 128 * part : 128 * part + 128].reshape(frames, tokens, 128)
            lhs = [
                jnp.concatenate([plane(t + p) for p in range(4)], axis=-1)
                for t in range(0, frames, 2)
            ]
            product = jnp.dot(jnp.concatenate(lhs, axis=0), rest_ref[at], preferred_element_type=F32)
            for f in range(frames):
                products[i % 2, k, f, wide // 128] = product[
                    f // 2 * tokens : (f // 2 + 1) * tokens, rest * (f % 2) : rest * (f % 2) + rest
                ]
    for f in range(frames):
        last_odd(f)
    pltpu.make_async_copy(out, out_hbm, out_sem).wait()


def keep(value):
    return pltpu.with_memory_space_constraint(value, pltpu.HBM)


def body(latent_tokens, w_in, b_in, gn_gain, gn_shift, w_mid, b_mid):
    half = latent_tokens.shape[1]
    channels = w_in.shape[-1]
    tokens = 2 * half
    wide = channels // 256 * 256
    rest = channels - wide
    parts = channels // 128
    vmem = pl.BlockSpec(memory_space=pltpu.VMEM)
    hbm = pl.BlockSpec(memory_space=pltpu.HBM)
    inputs = (latent_tokens, w_in.reshape(3, 3, -1, channels), b_in, gn_gain, gn_shift, b_mid, w_mid)
    prepared = pl.pallas_call(
        exchange_kernel,
        out_shape=(
            jax.ShapeDtypeStruct((6, 4, 2 * parts, tokens, 128), F32),
            jax.ShapeDtypeStruct((3, channels), F32),
            jax.ShapeDtypeStruct((16, 3 * channels + rest, wide), BF16),
            jax.ShapeDtypeStruct((16, 4 * channels, 2 * rest), BF16),
        ),
        in_specs=[hbm] * len(inputs),
        out_specs=(vmem, vmem, vmem, vmem),
        scratch_shapes=[
            pltpu.VMEM(latent_tokens.shape, BF16),
            pltpu.VMEM((4, channels), F32),
            pltpu.VMEM((2, 2, half, 128), BF16),
            pltpu.VMEM((3, 2, 2, tokens, 128), BF16),
            pltpu.VMEM((8, 3, tokens, 128), BF16),
            pltpu.VMEM((2, 4 * tokens, 2 * channels), F32),
            pltpu.VMEM((2, 3, 4, 64, 2 * channels), BF16),
            pltpu.VMEM(w_mid.shape, BF16),
            pltpu.VMEM((1, 128), F32),
            pltpu.VMEM((7, 1, 128), F32),
            pltpu.VMEM((1, 128), F32),
            pltpu.VMEM((RING_Z - 1, 1, 128), F32),
            pltpu.VMEM((max(8 * LATE, 2 * RING_X - 1 + RING_Z - 1 + 7 * EARLY), 1, 128), F32),
            pltpu.VMEM((2 * 384, 4 * 128), BF16),
            pltpu.VMEM((channels, 128), BF16),
            pltpu.VMEM((128, channels), BF16),
            pltpu.SemaphoreType.DMA,
            pltpu.SemaphoreType.DMA,
            pltpu.SemaphoreType.DMA,
            pltpu.SemaphoreType.DMA((3,)),
            pltpu.SemaphoreType.DMA,
            pltpu.SemaphoreType.DMA((3,)),
            pltpu.SemaphoreType.DMA,
            pltpu.SemaphoreType.DMA,
            pltpu.SemaphoreType.DMA,
            pltpu.SemaphoreType.DMA,
            pltpu.SemaphoreType.REGULAR,
            pltpu.SemaphoreType.REGULAR,
            pltpu.SemaphoreType.REGULAR,
            pltpu.SemaphoreType.REGULAR((EARLY,)),
        ],
        compiler_params=pltpu.CompilerParams(
            collective_id=0, has_side_effects=True, vmem_limit_bytes=18 * 2**20
        ),
        name="exchange",
    )(*[keep(value) for value in inputs])
    return pl.pallas_call(
        decode_kernel,
        out_shape=jax.ShapeDtypeStruct((4, 2, 2 * tokens, channels), BF16),
        in_specs=[vmem, vmem, vmem, vmem],
        out_specs=hbm,
        scratch_shapes=[
            pltpu.VMEM((6, parts, 4, 2, tokens + 16, 128), F32),
            pltpu.VMEM((4, 6, 4, tokens, wide), BF16),
            pltpu.VMEM((4, 3, 4, tokens, 2 * rest), BF16),
            pltpu.VMEM((2, 6, tokens, wide), BF16),
            pltpu.VMEM((4, 3, tokens, 2 * rest), BF16),
            pltpu.VMEM((2, 4, 4, parts, tokens, 128), F32),
            pltpu.VMEM((2, 2, 4, parts, tokens, 128), F32),
            pltpu.VMEM((2, 4, parts, 2 * tokens, 128), F32),
            pltpu.VMEM((4, 2, 2 * tokens, channels), BF16),
            pltpu.SemaphoreType.DMA,
        ],
        compiler_params=pltpu.CompilerParams(vmem_limit_bytes=22 * 2**20),
        name="decode",
    )(*prepared)


def solution(mesh):
    return jax.shard_map(
        body,
        mesh=mesh,
        in_specs=(P("clip", ("ha", "ta"), None), P(), P(), P(), P(), P(), P()),
        out_specs=P(("clip", "ta"), "ha", None, None),
        check_vma=False,
    )
```

```python
import functools

import jax
import jax.numpy as jnp
from jax import lax
from jax.experimental import pallas as pl
from jax.experimental.pallas import tpu as pltpu
from jax.sharding import PartitionSpec as P

GROUPS = 32
RING_X = 4
RING_Z = 16
LATE = 4
EARLY = 4
EPS = 1e-06
MESH = pl.DeviceIdType.MESH
BF16 = jnp.bfloat16
F32 = jnp.float32


def exchange_kernel(
    tok_hbm, w_hbm, b_hbm, gain_hbm, shift_hbm, b_mid_hbm, mid_hbm,
    h_ref, stat_ref, main_ref, rest_ref,
    tok, vectors, packed, field, patch, partial, w_big, mid, mine, plane_in, plane_sum, ring_in, direct_in,
    sel, gather, spread,
    tok_sem, vec_sem, w_sem, mid_sem, send_sem, recv_sem,
    sums_send, plane_recv, ring_recv, direct_recv,
    know_x, know_all, know_first, know_plane,
):
    ha, ta = lax.axis_index("ha"), lax.axis_index("ta")
    n_ha = lax.axis_size("ha")
    x, z = ha // RING_Z, ha % RING_Z
    channels = vectors.shape[1]
    members = channels // GROUPS
    parts = channels // 128

    def near(dx, dz, flip):
        hx = (x + dx) % RING_X
        hz = (z + dz) % RING_Z
        return {"ha": hx * RING_Z + hz, "ta": 1 - ta if flip else ta}
    ring_in[...] = jnp.zeros_like(ring_in)
    direct_in[0 : 8 * LATE] = jnp.zeros_like(direct_in[0 : 8 * LATE])
    barrier = pltpu.get_barrier_semaphore()

    def greet(device):
        pl.semaphore_signal(barrier, inc=1, device_id=device, device_id_type=MESH)

    last = RING_Z - 1

    @pl.when(ha < n_ha - 1)
    def _():
        for t in (0, 1):
            greet({"ha": ha + 1, "ta": t})

    @pl.when(ha > 0)
    def _():
        for t in (0, 1):
            greet({"ha": ha - 1, "ta": t})

    for flip in (False, True):
        for dx in (1, RING_X - 1):
            greet(near(dx, 0, flip))
    greet(near(0, 0, True))

    @pl.when(z == 0)
    def _():
        greet(near(0, last, False))

    for d in range(2, last):

        @pl.when((z >= 1) & (z + d <= last))
        def _():
            greet(near(0, d, False))

    tok_copy = pltpu.make_async_copy(tok_hbm, tok, tok_sem)
    tok_copy.start()
    w_copies = [
        pltpu.make_async_copy(
            w_hbm,
            w_big.at[high, :, pl.ds(high, 3), pl.ds(16 * b, 48), pl.ds(channels * b, channels)],
            w_sem,
        )
        for high in (0, 1)
        for b in (0, 1)
    ]
    for copy in w_copies:
        copy.start()
    vector_copies = [
        pltpu.make_async_copy(ref, vectors.at[i], vec_sem)
        for i, ref in enumerate((b_hbm, gain_hbm, shift_hbm, b_mid_hbm))
    ]
    for copy in vector_copies:
        copy.start()

    wide = main_ref.shape[2]
    rest = channels - wide

    def fetch(p):
        return pltpu.make_async_copy(mid_hbm.at[p], mid.at[p], mid_sem.at[p])

    for p in range(3):
        fetch(p).start()

    def bank(tap_0, tap_1, tap_2):
        ends = tap_0 + tap_2
        return tap_0, 0.5 * (ends + tap_1), 0.5 * (ends - tap_1), tap_2

    def transform(p):
        fetch(p).wait()

        def rows(moved, step, carry):
            at = pl.multiple_of(step * 16, 16)
            for part in range(parts):
                lanes = slice(128 * part, 128 * part + 128)
                taps = [[mid[p, q, r, pl.ds(at, 16), lanes].astype(F32) for r in range(3)] for q in range(3)]
                by_row = [bank(*[taps[q][r] for q in range(3)]) for r in range(3)]
                for i in range(4):
                    for k, value in enumerate(bank(*[by_row[r][i] for r in range(3)])):
                        value = value.astype(BF16)
                        if 128 * part >= wide:
                            rest_ref[4 * i + k, pl.ds(at + p * channels, 16), :rest] = value
                            rest_ref[4 * i + k, pl.ds(at + (p + 1) * channels, 16), rest:] = value
                        elif moved and i and k == 2:
                            for other in (0, 3):
                                main_ref[4 * i + other, pl.ds(at + 3 * channels - wide, 16), lanes] = value
                        else:
                            main_ref[4 * i + k, pl.ds(at + p * channels, 16), lanes] = value
            return carry

        end = wide // 16 if p == 2 else channels // 16
        lax.fori_loop(0, end, functools.partial(rows, False), 0)
        if p == 2:
            lax.fori_loop(end, channels // 16, functools.partial(rows, True), 0)

    early = z < 2
    lower = z < RING_Z // 2

    @pl.when(early)
    def _():
        transform(0)

    first = (ha == 0) & (ta == 0)

    @pl.when(early & jnp.logical_not(first))
    def _():
        transform(1)
    tok_copy.wait()
    lanes = tok.shape[2] // 2
    for a in (0, 1):
        for h in (0, 1):
            packed[a, h] = jnp.concatenate(
                [tok[4 * h + f, :, a * lanes : (a + 1) * lanes].astype(F32) for f in range(4)], axis=-1
            ).astype(BF16)
    half = packed.shape[2]
    own = pl.ds(ta * half, half)
    expected = (
        5
        + jnp.where(ha > 0, 2, 0)
        + jnp.where(ha < n_ha - 1, 2, 0)
        + jnp.maximum(z - 2, 0)
        + jnp.where(z == last, 1, 0)
    )
    pl.semaphore_wait(barrier, expected)
    def tokens_copy(place, a, to_ha, to_ta, arrival):
        frames = pl.ds(0, 2) if to_ta else pl.ds(1, 1)
        of = pl.ds(0, 2) if to_ta else pl.ds(0, 1)
        if a is None:
            src, dst = packed.at[:, of], field.at[place, :, frames, own]
        else:
            src, dst = packed.at[a, of], field.at[place, a, frames, own]
        return pltpu.make_async_remote_copy(
            src, dst, send_sem, recv_sem.at[arrival],
            device_id={"ha": to_ha, "ta": to_ta}, device_id_type=MESH,
        )

    def send_tokens(urgent):
        @pl.when(ha < n_ha - 1)
        def _():
            for t in (0, 1):
                tokens_copy(0, int(urgent), ha + 1, t, 1 if urgent else 2).start()

        @pl.when(ha > 0)
        def _():
            for t in (0, 1):
                tokens_copy(2, 1 - int(urgent), ha - 1, t, 1 if urgent else 2).start()

        if urgent:
            for t in (1, 0):

                @pl.when(ta == 1 - t)
                def _():
                    tokens_copy(1, None, ha, t, 0).start()

    inner = (ha > 0) & (ha < n_ha - 1)

    def await_tokens(urgent):
        for to_ta in (0, 1):
            frames = pl.ds(0, 2) if to_ta else pl.ds(1, 1)

            def arrived(ref, arrival):
                pltpu.make_async_remote_copy(
                    ref, ref, send_sem, recv_sem.at[arrival],
                    device_id={"ha": ha, "ta": 1 - ta}, device_id_type=MESH,
                ).wait_recv()

            if urgent is None:

                @pl.when(ta == to_ta)
                def _():
                    arrived(field.at[1, :, frames, pl.ds((1 - to_ta) * half, half)], 0)

            else:

                @pl.when((ta == to_ta) & inner)
                def _():
                    arrived(field.at[0, :, frames], 1 if urgent else 2)

                @pl.when((ta == to_ta) & jnp.logical_not(inner))
                def _():
                    arrived(field.at[0, 0, frames], 1 if urgent else 2)

    def tokens_left():
        for to_ta, blocks, where in ((1, 16, inner), (0, 14, inner)) + tuple(
            (t, n, jnp.logical_not(inner)) for t, n in ((1, 10), (0, 8))
        ):

            @pl.when(where & (ta == 1 - to_ta))
            def _():
                gone = patch.at[pl.ds(0, blocks // 2), 0]
                pltpu.make_async_remote_copy(
                    gone, gone, send_sem, recv_sem.at[0],
                    device_id={"ha": ha, "ta": 1 - ta}, device_id_type=MESH,
                ).wait_send()

    def tell(sem, device):
        pl.semaphore_signal(sem, inc=1, device_id=device, device_id_type=MESH)

    @pl.when(z == last)
    def _():
        for d in range(1, 1 + EARLY):
            tell(know_all, near(0, d, False))

    send_tokens(True)

    tell(know_x, near(1, 0, False))
    tell(know_x, near(RING_X - 1, 0, False))

    def pass_first(where, onwards):
        @pl.when(where)
        def _():
            pl.semaphore_wait(know_first, 1)

        @pl.when(where & onwards)
        def _():
            tell(know_first, near(0, 1, False))

    @pl.when(z == 1)
    def _():
        tell(know_first, near(0, 1, False))

    middle = (z == RING_Z // 2) | (z == RING_Z // 2 + 1)

    @pl.when(z == last)
    def _():
        for d in range(1 + EARLY, RING_Z):
            tell(know_all, near(0, d, False))
    @pl.when(ta == 0)
    def _():
        field[:, :, 0] = jnp.zeros_like(field[:, :, 0])
        field[1, :, 1, own] = packed[:, 0]

    @pl.when(ta == 1)
    def _():
        field[1, :, :, own] = packed[...]

    @pl.when(ha == 0)
    def _():
        field[0] = jnp.zeros_like(field[0])

    @pl.when(ha == n_ha - 1)
    def _():
        field[2] = jnp.zeros_like(field[2])

    for high in (0, 1):
        w_big[high, :, 3 * (1 - high)] = jnp.zeros_like(w_big[high, :, 0])
        for p in range(3):
            for q in range(3):
                w_big[high, p, high + q, 48:64, :channels] = jnp.zeros((16, channels), BF16)
                w_big[high, p, high + q, 0:16, channels:] = jnp.zeros((16, channels), BF16)
    for i in range(16):
        rest_ref[i, 3 * channels :, :rest] = jnp.zeros((channels, rest), BF16)
        rest_ref[i, :channels, rest:] = jnp.zeros((channels, rest), BF16)
    sel[...] = jnp.zeros_like(sel)
    k = lax.broadcasted_iota(jnp.int32, (lanes, 128), 0)
    n = lax.broadcasted_iota(jnp.int32, (lanes, 128), 1)
    for a in (0, 1):
        for step in range(3):
            column = 2 * step + k // 16 - 1
            block = (n // 64 == a) & (k % 16 == n % 16) & ((n // 16) % 4 == column)
            block = jnp.where(block, 1.0, 0.0).astype(BF16)
            for f in range(4):
                sel[384 * a + 128 * step + lanes * f : 384 * a + 128 * step + lanes * (f + 1), 128 * f : 128 * f + 128] = block
    k = lax.broadcasted_iota(jnp.int32, gather.shape, 0)
    n = lax.broadcasted_iota(jnp.int32, gather.shape, 1)
    gather[...] = jnp.where((k // members == n % GROUPS) & (n < 2 * GROUPS), 1.0, 0.0).astype(BF16)
    k = lax.broadcasted_iota(jnp.int32, spread.shape, 0)
    n = lax.broadcasted_iota(jnp.int32, spread.shape, 1)
    spread[...] = jnp.where((n // members == k % GROUPS) & (k < 2 * GROUPS), 1.0, 0.0).astype(BF16)
    pltpu.make_async_copy(vectors, vectors, vec_sem).wait()
    stat_ref[2:3] = vectors[3].reshape(1, -1)
    spread_over = w_big.at[:, :, pl.ds(0, 3), pl.ds(0, 48)]
    pltpu.make_async_copy(spread_over, spread_over, w_sem).wait()
    send_tokens(False)

    @pl.when(first)
    def _():
        transform(1)
    late = z >= RING_Z - LATE

    def tell_plane(z0):
        @pl.when(z == z0)
        def _():
            for to in range(RING_Z - LATE, RING_Z):
                tell(know_plane.at[z0], {"ha": x * RING_Z + to, "ta": ta})

    @pl.when(z <= 1)
    def _():
        pl.semaphore_wait(know_x, 2)
        pl.semaphore_wait(know_all, 1)

    tell_plane(0)
    tell_plane(1)
    pass_first((z == 2) | (z == 3), True)
    await_tokens(None)
    tokens = field.shape[3]
    row = lax.broadcasted_iota(jnp.int32, (tokens, 128), 0)

    def patches(i, sides):
        stack = []
        for h in (0, 1):
            pieces = []
            for a in sides:
                now = field[i, a, h].astype(F32)
                pieces.append(jnp.where(row == 0, 0.0, pltpu.roll(now, 1, 0)))
                pieces.append(now)
                pieces.append(jnp.where(row == tokens - 1, 0.0, pltpu.roll(now, tokens - 1, 0)))
            stack.append(jnp.concatenate(pieces, axis=-1).astype(BF16))
        chosen = sel[384 * sides[0] : 384 * (sides[-1] + 1)]
        moved = jnp.dot(jnp.concatenate(stack, axis=0), chosen, preferred_element_type=F32).astype(BF16)
        for h in (0, 1):
            for f in range(4):
                patch[4 * h + f, i] = moved[h * tokens : (h + 1) * tokens, 128 * f : 128 * f + 128]

    bias = vectors[0].reshape(1, -1)
    bias = jnp.concatenate([bias, bias], axis=-1)

    def keep_hidden(y, first, frames, total):
        for n in range(2 * parts):
            part = total[:, 128 * n : 128 * n + 128].astype(BF16).astype(F32)
            h_ref[first : first + frames, y, n] = part.reshape(frames, tokens, 128)

    def hidden_rows(y, first, frames):
        low, high = y // 2, y % 2
        total = bias
        for p in range(3):
            lhs = [
                patch[first + p : first + p + frames, i].reshape(frames * tokens, 128) for i in (low, low + 1)
            ]
            lhs = jnp.concatenate(lhs, axis=-1)
            total = total + jnp.dot(
                lhs, w_big[high, p].reshape(256, 2 * channels), preferred_element_type=F32
            )
        keep_hidden(y, first, frames, total)

    def part_of_own(y, i, start):
        low, high = y // 2, y % 2
        taps = [
            (
                patch[2 + p : 6 + p, i].reshape(4 * tokens, 128),
                w_big[high, p, 2 * (i - low) : 2 * (i - low) + 2].reshape(128, 2 * channels),
            )
            for p in range(3)
        ]
        lhs = jnp.concatenate([taps[0][0], taps[1][0]], axis=-1)
        rhs = jnp.concatenate([taps[0][1], taps[1][1]], axis=0)
        total = start + jnp.dot(lhs, rhs, preferred_element_type=F32)
        return total + jnp.dot(*taps[2], preferred_element_type=F32)

    patches(1, (0, 1))
    for y in (1, 2):
        partial[y - 1] = part_of_own(y, 1, bias)
    await_tokens(True)
    patches(0, (1,))
    patches(2, (0,))
    sums = jnp.zeros((1, 2 * channels), F32)
    squares = jnp.zeros((1, 2 * channels), F32)
    for y in (1, 2):
        values = part_of_own(y, 2 * (y - 1), partial[y - 1])
        keep_hidden(y, 2, 4, values)
        sums = sums + jnp.sum(values, axis=0, keepdims=True)
        squares = squares + jnp.sum(values * values, axis=0, keepdims=True)
    def product(values, matrix):
        terms = []
        for value in values:
            for _ in range(3):
                term = value.astype(BF16)
                terms.append(term.astype(F32))
                value = value - terms[-1]
        terms = jnp.concatenate(terms + [jnp.zeros((2, values[0].shape[1]), F32)], axis=0).astype(BF16)
        result = jnp.dot(terms, matrix, preferred_element_type=F32)
        return [result[at : at + 1] + result[at + 1 : at + 2] + result[at + 2 : at + 3] for at in (0, 3)]

    folded = [both[:, :channels] + both[:, channels:] for both in (sums, squares)]
    of_sums = lax.broadcasted_iota(jnp.int32, (1, 128), 1) < GROUPS
    mine[...] = jnp.where(of_sums, *product(folded, gather[...]))
    @pl.when(z > 1)
    def _():
        pl.semaphore_wait(know_x, 2)
    def direct_to(z0, where):
        @pl.when(late & where)
        def _():
            pl.semaphore_wait(know_plane.at[z0], 1)
            for to_x in range(RING_X):
                for to_ta in (1, 0):
                    slot = (last - z) * 8 + (to_x - x + RING_X) % RING_X * 2 + (to_ta + ta) % 2
                    pltpu.make_async_remote_copy(
                        mine, direct_in.at[slot], sums_send, direct_recv,
                        device_id={"ha": to_x * RING_Z + z0, "ta": to_ta}, device_id_type=MESH,
                    ).start()

    direct_to(0, z >= last - 1)
    plane = []
    for dx in (2, 1, 3, 0):
        for flip in (0, 1):
            if dx or flip:
                slot = 2 * dx + flip - 1
                plane.append(
                    pltpu.make_async_remote_copy(
                        mine, plane_in.at[slot], sums_send, plane_recv,
                        device_id=near(dx, 0, bool(flip)), device_id_type=MESH,
                    )
                )
    for copy in plane:
        copy.start()
    direct_to(0, z < last - 1)
    direct_to(1, True)
    pass_first(lower & (z >= 4), True)
    await_tokens(False)
    patches(0, (0, 1))
    patches(2, (0, 1))
    hidden_rows(0, 0, 6)
    direct_to(2, True)
    hidden_rows(3, 0, 6)
    hidden_rows(1, 0, 2)
    hidden_rows(2, 0, 2)
    for z0 in range(3, EARLY):
        direct_to(z0, True)
    total = mine[...]
    all_plane = pltpu.make_async_remote_copy(
        plane_in, plane_in, sums_send, plane_recv, device_id=near(0, 0, True), device_id_type=MESH
    )
    all_plane.wait_recv()
    for slot in range(plane_in.shape[0]):
        total = total + plane_in[slot]
    plane_sum[...] = total
    def ring_copy(d):
        return pltpu.make_async_remote_copy(
            plane_sum, ring_in.at[d - 1], sums_send, ring_recv,
            device_id=near(0, d, False), device_id_type=MESH,
        )

    def straight(d):
        return late & (z + d >= RING_Z) & (z + d < RING_Z + EARLY)

    pass_first(middle, z == RING_Z // 2)
    upper = (z > RING_Z // 2 + 1) & jnp.logical_not(late)

    @pl.when(upper)
    def _():
        pl.semaphore_wait(know_all, 1)

    for d in (*range(5, RING_Z), *range(1, 5)):

        @pl.when(jnp.logical_not(straight(d)) & ((d == 1) | (z + d >= RING_Z)))
        def _():
            ring_copy(d).start()
    @pl.when(early)
    def _():
        transform(2)
    @pl.when((z > 1) & (z < last) & jnp.logical_not(upper))
    def _():
        pl.semaphore_wait(know_all, 1)

    for z0 in range(2, EARLY):
        tell_plane(z0)
    for d in range(2, RING_Z):

        @pl.when(z + d <= last)
        def _():
            ring_copy(d).start()
    @pl.when(jnp.logical_not(early))
    def _():
        for p in range(3):
            transform(p)
    tokens_left()
    def ring_copies(number):
        return pltpu.make_async_remote_copy(
            ring_in.at[pl.ds(0, number)], ring_in.at[pl.ds(0, number)], sums_send, ring_recv,
            device_id=near(0, 1, False), device_id_type=MESH,
        )

    def direct_copies(number):
        return pltpu.make_async_remote_copy(
            direct_in.at[pl.ds(0, number)], direct_in.at[pl.ds(0, number)], sums_send, direct_recv,
            device_id=near(0, 1, False), device_id_type=MESH,
        )

    @pl.when(z < EARLY)
    def _():
        ring_copies(last - LATE).wait_recv()
    @pl.when(z < EARLY)
    def _():
        direct_copies(8 * LATE).wait_recv()

    @pl.when(z >= EARLY)
    def _():
        ring_copies(last).wait_recv()

    for slot in range(ring_in.shape[0]):
        total = total + ring_in[slot]
    rows = [direct_in[slot] for slot in range(8 * LATE)]
    while len(rows) > 1:
        rows = [sum(rows[at + 1 : at + 2], rows[at]) for at in range(0, len(rows), 2)]
    total = total + rows[0]
    count = n_ha * lax.axis_size("ta") * 4 * 2 * 2 * tokens * members
    total = total * (1.0 / count)
    mean, square = product((jnp.where(of_sums, total, 0.0), jnp.where(of_sums, 0.0, total)), spread[...])
    var = jnp.maximum(square - mean * mean, 0.0)
    scale = lax.rsqrt(var + EPS) * vectors[1].reshape(1, -1)
    stat_ref[0:1] = 0.5 * scale
    stat_ref[1:2] = 0.5 * (vectors[2].reshape(1, -1) - mean * scale)

    by_late = len(plane) + last - EARLY + 8 * EARLY

    @pl.when(late)
    def _():
        direct_copies(by_late).wait_send()

    @pl.when(jnp.logical_not(late))
    def _():
        direct_copies(len(plane) + last).wait_send()


def decode_kernel(
    h_ref, stat_ref, main_ref, rest_ref, out_hbm,
    shifted, columns_wide, columns_rest, planes_wide, planes_rest, products, total, rows_f32, out, out_sem,
):
    ha, ta = lax.axis_index("ha"), lax.axis_index("ta")
    n_ha = lax.axis_size("ha")
    frames_in, rows_in, pieces, tokens, _ = h_ref.shape
    parts = pieces // 2
    channels = 128 * parts
    frames, rows = frames_in - 2, rows_in - 2
    wide = main_ref.shape[2]
    rest = channels - wide
    for f in range(frames_in):
        for part in range(parts):
            for y in range(rows_in):
                shifted[f, part, y, 0, 8 + tokens :] = jnp.zeros((8, 128), F32)
                shifted[f, part, y, 1, :8] = jnp.zeros((8, 128), F32)

    held = {}

    def activate(y, b):
        later = held.get("product", 0.0)
        for f in range(frames_in):
            inside = (ha * rows + y >= 1) & (ha * rows + y <= n_ha * rows)
            if f < 2:
                inside = inside & (ta > 0)
            for part in range(parts):
                lanes = slice(128 * part, 128 * part + 128)
                row_scale = jnp.where(inside, stat_ref[0:1, lanes], 0.0) + later
                row_shift = jnp.where(inside, stat_ref[1:2, lanes], 0.0)
                value = h_ref[f, y, b * parts + part] * row_scale + row_shift
                shifted[f, part, y, b, 8 : 8 + tokens] = value + value * jnp.tanh(value)

    def by_columns(y, k):
        def one(f, part):
            even, odd = [shifted.at[f, part, y, b] for b in (0, 1)]
            if k == 0:
                return odd[7 : 7 + tokens] - odd[8 : 8 + tokens]
            if k == 1:
                return even[8 : 8 + tokens] + odd[8 : 8 + tokens]
            if k == 2:
                return odd[8 : 8 + tokens] - even[8 : 8 + tokens]
            return even[8 : 8 + tokens] - even[9 : 9 + tokens]

        for f in range(frames_in):
            value = jnp.concatenate([one(f, part) for part in range(wide // 128)], axis=-1)
            columns_wide[k, f, y] = value.astype(BF16)
        for f in range(0, frames_in, 2):
            value = jnp.concatenate([one(f, parts - 1), one(f + 1, parts - 1)], axis=-1)
            columns_rest[k, f // 2, y] = value.astype(BF16)

    order = [(i, k) for i in range(4) for k in ((1, 2, 0, 3) if i else range(4))]
    slot_of = {pair: step % 2 for step, pair in enumerate(order)}

    def by_rows(i, k):
        one, two = ((0, 2), (1, 2), (2, 1), (1, 3))[i]
        for columns, planes, slot in ((columns_wide, planes_wide, slot_of[i, k]), (columns_rest, planes_rest, k)):
            if i == 1:
                planes[slot] = columns[k, :, one] + columns[k, :, two]
            else:
                planes[slot] = columns[k, :, one] - columns[k, :, two]

    ahead = {
        0: [(activate, 0, 0), (activate, 2, 0), (by_columns, 0, 1), (by_columns, 2, 1)],
        1: [(by_columns, 0, 2), (by_columns, 2, 2), (activate, 1, 1)],
        2: [(by_columns, 0, 3), (by_columns, 2, 3), (activate, 1, 0)],
        3: [(by_columns, 1, 0), (by_columns, 1, 1)],
        4: [(by_columns, 1, 2), (by_columns, 1, 3)],
        5: [(activate, 3, 1)],
        6: [(activate, 3, 0)],
        7: [(by_columns, 3, 0)],
        8: [(by_columns, 3, 1)],
        9: [(by_columns, 3, 2)],
        10: [(by_columns, 3, 3)],
    }
    for y in (0, 2):
        activate(y, 1)
    for y in (0, 2):
        by_columns(y, 0)
    by_rows(0, 0)
    bias = stat_ref[2:3]
    copies = []

    def done(y, b, f, part, value):
        hidden = h_ref[f + 2, y + 1, b * parts + part] + bias[:, 128 * part : 128 * part + 128]
        rows_f32[y, f, part, pl.ds(b, tokens, stride=2)] = value + hidden

    def send(y, f):
        for part in range(parts):
            out[f, y, :, 128 * part : 128 * part + 128] = rows_f32[y, f, part].astype(BF16)
        copies.append(pltpu.make_async_copy(out.at[f, y], out_hbm.at[f, y], out_sem))
        copies[-1].start()

    def combine(i, f):
        for part in range(parts):
            m0, m1, m2, m3 = [products[i % 2, k, f, part] for k in range(4)]
            for b, value in ((0, m0 + m1 + m2), (1, m1 - m2 - m3)):
                if i == 0:
                    total[0, b, f, part] = value
                elif i == 1:
                    total[0, b, f, part] = total[0, b, f, part] + value
                    total[1, b, f, part] = value
                elif i == 2:
                    done(0, b, f, part, total[0, b, f, part] + value)
                    total[1, b, f, part] = total[1, b, f, part] - value
        if i == 2:
            send(0, f)

    def last_even(f):
        for part in range(parts):
            m0, m1, m2 = [products[1, k, f, part] for k in range(3)]
            done(1, 0, f, part, total[1, 0, f, part] - (m0 + m1 + m2))
            total[1, 1, f, part] = total[1, 1, f, part] - (m1 - m2)

    def last_odd(f):
        for part in range(parts):
            done(1, 1, f, part, total[1, 1, f, part] + products[1, 3, f, part])
        send(1, f)

    for step, (i, k) in enumerate(order):
            at = 4 * i + k
            for make, one, two in ahead.get(step, ()):
                make(one, two)
            if step < 15:
                by_rows(*order[step + 1])
            if i and step % 4 < 2:
                combine(i - 1, 2 * (step % 4))
                combine(i - 1, 2 * (step % 4) + 1)
            if step == 15:
                for f in range(frames):
                    last_even(f)

            def last_channels(f, k):
                return planes_rest[k, f // 2, :, rest * (f % 2) : rest * (f % 2) + rest]

            def plane(f):
                return jnp.concatenate([planes_wide[slot_of[i, k], f], last_channels(f, k)], axis=-1)

            lhs = [[plane(f + p) for p in range(3)] for f in range(frames)]
            if i and k in (0, 3):
                lhs = [taps + [last_channels(f + 2, 2)] for f, taps in enumerate(lhs)]
            lhs = jnp.concatenate([jnp.concatenate(taps, axis=-1) for taps in lhs], axis=0)
            if i and k == 2:
                lhs = lhs[:, : 3 * channels - rest]
            product = jnp.dot(lhs, main_ref[at, : lhs.shape[1]], preferred_element_type=F32)
            held["product"] = 0.0 * product[0:1, 0:128]
            for part in range(wide // 128):
                products[i % 2, k, :, part] = product[:, 128 * part : 128 * part + 128].reshape(frames, tokens, 128)
            lhs = [
                jnp.concatenate([plane(t + p) for p in range(4)], axis=-1)
                for t in range(0, frames, 2)
            ]
            product = jnp.dot(jnp.concatenate(lhs, axis=0), rest_ref[at], preferred_element_type=F32)
            for f in range(frames):
                products[i % 2, k, f, wide // 128] = product[
                    f // 2 * tokens : (f // 2 + 1) * tokens, rest * (f % 2) : rest * (f % 2) + rest
                ]
    for f in range(frames):
        last_odd(f)
    pltpu.make_async_copy(out, out_hbm, out_sem).wait()


def keep(value):
    return pltpu.with_memory_space_constraint(value, pltpu.HBM)


def body(latent_tokens, w_in, b_in, gn_gain, gn_shift, w_mid, b_mid):
    half = latent_tokens.shape[1]
    channels = w_in.shape[-1]
    tokens = 2 * half
    wide = channels // 256 * 256
    rest = channels - wide
    parts = channels // 128
    vmem = pl.BlockSpec(memory_space=pltpu.VMEM)
    hbm = pl.BlockSpec(memory_space=pltpu.HBM)
    inputs = (latent_tokens, w_in.reshape(3, 3, -1, channels), b_in, gn_gain, gn_shift, b_mid, w_mid)
    prepared = pl.pallas_call(
        exchange_kernel,
        out_shape=(
            jax.ShapeDtypeStruct((6, 4, 2 * parts, tokens, 128), F32),
            jax.ShapeDtypeStruct((3, channels), F32),
            jax.ShapeDtypeStruct((16, 3 * channels + rest, wide), BF16),
            jax.ShapeDtypeStruct((16, 4 * channels, 2 * rest), BF16),
        ),
        in_specs=[hbm] * len(inputs),
        out_specs=(vmem, vmem, vmem, vmem),
        scratch_shapes=[
            pltpu.VMEM(latent_tokens.shape, BF16),
            pltpu.VMEM((4, channels), F32),
            pltpu.VMEM((2, 2, half, 128), BF16),
            pltpu.VMEM((3, 2, 2, tokens, 128), BF16),
            pltpu.VMEM((8, 3, tokens, 128), BF16),
            pltpu.VMEM((2, 4 * tokens, 2 * channels), F32),
            pltpu.VMEM((2, 3, 4, 64, 2 * channels), BF16),
            pltpu.VMEM(w_mid.shape, BF16),
            pltpu.VMEM((1, 128), F32),
            pltpu.VMEM((7, 1, 128), F32),
            pltpu.VMEM((1, 128), F32),
            pltpu.VMEM((RING_Z - 1, 1, 128), F32),
            pltpu.VMEM((max(8 * LATE, 2 * RING_X - 1 + RING_Z - 1 + 7 * EARLY), 1, 128), F32),
            pltpu.VMEM((2 * 384, 4 * 128), BF16),
            pltpu.VMEM((channels, 128), BF16),
            pltpu.VMEM((128, channels), BF16),
            pltpu.SemaphoreType.DMA,
            pltpu.SemaphoreType.DMA,
            pltpu.SemaphoreType.DMA,
            pltpu.SemaphoreType.DMA((3,)),
            pltpu.SemaphoreType.DMA,
            pltpu.SemaphoreType.DMA((3,)),
            pltpu.SemaphoreType.DMA,
            pltpu.SemaphoreType.DMA,
            pltpu.SemaphoreType.DMA,
            pltpu.SemaphoreType.DMA,
            pltpu.SemaphoreType.REGULAR,
            pltpu.SemaphoreType.REGULAR,
            pltpu.SemaphoreType.REGULAR,
            pltpu.SemaphoreType.REGULAR((EARLY,)),
        ],
        compiler_params=pltpu.CompilerParams(
            collective_id=0, has_side_effects=True, vmem_limit_bytes=18 * 2**20
        ),
        name="exchange",
    )(*[keep(value) for value in inputs])
    return pl.pallas_call(
        decode_kernel,
        out_shape=jax.ShapeDtypeStruct((4, 2, 2 * tokens, channels), BF16),
        in_specs=[vmem, vmem, vmem, vmem],
        out_specs=hbm,
        scratch_shapes=[
            pltpu.VMEM((6, parts, 4, 2, tokens + 16, 128), F32),
            pltpu.VMEM((4, 6, 4, tokens, wide), BF16),
            pltpu.VMEM((4, 3, 4, tokens, 2 * rest), BF16),
            pltpu.VMEM((2, 6, tokens, wide), BF16),
            pltpu.VMEM((4, 3, tokens, 2 * rest), BF16),
            pltpu.VMEM((2, 4, 4, parts, tokens, 128), F32),
            pltpu.VMEM((2, 2, 4, parts, tokens, 128), F32),
            pltpu.VMEM((2, 4, parts, 2 * tokens, 128), F32),
            pltpu.VMEM((4, 2, 2 * tokens, channels), BF16),
            pltpu.SemaphoreType.DMA,
        ],
        compiler_params=pltpu.CompilerParams(vmem_limit_bytes=22 * 2**20),
        name="decode",
    )(*prepared)


def solution(mesh):
    return jax.shard_map(
        body,
        mesh=mesh,
        in_specs=(P("clip", ("ha", "ta"), None), P(), P(), P(), P(), P(), P()),
        out_specs=P(("clip", "ta"), "ha", None, None),
        check_vma=False,
    )
```

```python
import functools

import jax
import jax.numpy as jnp
from jax import lax
from jax.experimental import pallas as pl
from jax.experimental.pallas import tpu as pltpu
from jax.sharding import PartitionSpec as P

GROUPS = 32
RING_X = 4
RING_Z = 16
LATE = 4
EARLY = 4
EPS = 1e-06
MESH = pl.DeviceIdType.MESH
BF16 = jnp.bfloat16
F32 = jnp.float32


def exchange_kernel(
    tok_hbm, w_hbm, b_hbm, gain_hbm, shift_hbm, b_mid_hbm, mid_hbm,
    h_ref, stat_ref, main_ref, rest_ref,
    tok, vectors, packed, field, patch, partial, w_big, mid, mine, plane_in, plane_sum, ring_in, direct_in,
    sel, gather, spread,
    tok_sem, vec_sem, w_sem, mid_sem, send_sem, recv_sem,
    sums_send, plane_recv, ring_recv, direct_recv,
    know_x, know_all, know_first, know_plane,
):
    ha, ta = lax.axis_index("ha"), lax.axis_index("ta")
    n_ha = lax.axis_size("ha")
    x, z = ha // RING_Z, ha % RING_Z
    channels = vectors.shape[1]
    members = channels // GROUPS
    parts = channels // 128

    def near(dx, dz, flip):
        hx = (x + dx) % RING_X
        hz = (z + dz) % RING_Z
        return {"ha": hx * RING_Z + hz, "ta": 1 - ta if flip else ta}
    ring_in[...] = jnp.zeros_like(ring_in)
    direct_in[0 : 8 * LATE] = jnp.zeros_like(direct_in[0 : 8 * LATE])
    barrier = pltpu.get_barrier_semaphore()

    def greet(device):
        pl.semaphore_signal(barrier, inc=1, device_id=device, device_id_type=MESH)

    last = RING_Z - 1

    @pl.when(ha < n_ha - 1)
    def _():
        for t in (0, 1):
            greet({"ha": ha + 1, "ta": t})

    @pl.when(ha > 0)
    def _():
        for t in (0, 1):
            greet({"ha": ha - 1, "ta": t})

    for flip in (False, True):
        for dx in (1, RING_X - 1):
            greet(near(dx, 0, flip))
    greet(near(0, 0, True))

    @pl.when(z == 0)
    def _():
        greet(near(0, last, False))

    for d in range(2, last):

        @pl.when((z >= 1) & (z + d <= last))
        def _():
            greet(near(0, d, False))

    tok_copy = pltpu.make_async_copy(tok_hbm, tok, tok_sem)
    tok_copy.start()
    w_copies = [
        pltpu.make_async_copy(
            w_hbm,
            w_big.at[high, :, pl.ds(high, 3), pl.ds(16 * b, 48), pl.ds(channels * b, channels)],
            w_sem,
        )
        for high in (0, 1)
        for b in (0, 1)
    ]
    for copy in w_copies:
        copy.start()
    vector_copies = [
        pltpu.make_async_copy(ref, vectors.at[i], vec_sem)
        for i, ref in enumerate((b_hbm, gain_hbm, shift_hbm, b_mid_hbm))
    ]
    for copy in vector_copies:
        copy.start()

    wide = main_ref.shape[2]
    rest = channels - wide

    def fetch(p):
        return pltpu.make_async_copy(mid_hbm.at[p], mid.at[p], mid_sem.at[p])

    for p in range(3):
        fetch(p).start()

    def bank(tap_0, tap_1, tap_2):
        ends = tap_0 + tap_2
        return tap_0, 0.5 * (ends + tap_1), 0.5 * (ends - tap_1), tap_2

    def transform(p):
        fetch(p).wait()

        def rows(moved, step, carry):
            at = pl.multiple_of(step * 16, 16)
            for part in range(parts):
                lanes = slice(128 * part, 128 * part + 128)
                taps = [[mid[p, q, r, pl.ds(at, 16), lanes].astype(F32) for r in range(3)] for q in range(3)]
                by_row = [bank(*[taps[q][r] for q in range(3)]) for r in range(3)]
                for i in range(4):
                    for k, value in enumerate(bank(*[by_row[r][i] for r in range(3)])):
                        value = value.astype(BF16)
                        if 128 * part >= wide:
                            rest_ref[4 * i + k, pl.ds(at + p * channels, 16), :rest] = value
                            rest_ref[4 * i + k, pl.ds(at + (p + 1) * channels, 16), rest:] = value
                        elif moved and i and k == 2:
                            for other in (0, 3):
                                main_ref[4 * i + other, pl.ds(at + 3 * channels - wide, 16), lanes] = value
                        else:
                            main_ref[4 * i + k, pl.ds(at + p * channels, 16), lanes] = value
            return carry

        end = wide // 16 if p == 2 else channels // 16
        lax.fori_loop(0, end, functools.partial(rows, False), 0)
        if p == 2:
            lax.fori_loop(end, channels // 16, functools.partial(rows, True), 0)

    early = z < 2
    lower = z < RING_Z // 2

    @pl.when(early)
    def _():
        transform(0)

    first = (ha == 0) & (ta == 0)

    @pl.when(early & jnp.logical_not(first))
    def _():
        transform(1)
    tok_copy.wait()
    lanes = tok.shape[2] // 2
    for a in (0, 1):
        for h in (0, 1):
            packed[a, h] = jnp.concatenate(
                [tok[4 * h + f, :, a * lanes : (a + 1) * lanes].astype(F32) for f in range(4)], axis=-1
            ).astype(BF16)
    half = packed.shape[2]
    own = pl.ds(ta * half, half)
    expected = (
        5
        + jnp.where(ha > 0, 2, 0)
        + jnp.where(ha < n_ha - 1, 2, 0)
        + jnp.maximum(z - 2, 0)
        + jnp.where(z == last, 1, 0)
    )
    pl.semaphore_wait(barrier, expected)
    def tokens_copy(place, a, to_ha, to_ta, arrival):
        frames = pl.ds(0, 2) if to_ta else pl.ds(1, 1)
        of = pl.ds(0, 2) if to_ta else pl.ds(0, 1)
        if a is None:
            src, dst = packed.at[:, of], field.at[place, :, frames, own]
        else:
            src, dst = packed.at[a, of], field.at[place, a, frames, own]
        return pltpu.make_async_remote_copy(
            src, dst, send_sem, recv_sem.at[arrival],
            device_id={"ha": to_ha, "ta": to_ta}, device_id_type=MESH,
        )

    def send_tokens(urgent):
        @pl.when(ha < n_ha - 1)
        def _():
            for t in (0, 1):
                tokens_copy(0, int(urgent), ha + 1, t, 1 if urgent else 2).start()

        @pl.when(ha > 0)
        def _():
            for t in (0, 1):
                tokens_copy(2, 1 - int(urgent), ha - 1, t, 1 if urgent else 2).start()

        if urgent:
            for t in (1, 0):

                @pl.when(ta == 1 - t)
                def _():
                    tokens_copy(1, None, ha, t, 0).start()

    inner = (ha > 0) & (ha < n_ha - 1)

    def await_tokens(urgent):
        for to_ta in (0, 1):
            frames = pl.ds(0, 2) if to_ta else pl.ds(1, 1)

            def arrived(ref, arrival):
                pltpu.make_async_remote_copy(
                    ref, ref, send_sem, recv_sem.at[arrival],
                    device_id={"ha": ha, "ta": 1 - ta}, device_id_type=MESH,
                ).wait_recv()

            if urgent is None:

                @pl.when(ta == to_ta)
                def _():
                    arrived(field.at[1, :, frames, pl.ds((1 - to_ta) * half, half)], 0)

            else:

                @pl.when((ta == to_ta) & inner)
                def _():
                    arrived(field.at[0, :, frames], 1 if urgent else 2)

                @pl.when((ta == to_ta) & jnp.logical_not(inner))
                def _():
                    arrived(field.at[0, 0, frames], 1 if urgent else 2)

    def tokens_left():
        for to_ta, blocks, where in ((1, 16, inner), (0, 14, inner)) + tuple(
            (t, n, jnp.logical_not(inner)) for t, n in ((1, 10), (0, 8))
        ):

            @pl.when(where & (ta == 1 - to_ta))
            def _():
                gone = patch.at[pl.ds(0, blocks // 2), 0]
                pltpu.make_async_remote_copy(
                    gone, gone, send_sem, recv_sem.at[0],
                    device_id={"ha": ha, "ta": 1 - ta}, device_id_type=MESH,
                ).wait_send()

    def tell(sem, device):
        pl.semaphore_signal(sem, inc=1, device_id=device, device_id_type=MESH)

    @pl.when(z == last)
    def _():
        for d in range(1, 1 + EARLY):
            tell(know_all, near(0, d, False))

    def tell_across(where):
        @pl.when(where)
        def _():
            tell(know_x, near(1, 0, False))
            tell(know_x, near(RING_X - 1, 0, False))

    tell_across(z <= 1)
    send_tokens(True)

    tell_across(z > 1)

    def pass_first(where, onwards):
        @pl.when(where)
        def _():
            pl.semaphore_wait(know_first, 1)

        @pl.when(where & onwards)
        def _():
            tell(know_first, near(0, 1, False))

    @pl.when(z == 1)
    def _():
        tell(know_first, near(0, 1, False))

    middle = (z == RING_Z // 2) | (z == RING_Z // 2 + 1)

    @pl.when(z == last)
    def _():
        for d in range(1 + EARLY, RING_Z):
            tell(know_all, near(0, d, False))
    @pl.when(ta == 0)
    def _():
        field[:, :, 0] = jnp.zeros_like(field[:, :, 0])
        field[1, :, 1, own] = packed[:, 0]

    @pl.when(ta == 1)
    def _():
        field[1, :, :, own] = packed[...]

    @pl.when(ha == 0)
    def _():
        field[0] = jnp.zeros_like(field[0])

    @pl.when(ha == n_ha - 1)
    def _():
        field[2] = jnp.zeros_like(field[2])

    for high in (0, 1):
        w_big[high, :, 3 * (1 - high)] = jnp.zeros_like(w_big[high, :, 0])
        for p in range(3):
            for q in range(3):
                w_big[high, p, high + q, 48:64, :channels] = jnp.zeros((16, channels), BF16)
                w_big[high, p, high + q, 0:16, channels:] = jnp.zeros((16, channels), BF16)
    for i in range(16):
        rest_ref[i, 3 * channels :, :rest] = jnp.zeros((channels, rest), BF16)
        rest_ref[i, :channels, rest:] = jnp.zeros((channels, rest), BF16)
    sel[...] = jnp.zeros_like(sel)
    k = lax.broadcasted_iota(jnp.int32, (lanes, 128), 0)
    n = lax.broadcasted_iota(jnp.int32, (lanes, 128), 1)
    for a in (0, 1):
        for step in range(3):
            column = 2 * step + k // 16 - 1
            block = (n // 64 == a) & (k % 16 == n % 16) & ((n // 16) % 4 == column)
            block = jnp.where(block, 1.0, 0.0).astype(BF16)
            for f in range(4):
                sel[384 * a + 128 * step + lanes * f : 384 * a + 128 * step + lanes * (f + 1), 128 * f : 128 * f + 128] = block
    k = lax.broadcasted_iota(jnp.int32, gather.shape, 0)
    n = lax.broadcasted_iota(jnp.int32, gather.shape, 1)
    gather[...] = jnp.where((k // members == n % GROUPS) & (n < 2 * GROUPS), 1.0, 0.0).astype(BF16)
    k = lax.broadcasted_iota(jnp.int32, spread.shape, 0)
    n = lax.broadcasted_iota(jnp.int32, spread.shape, 1)
    spread[...] = jnp.where((n // members == k % GROUPS) & (k < 2 * GROUPS), 1.0, 0.0).astype(BF16)
    pltpu.make_async_copy(vectors, vectors, vec_sem).wait()
    stat_ref[2:3] = vectors[3].reshape(1, -1)
    spread_over = w_big.at[:, :, pl.ds(0, 3), pl.ds(0, 48)]
    pltpu.make_async_copy(spread_over, spread_over, w_sem).wait()
    send_tokens(False)

    @pl.when(first)
    def _():
        transform(1)
    late = z >= RING_Z - LATE

    def tell_plane(z0):
        @pl.when(z == z0)
        def _():
            for to in range(RING_Z - LATE, RING_Z):
                tell(know_plane.at[z0], {"ha": x * RING_Z + to, "ta": ta})

    @pl.when(z <= 1)
    def _():
        pl.semaphore_wait(know_x, 2)
        pl.semaphore_wait(know_all, 1)

    tell_plane(0)
    tell_plane(1)
    pass_first((z == 2) | (z == 3), True)
    await_tokens(None)
    tokens = field.shape[3]
    row = lax.broadcasted_iota(jnp.int32, (tokens, 128), 0)

    def patches(i, sides):
        stack = []
        for h in (0, 1):
            pieces = []
            for a in sides:
                now = field[i, a, h].astype(F32)
                pieces.append(jnp.where(row == 0, 0.0, pltpu.roll(now, 1, 0)))
                pieces.append(now)
                pieces.append(jnp.where(row == tokens - 1, 0.0, pltpu.roll(now, tokens - 1, 0)))
            stack.append(jnp.concatenate(pieces, axis=-1).astype(BF16))
        chosen = sel[384 * sides[0] : 384 * (sides[-1] + 1)]
        moved = jnp.dot(jnp.concatenate(stack, axis=0), chosen, preferred_element_type=F32).astype(BF16)
        for h in (0, 1):
            for f in range(4):
                patch[4 * h + f, i] = moved[h * tokens : (h + 1) * tokens, 128 * f : 128 * f + 128]

    bias = vectors[0].reshape(1, -1)
    bias = jnp.concatenate([bias, bias], axis=-1)

    def keep_hidden(y, first, frames, total):
        for n in range(2 * parts):
            part = total[:, 128 * n : 128 * n + 128].astype(BF16).astype(F32)
            h_ref[first : first + frames, y, n] = part.reshape(frames, tokens, 128)

    def hidden_rows(y, first, frames):
        low, high = y // 2, y % 2
        total = bias
        for p in range(3):
            lhs = [
                patch[first + p : first + p + frames, i].reshape(frames * tokens, 128) for i in (low, low + 1)
            ]
            lhs = jnp.concatenate(lhs, axis=-1)
            total = total + jnp.dot(
                lhs, w_big[high, p].reshape(256, 2 * channels), preferred_element_type=F32
            )
        keep_hidden(y, first, frames, total)

    def part_of_own(y, i, start):
        low, high = y // 2, y % 2
        taps = [
            (
                patch[2 + p : 6 + p, i].reshape(4 * tokens, 128),
                w_big[high, p, 2 * (i - low) : 2 * (i - low) + 2].reshape(128, 2 * channels),
            )
            for p in range(3)
        ]
        lhs = jnp.concatenate([taps[0][0], taps[1][0]], axis=-1)
        rhs = jnp.concatenate([taps[0][1], taps[1][1]], axis=0)
        total = start + jnp.dot(lhs, rhs, preferred_element_type=F32)
        return total + jnp.dot(*taps[2], preferred_element_type=F32)

    patches(1, (0, 1))
    for y in (1, 2):
        partial[y - 1] = part_of_own(y, 1, bias)
    await_tokens(True)
    patches(0, (1,))
    patches(2, (0,))
    sums = jnp.zeros((1, 2 * channels), F32)
    squares = jnp.zeros((1, 2 * channels), F32)
    for y in (1, 2):
        values = part_of_own(y, 2 * (y - 1), partial[y - 1])
        keep_hidden(y, 2, 4, values)
        sums = sums + jnp.sum(values, axis=0, keepdims=True)
        squares = squares + jnp.sum(values * values, axis=0, keepdims=True)
    def product(values, matrix):
        terms = []
        for value in values:
            for _ in range(3):
                term = value.astype(BF16)
                terms.append(term.astype(F32))
                value = value - terms[-1]
        terms = jnp.concatenate(terms + [jnp.zeros((2, values[0].shape[1]), F32)], axis=0).astype(BF16)
        result = jnp.dot(terms, matrix, preferred_element_type=F32)
        return [result[at : at + 1] + result[at + 1 : at + 2] + result[at + 2 : at + 3] for at in (0, 3)]

    folded = [both[:, :channels] + both[:, channels:] for both in (sums, squares)]
    of_sums = lax.broadcasted_iota(jnp.int32, (1, 128), 1) < GROUPS
    mine[...] = jnp.where(of_sums, *product(folded, gather[...]))
    @pl.when(z > 1)
    def _():
        pl.semaphore_wait(know_x, 2)
    def direct_to(z0, where):
        @pl.when(late & where)
        def _():
            pl.semaphore_wait(know_plane.at[z0], 1)
            for to_x in range(RING_X):
                for to_ta in (1, 0):
                    slot = (last - z) * 8 + (to_x - x + RING_X) % RING_X * 2 + (to_ta + ta) % 2
                    pltpu.make_async_remote_copy(
                        mine, direct_in.at[slot], sums_send, direct_recv,
                        device_id={"ha": to_x * RING_Z + z0, "ta": to_ta}, device_id_type=MESH,
                    ).start()

    direct_to(0, z >= last - 1)
    plane = []
    for dx in (2, 1, 3, 0):
        for flip in (0, 1):
            if dx or flip:
                slot = 2 * dx + flip - 1
                plane.append(
                    pltpu.make_async_remote_copy(
                        mine, plane_in.at[slot], sums_send, plane_recv,
                        device_id=near(dx, 0, bool(flip)), device_id_type=MESH,
                    )
                )
    for copy in plane:
        copy.start()
    direct_to(0, z < last - 1)
    direct_to(1, True)
    pass_first(lower & (z >= 4), True)
    await_tokens(False)
    patches(0, (0, 1))
    patches(2, (0, 1))
    hidden_rows(0, 0, 6)
    direct_to(2, True)
    hidden_rows(3, 0, 6)
    hidden_rows(1, 0, 2)
    hidden_rows(2, 0, 2)
    for z0 in range(3, EARLY):
        direct_to(z0, True)
    total = mine[...]
    all_plane = pltpu.make_async_remote_copy(
        plane_in, plane_in, sums_send, plane_recv, device_id=near(0, 0, True), device_id_type=MESH
    )
    all_plane.wait_recv()
    for slot in range(plane_in.shape[0]):
        total = total + plane_in[slot]
    plane_sum[...] = total
    def ring_copy(d):
        return pltpu.make_async_remote_copy(
            plane_sum, ring_in.at[d - 1], sums_send, ring_recv,
            device_id=near(0, d, False), device_id_type=MESH,
        )

    def straight(d):
        return late & (z + d >= RING_Z) & (z + d < RING_Z + EARLY)

    pass_first(middle, z == RING_Z // 2)
    upper = (z > RING_Z // 2 + 1) & jnp.logical_not(late)

    @pl.when(upper)
    def _():
        pl.semaphore_wait(know_all, 1)

    for d in (*range(5, RING_Z), *range(1, 5)):

        @pl.when(jnp.logical_not(straight(d)) & ((d == 1) | (z + d >= RING_Z)))
        def _():
            ring_copy(d).start()
    @pl.when(early)
    def _():
        transform(2)
    @pl.when((z > 1) & (z < last) & jnp.logical_not(upper))
    def _():
        pl.semaphore_wait(know_all, 1)

    for z0 in range(2, EARLY):
        tell_plane(z0)
    for d in range(2, RING_Z):

        @pl.when(z + d <= last)
        def _():
            ring_copy(d).start()
    @pl.when(jnp.logical_not(early))
    def _():
        for p in range(3):
            transform(p)
    tokens_left()
    def ring_copies(number):
        return pltpu.make_async_remote_copy(
            ring_in.at[pl.ds(0, number)], ring_in.at[pl.ds(0, number)], sums_send, ring_recv,
            device_id=near(0, 1, False), device_id_type=MESH,
        )

    def direct_copies(number):
        return pltpu.make_async_remote_copy(
            direct_in.at[pl.ds(0, number)], direct_in.at[pl.ds(0, number)], sums_send, direct_recv,
            device_id=near(0, 1, False), device_id_type=MESH,
        )

    @pl.when(z < EARLY)
    def _():
        ring_copies(last - LATE).wait_recv()
    @pl.when(z < EARLY)
    def _():
        direct_copies(8 * LATE).wait_recv()

    @pl.when(z >= EARLY)
    def _():
        ring_copies(last).wait_recv()

    for slot in range(ring_in.shape[0]):
        total = total + ring_in[slot]
    rows = [direct_in[slot] for slot in range(8 * LATE)]
    while len(rows) > 1:
        rows = [sum(rows[at + 1 : at + 2], rows[at]) for at in range(0, len(rows), 2)]
    total = total + rows[0]
    count = n_ha * lax.axis_size("ta") * 4 * 2 * 2 * tokens * members
    total = total * (1.0 / count)
    mean, square = product((jnp.where(of_sums, total, 0.0), jnp.where(of_sums, 0.0, total)), spread[...])
    var = jnp.maximum(square - mean * mean, 0.0)
    scale = lax.rsqrt(var + EPS) * vectors[1].reshape(1, -1)
    stat_ref[0:1] = 0.5 * scale
    stat_ref[1:2] = 0.5 * (vectors[2].reshape(1, -1) - mean * scale)

    by_late = len(plane) + last - EARLY + 8 * EARLY

    @pl.when(late)
    def _():
        direct_copies(by_late).wait_send()

    @pl.when(jnp.logical_not(late))
    def _():
        direct_copies(len(plane) + last).wait_send()


def decode_kernel(
    h_ref, stat_ref, main_ref, rest_ref, out_hbm,
    shifted, columns_wide, columns_rest, planes_wide, planes_rest, products, total, rows_f32, out, out_sem,
):
    ha, ta = lax.axis_index("ha"), lax.axis_index("ta")
    n_ha = lax.axis_size("ha")
    frames_in, rows_in, pieces, tokens, _ = h_ref.shape
    parts = pieces // 2
    channels = 128 * parts
    frames, rows = frames_in - 2, rows_in - 2
    wide = main_ref.shape[2]
    rest = channels - wide
    for f in range(frames_in):
        for part in range(parts):
            for y in range(rows_in):
                shifted[f, part, y, 0, 8 + tokens :] = jnp.zeros((8, 128), F32)
                shifted[f, part, y, 1, :8] = jnp.zeros((8, 128), F32)

    held = {}

    def activate(y, b):
        later = held.get("product", 0.0)
        for f in range(frames_in):
            inside = (ha * rows + y >= 1) & (ha * rows + y <= n_ha * rows)
            if f < 2:
                inside = inside & (ta > 0)
            for part in range(parts):
                lanes = slice(128 * part, 128 * part + 128)
                row_scale = jnp.where(inside, stat_ref[0:1, lanes], 0.0) + later
                row_shift = jnp.where(inside, stat_ref[1:2, lanes], 0.0)
                value = h_ref[f, y, b * parts + part] * row_scale + row_shift
                shifted[f, part, y, b, 8 : 8 + tokens] = value + value * jnp.tanh(value)

    def by_columns(y, k):
        def one(f, part):
            even, odd = [shifted.at[f, part, y, b] for b in (0, 1)]
            if k == 0:
                return odd[7 : 7 + tokens] - odd[8 : 8 + tokens]
            if k == 1:
                return even[8 : 8 + tokens] + odd[8 : 8 + tokens]
            if k == 2:
                return odd[8 : 8 + tokens] - even[8 : 8 + tokens]
            return even[8 : 8 + tokens] - even[9 : 9 + tokens]

        for f in range(frames_in):
            value = jnp.concatenate([one(f, part) for part in range(wide // 128)], axis=-1)
            columns_wide[k, f, y] = value.astype(BF16)
        for f in range(0, frames_in, 2):
            value = jnp.concatenate([one(f, parts - 1), one(f + 1, parts - 1)], axis=-1)
            columns_rest[k, f // 2, y] = value.astype(BF16)

    order = [(i, k) for i in range(4) for k in ((1, 2, 0, 3) if i else range(4))]
    slot_of = {pair: step % 2 for step, pair in enumerate(order)}

    def by_rows(i, k):
        one, two = ((0, 2), (1, 2), (2, 1), (1, 3))[i]
        for columns, planes, slot in ((columns_wide, planes_wide, slot_of[i, k]), (columns_rest, planes_rest, k)):
            if i == 1:
                planes[slot] = columns[k, :, one] + columns[k, :, two]
            else:
                planes[slot] = columns[k, :, one] - columns[k, :, two]

    ahead = {
        0: [(activate, 0, 0), (activate, 2, 0), (by_columns, 0, 1), (by_columns, 2, 1)],
        1: [(by_columns, 0, 2), (by_columns, 2, 2), (activate, 1, 1)],
        2: [(by_columns, 0, 3), (by_columns, 2, 3), (activate, 1, 0)],
        3: [(by_columns, 1, 0), (by_columns, 1, 1)],
        4: [(by_columns, 1, 2), (by_columns, 1, 3)],
        5: [(activate, 3, 1)],
        6: [(activate, 3, 0)],
        7: [(by_columns, 3, 0)],
        8: [(by_columns, 3, 1)],
        9: [(by_columns, 3, 2)],
        10: [(by_columns, 3, 3)],
    }
    for y in (0, 2):
        activate(y, 1)
    for y in (0, 2):
        by_columns(y, 0)
    by_rows(0, 0)
    bias = stat_ref[2:3]
    copies = []

    def done(y, b, f, part, value):
        hidden = h_ref[f + 2, y + 1, b * parts + part] + bias[:, 128 * part : 128 * part + 128]
        rows_f32[y, f, part, pl.ds(b, tokens, stride=2)] = value + hidden

    def send(y, f):
        for part in range(parts):
            out[f, y, :, 128 * part : 128 * part + 128] = rows_f32[y, f, part].astype(BF16)
        copies.append(pltpu.make_async_copy(out.at[f, y], out_hbm.at[f, y], out_sem))
        copies[-1].start()

    def combine(i, f):
        for part in range(parts):
            m0, m1, m2, m3 = [products[i % 2, k, f, part] for k in range(4)]
            for b, value in ((0, m0 + m1 + m2), (1, m1 - m2 - m3)):
                if i == 0:
                    total[0, b, f, part] = value
                elif i == 1:
                    total[0, b, f, part] = total[0, b, f, part] + value
                    total[1, b, f, part] = value
                elif i == 2:
                    done(0, b, f, part, total[0, b, f, part] + value)
                    total[1, b, f, part] = total[1, b, f, part] - value
        if i == 2:
            send(0, f)

    def last_even(f):
        for part in range(parts):
            m0, m1, m2 = [products[1, k, f, part] for k in range(3)]
            done(1, 0, f, part, total[1, 0, f, part] - (m0 + m1 + m2))
            total[1, 1, f, part] = total[1, 1, f, part] - (m1 - m2)

    def last_odd(f):
        for part in range(parts):
            done(1, 1, f, part, total[1, 1, f, part] + products[1, 3, f, part])
        send(1, f)

    for step, (i, k) in enumerate(order):
            at = 4 * i + k
            for make, one, two in ahead.get(step, ()):
                make(one, two)
            if step < 15:
                by_rows(*order[step + 1])
            if i and step % 4 < 2:
                combine(i - 1, 2 * (step % 4))
                combine(i - 1, 2 * (step % 4) + 1)
            if step == 15:
                for f in range(frames):
                    last_even(f)

            def last_channels(f, k):
                return planes_rest[k, f // 2, :, rest * (f % 2) : rest * (f % 2) + rest]

            def plane(f):
                return jnp.concatenate([planes_wide[slot_of[i, k], f], last_channels(f, k)], axis=-1)

            lhs = [[plane(f + p) for p in range(3)] for f in range(frames)]
            if i and k in (0, 3):
                lhs = [taps + [last_channels(f + 2, 2)] for f, taps in enumerate(lhs)]
            lhs = jnp.concatenate([jnp.concatenate(taps, axis=-1) for taps in lhs], axis=0)
            if i and k == 2:
                lhs = lhs[:, : 3 * channels - rest]
            product = jnp.dot(lhs, main_ref[at, : lhs.shape[1]], preferred_element_type=F32)
            held["product"] = 0.0 * product[0:1, 0:128]
            for part in range(wide // 128):
                products[i % 2, k, :, part] = product[:, 128 * part : 128 * part + 128].reshape(frames, tokens, 128)
            lhs = [
                jnp.concatenate([plane(t + p) for p in range(4)], axis=-1)
                for t in range(0, frames, 2)
            ]
            product = jnp.dot(jnp.concatenate(lhs, axis=0), rest_ref[at], preferred_element_type=F32)
            for f in range(frames):
                products[i % 2, k, f, wide // 128] = product[
                    f // 2 * tokens : (f // 2 + 1) * tokens, rest * (f % 2) : rest * (f % 2) + rest
                ]
    for f in range(frames):
        last_odd(f)
    pltpu.make_async_copy(out, out_hbm, out_sem).wait()


def keep(value):
    return pltpu.with_memory_space_constraint(value, pltpu.HBM)


def body(latent_tokens, w_in, b_in, gn_gain, gn_shift, w_mid, b_mid):
    half = latent_tokens.shape[1]
    channels = w_in.shape[-1]
    tokens = 2 * half
    wide = channels // 256 * 256
    rest = channels - wide
    parts = channels // 128
    vmem = pl.BlockSpec(memory_space=pltpu.VMEM)
    hbm = pl.BlockSpec(memory_space=pltpu.HBM)
    inputs = (latent_tokens, w_in.reshape(3, 3, -1, channels), b_in, gn_gain, gn_shift, b_mid, w_mid)
    prepared = pl.pallas_call(
        exchange_kernel,
        out_shape=(
            jax.ShapeDtypeStruct((6, 4, 2 * parts, tokens, 128), F32),
            jax.ShapeDtypeStruct((3, channels), F32),
            jax.ShapeDtypeStruct((16, 3 * channels + rest, wide), BF16),
            jax.ShapeDtypeStruct((16, 4 * channels, 2 * rest), BF16),
        ),
        in_specs=[hbm] * len(inputs),
        out_specs=(vmem, vmem, vmem, vmem),
        scratch_shapes=[
            pltpu.VMEM(latent_tokens.shape, BF16),
            pltpu.VMEM((4, channels), F32),
            pltpu.VMEM((2, 2, half, 128), BF16),
            pltpu.VMEM((3, 2, 2, tokens, 128), BF16),
            pltpu.VMEM((8, 3, tokens, 128), BF16),
            pltpu.VMEM((2, 4 * tokens, 2 * channels), F32),
            pltpu.VMEM((2, 3, 4, 64, 2 * channels), BF16),
            pltpu.VMEM(w_mid.shape, BF16),
            pltpu.VMEM((1, 128), F32),
            pltpu.VMEM((7, 1, 128), F32),
            pltpu.VMEM((1, 128), F32),
            pltpu.VMEM((RING_Z - 1, 1, 128), F32),
            pltpu.VMEM((max(8 * LATE, 2 * RING_X - 1 + RING_Z - 1 + 7 * EARLY), 1, 128), F32),
            pltpu.VMEM((2 * 384, 4 * 128), BF16),
            pltpu.VMEM((channels, 128), BF16),
            pltpu.VMEM((128, channels), BF16),
            pltpu.SemaphoreType.DMA,
            pltpu.SemaphoreType.DMA,
            pltpu.SemaphoreType.DMA,
            pltpu.SemaphoreType.DMA((3,)),
            pltpu.SemaphoreType.DMA,
            pltpu.SemaphoreType.DMA((3,)),
            pltpu.SemaphoreType.DMA,
            pltpu.SemaphoreType.DMA,
            pltpu.SemaphoreType.DMA,
            pltpu.SemaphoreType.DMA,
            pltpu.SemaphoreType.REGULAR,
            pltpu.SemaphoreType.REGULAR,
            pltpu.SemaphoreType.REGULAR,
            pltpu.SemaphoreType.REGULAR((EARLY,)),
        ],
        compiler_params=pltpu.CompilerParams(
            collective_id=0, has_side_effects=True, vmem_limit_bytes=18 * 2**20
        ),
        name="exchange",
    )(*[keep(value) for value in inputs])
    return pl.pallas_call(
        decode_kernel,
        out_shape=jax.ShapeDtypeStruct((4, 2, 2 * tokens, channels), BF16),
        in_specs=[vmem, vmem, vmem, vmem],
        out_specs=hbm,
        scratch_shapes=[
            pltpu.VMEM((6, parts, 4, 2, tokens + 16, 128), F32),
            pltpu.VMEM((4, 6, 4, tokens, wide), BF16),
            pltpu.VMEM((4, 3, 4, tokens, 2 * rest), BF16),
            pltpu.VMEM((2, 6, tokens, wide), BF16),
            pltpu.VMEM((4, 3, tokens, 2 * rest), BF16),
            pltpu.VMEM((2, 4, 4, parts, tokens, 128), F32),
            pltpu.VMEM((2, 2, 4, parts, tokens, 128), F32),
            pltpu.VMEM((2, 4, parts, 2 * tokens, 128), F32),
            pltpu.VMEM((4, 2, 2 * tokens, channels), BF16),
            pltpu.SemaphoreType.DMA,
        ],
        compiler_params=pltpu.CompilerParams(vmem_limit_bytes=22 * 2**20),
        name="decode",
    )(*prepared)


def solution(mesh):
    return jax.shard_map(
        body,
        mesh=mesh,
        in_specs=(P("clip", ("ha", "ta"), None), P(), P(), P(), P(), P(), P()),
        out_specs=P(("clip", "ta"), "ha", None, None),
        check_vma=False,
    )
```
